32 devices in a mesh: wave: 16 (over z, x, core), lev: 2 (over y).
Axes of the slice: x: 2, y: 2, z: 4, core: 2. Of those that a mesh axis runs over, the one named last changes fastest.
Arguments:
- spin_tendency: bfloat16 [32, 2, 136, 768], P('wave', None, 'lev'), may hold values from -6 to 6
- spreading_source: bfloat16 [32, 2, 136, 768], P('wave', None, 'lev'), may hold values from -6 to 6
- heat_source: bfloat16 [32, 2, 136, 768], P('wave', None, 'lev'), may hold values from -6 to 6
- helmholtz_inverses: bfloat16 [2, 384, 136, 136], P('lev', 'wave'), may hold values from -0.5 to 0.5
- heat_spreading_coupler: bfloat16 [136, 136], replicated, may hold values from -0.5 to 0.5
- smoothing_strengths: float32 [136], replicated, may hold values from 0.5 to 30
- azimuthal_order_list: int32 [32], P('wave'), may hold values from 0 to 767
Outputs:
- vorticity_new: bfloat16 [32, 2, 136, 768], P('wave', None, 'lev')
- divergence_new: bfloat16 [32, 2, 136, 768], P('wave', None, 'lev')
- temperature_new: bfloat16 [32, 2, 136, 768], P('wave', None, 'lev')
The draws below stay inside these ranges and needn't reach their ends.
All inputs are finite; a program needn't handle non-finite values.
Results may differ from the reference program's by a relative error of at most 0.0075.
Values may be sent and summed in bfloat16 or wider, within the bound.
A program may use at most 64 MiB of HBM per device.

```python
import math
import jax
import jax.numpy as jnp
from jax import lax

DEGREE_LIMIT = 768
STRATA_NUMBER = 136
ORDER_ENTRIES = 32
NQ = 384
N_LEV = 2


def with_ends(drawn, own_key, least, top_value):
    longest = drawn.shape.index(max(drawn.shape))
    spots = []
    for shift in (0, 1):
        where = [jax.random.randint(jax.random.fold_in(own_key, axis), (), 0, length) for axis, length in enumerate(drawn.shape)]
        where[longest] = (where[longest] + shift) % drawn.shape[longest]
        spots.append(tuple(where))
    return drawn.at[spots[0]].set(least).at[spots[1]].set(top_value)


def block_levels(rng, shape, split, low, high):
    loudness, own = 1.0, jax.random.fold_in(rng, 6)
    for position, parts in split:
        steps = jnp.exp(jax.random.uniform(jax.random.fold_in(own, position), (parts,), jnp.float32, low / len(split), high / len(split)))
        loudness = loudness * jnp.repeat(steps, shape[position] // parts).reshape([-1 if axis == position else 1 for axis in range(len(shape))])
    return loudness


def noise(key, extent, scale, most, shards=(), held_as=jnp.bfloat16):
    array = jax.random.normal(key, extent, jnp.float32) * scale
    if len(shards) > 0:
        array = block_levels(key, extent, shards, -0.22, 0.18) * array
    return jnp.clip(array, min=-most, max=most).astype(held_as)


def setup_inputs(seed: int = 0) -> dict:
    key_of = jax.random.split(jax.random.key(seed), 8)
    return {
        "spin_tendency": noise(key_of[0], (ORDER_ENTRIES, 2, STRATA_NUMBER, DEGREE_LIMIT), 1.0, 6.0, ((0, 16), (2, 2))),
        "spreading_source": noise(key_of[1], (ORDER_ENTRIES, 2, STRATA_NUMBER, DEGREE_LIMIT), 1.0, 6.0, ((0, 16), (2, 2))),
        "heat_source": noise(key_of[2], (ORDER_ENTRIES, 2, STRATA_NUMBER, DEGREE_LIMIT), 1.0, 6.0, ((0, 16), (2, 2))),
        "helmholtz_inverses": noise(key_of[3], (N_LEV, NQ, STRATA_NUMBER, STRATA_NUMBER), STRATA_NUMBER ** -0.5, 0.5, ((0, 2), (1, 16))),
        "heat_spreading_coupler": noise(key_of[4], (STRATA_NUMBER, STRATA_NUMBER), STRATA_NUMBER ** -0.5, 0.5),
        "smoothing_strengths": jnp.clip(jnp.exp(jax.random.uniform(key_of[5], (STRATA_NUMBER,), jnp.float32, math.log(0.5), math.log(30.0))), 0.5, 30.0),
        "azimuthal_order_list": with_ends(jax.random.randint(key_of[6], (ORDER_ENTRIES,), 0, DEGREE_LIMIT), jax.random.fold_in(key_of[6], 1), 0, DEGREE_LIMIT - 1).astype(jnp.int32),
    }


def damping_table(smoothing_strengths, wavenumbers):
    scaled = (wavenumbers * (wavenumbers + 1)).astype(jnp.float32) / jnp.float32((DEGREE_LIMIT - 1) * DEGREE_LIMIT)
    return 1.0 / (1.0 + smoothing_strengths.astype(jnp.float32)[:, None] * scaled[None, :] ** 2)


def reference(spin_tendency, spreading_source, heat_source, helmholtz_inverses, heat_spreading_coupler, smoothing_strengths, azimuthal_order_list):
    matrices = helmholtz_inverses.reshape(DEGREE_LIMIT, STRATA_NUMBER, STRATA_NUMBER).astype(jnp.float32)
    blending_matrix = heat_spreading_coupler.astype(jnp.float32)
    wavenumbers = jnp.arange(DEGREE_LIMIT, dtype=jnp.int32)
    damping = damping_table(smoothing_strengths, wavenumbers)

    def lone_order_entry(members):
        rhs_div, rhs_temp, rhs_vort, zonal = members
        answer_fields = jnp.einsum("nkp,cpn->ckn", matrices, rhs_div.astype(jnp.float32)).astype(jnp.bfloat16)
        coupled = jnp.einsum("kp,cpn->ckn", blending_matrix, answer_fields.astype(jnp.float32)).astype(jnp.bfloat16)
        temp_new = (rhs_temp.astype(jnp.float32) - coupled.astype(jnp.float32)).astype(jnp.bfloat16)
        vort_new = (rhs_vort.astype(jnp.float32) * damping[None]).astype(jnp.bfloat16)
        interior_slice = (wavenumbers >= zonal)[None, None, :]
        empty_placeholder = jnp.zeros((), jnp.bfloat16)
        return (jnp.where(interior_slice, vort_new, empty_placeholder), jnp.where(interior_slice, answer_fields, empty_placeholder), jnp.where(interior_slice, temp_new, empty_placeholder))

    spin_updated, spreading_updated, heat_updated = lax.map(lone_order_entry, (spreading_source, heat_source, spin_tendency, azimuthal_order_list))
    return (spin_updated, spreading_updated, heat_updated)
```

```python
import functools
import jax
import jax.numpy as jnp
from jax import lax
from jax.experimental import pallas as pl
from jax.experimental.pallas import tpu as pltpu
from jax.sharding import PartitionSpec as P

LANES = 128
MESH = pl.DeviceIdType.MESH
NN = (((1,), (0,)), ((), ()))
NT = (((1,), (1,)), ((), ()))


def damping_table(level_gain, wavenumbers, total_n):
    scaled = (wavenumbers * (wavenumbers + 1)).astype(jnp.float32) / jnp.float32(
        (total_n - 1) * total_n
    )
    return 1.0 / (1.0 + level_gain[:, None] * scaled[None, :] ** 2)


def exchange_by_collectives(spreading_source, helmholtz_inverses, heat_spreading_coupler):
    lev_count = lax.axis_size("lev")
    row_count, part_count, lev_local, total_n = spreading_source.shape
    block_n = total_n // lev_count
    layer_count = lev_local * lev_count
    flat_rows = row_count * part_count
    wave_count = lax.axis_size("wave")
    local_n = block_n // wave_count
    rhs_div = lax.all_to_all(spreading_source, "lev", split_axis=3, concat_axis=2, tiled=True)
    outgoing = rhs_div.reshape(flat_rows, layer_count, wave_count, local_n).transpose(2, 3, 0, 1)
    outgoing = outgoing.reshape(wave_count, local_n, flat_rows * layer_count)
    columns = lax.all_to_all(outgoing, "wave", split_axis=0, concat_axis=0, tiled=True)
    columns = columns.reshape(wave_count, local_n, flat_rows, layer_count)
    solved_columns = jnp.einsum(
        "jkp,wjcp->wjck", helmholtz_inverses[0], columns, preferred_element_type=jnp.float32
    ).astype(jnp.bfloat16)
    solved_columns = solved_columns.reshape(wave_count, local_n, flat_rows * layer_count)
    returned = lax.all_to_all(solved_columns, "wave", split_axis=0, concat_axis=0, tiled=True)
    answer_fields = returned.reshape(block_n, flat_rows, layer_count).transpose(1, 2, 0)
    coupled = jnp.einsum(
        "om,dms->dos", heat_spreading_coupler, answer_fields, preferred_element_type=jnp.float32
    ).astype(jnp.bfloat16)
    both = jnp.stack([answer_fields, coupled])
    both = lax.all_to_all(both, "lev", split_axis=2, concat_axis=3, tiled=True)
    both = both.reshape(2, row_count, part_count, lev_local, total_n)
    spreading_updated, coupled_out = both[0], both[1]
    return spreading_updated, coupled_out


def f32_dot(left, right, dims):
    return lax.dot_general(left, right, dims, preferred_element_type=jnp.float32)


def grid_of(shape, axis):
    return lax.broadcasted_iota(jnp.int32, shape, axis)


def ones_where(condition, dtype=jnp.bfloat16):
    return jnp.where(condition, 1.0, 0.0).astype(dtype)


def step_kernel(
    wave_count, lev_count, spin, source, heat, matrices, coupler, strengths, orders,
    vort_out, div_out, temp_out,
    spin_in, source_in, heat_in, mats_in, coupler_in, strengths_in, orders_in,
    first_out, next_out, first_in, next_in, gathered, rest_in, tables, strided, rest_out,
    weights, back_out, back_in, relayed,
    load_sem, fwd_send, fwd_recv, back_send, back_recv, relay_send, relay_recv,
):
    wave, lev = lax.axis_index("wave"), lax.axis_index("lev")
    row_count, lev_local, part_count, total_n = source.shape
    block_n = total_n // lev_count
    local_n = block_n // wave_count
    groups = local_n // 8
    layer_count = lev_local * lev_count
    fields = lev_local * part_count
    half = LANES // part_count
    short = lev_local - half
    extra = layer_count - LANES
    depth = tables.shape[1]
    sources = wave_count * lev_count

    loads = []
    for i, (src, dst) in enumerate(
        ((source, source_in), (matrices, mats_in), (coupler, coupler_in), (strengths, strengths_in),
         (orders, orders_in), (spin, spin_in), (heat, heat_in))
    ):
        copy = pltpu.make_async_copy(src, dst, load_sem.at[i])
        copy.start()
        loads.append(copy)

    order = sorted(range(wave_count), key=lambda s: abs(2 * s - wave_count))
    peers = [(lax.rem(wave + s, wave_count), lax.rem(lev + t, lev_count), s * lev_count + t)
             for s in order for t in range(lev_count) if s or t]
    wave_peers = [(lax.rem(wave + s, wave_count), s) for s in order if s]
    arrivals = [(lax.rem(wave + wave_count - s, wave_count), s) for s in order if s]
    barrier = pltpu.get_barrier_semaphore()
    for w, q, _ in peers:
        pl.semaphore_signal(barrier, inc=1, device_id=(w, q), device_id_type=MESH)

    wide = 2 * LANES
    out_row, in_row = grid_of((wide, fields), 0), grid_of((wide, fields), 1)
    level, part = in_row // part_count, in_row % part_count
    main_spot = lax.rem(part + lev, part_count) * half + level
    eye = ones_where(grid_of((wide, wide), 0) == grid_of((wide, wide), 1))
    loads[0].wait()
    flat = source_in.reshape(row_count, fields, total_n)
    mains, rest = [], None
    for r in range(row_count):
        rest_spot = LANES + (r * part_count + part) * extra + lev * short + level - half
        spot = jnp.where(level < half, main_spot, rest_spot)
        picked = f32_dot(ones_where(out_row == spot), flat[r], NN)
        mains.append(picked[:LANES].astype(jnp.bfloat16))
        rest = picked[LANES:] if rest is None else rest + picked[LANES:]
    mains[0] = jnp.concatenate([mains[0], rest.astype(jnp.bfloat16)], axis=0)
    step = row_count * part_count * extra
    for r in range(row_count):
        turned = jnp.concatenate(
            [f32_dot(eye, mains[r][:, k:k + wide], NT) for k in range(0, total_n, wide)], axis=0
        )
        main = turned[:, :LANES].reshape(sources, local_n, LANES)
        if r:
            next_out[r - 1] = main.astype(jnp.bfloat16)
            continue
        tail = turned[:, LANES:].reshape(sources, groups, 8, LANES)
        folded = tail[:, 0].reshape(sources * 8, LANES)
        for g in range(1, groups):
            folded += pltpu.roll(tail[:, g].reshape(sources * 8, LANES), g * step, 1)
        first_out[...] = jnp.concatenate(
            [main, folded.reshape(sources, 8, LANES)], axis=1
        ).astype(jnp.bfloat16)

    pl.semaphore_wait(barrier, sources - 1)
    mine = lev * wave_count + wave

    def outgoing(r):
        return first_out if r == 0 else next_out.at[r - 1]

    def incoming(r):
        return first_in if r == 0 else next_in.at[r - 1]

    fwd = []
    for r in range(row_count):
        fwd.append([])
        for w, q, i in peers:
            copy = pltpu.make_async_remote_copy(
                src_ref=outgoing(r).at[q * wave_count + w], dst_ref=incoming(r).at[mine],
                send_sem=fwd_send.at[r, i], recv_sem=fwd_recv.at[r, i],
                device_id=(w, q), device_id_type=MESH,
            )
            copy.start()
            fwd[r].append(copy)
    for r in range(row_count):
        incoming(r)[mine] = outgoing(r)[mine]

    loads[1].wait()
    deep, flat_level = grid_of((depth, layer_count), 0), grid_of((depth, layer_count), 1)
    owner, place = flat_level // lev_local, flat_level % lev_local
    spot = jnp.where(place < half, owner * half + place, LANES + owner * short + place - half)
    ordered = ones_where(deep == spot)
    lanes = grid_of((depth, LANES), 1)
    zeros = jnp.zeros((depth, LANES - extra), jnp.float32)

    def prepare(s, carry):
        for g in range(groups):
            j = g * 8 + s
            turned = f32_dot(ordered, mats_in[j], NT)
            last = jnp.concatenate([turned[:, LANES:], zeros], axis=1)
            if g:
                last = pltpu.roll(last, g * part_count * extra, 1)
            tables[j] = jnp.concatenate([turned[:, :LANES], last], axis=1).astype(jnp.bfloat16)
        return carry

    lax.fori_loop(0, 8, prepare, 0)

    loads[2].wait()
    row, col = grid_of((fields, layer_count), 0), grid_of((fields, layer_count), 1)
    chosen = ones_where(col == lev * lev_local + row // part_count)
    coupled_rows = f32_dot(chosen, coupler_in[...], NN)
    tops = jnp.concatenate([chosen.astype(jnp.float32), coupled_rows], axis=0)
    tops_part = lax.rem(grid_of(tops.shape, 0), part_count)
    keeps = [jnp.where(tops_part == c, tops, 0.0) for c in range(part_count)]
    pieces = [k[:, :LANES] for k in keeps] + [k[:, LANES:] for k in keeps]
    pieces.append(jnp.zeros((2 * fields, LANES - part_count * extra), jnp.float32))
    weights[...] = jnp.concatenate(pieces, axis=1).astype(jnp.bfloat16)

    for copy in loads[3:6]:
        copy.wait()
    row, col = grid_of((fields, layer_count), 0), grid_of((fields, layer_count), 1)
    gain = jnp.sum(
        jnp.where(col == lev * lev_local + row // part_count, strengths_in[...], 0.0),
        axis=1, keepdims=True,
    )
    n = grid_of((1, total_n), 1)
    scaled = (n * (n + 1)).astype(jnp.float32) / jnp.float32((total_n - 1) * total_n)
    damping = 1.0 / (1.0 + gain * scaled ** 2)
    spin_flat = spin_in.reshape(row_count, fields, total_n)
    vort_flat = vort_out.reshape(row_count, fields, total_n)
    for r in range(row_count):
        value = (spin_flat[r].astype(jnp.float32) * damping)
        value = jnp.where(n >= orders_in[:, r:r + 1], value, 0.0)
        vort_flat[r] = value.astype(jnp.bfloat16)

    lane = grid_of((wave_count, LANES), 1)
    back = []
    for r in range(row_count):
        for copy in fwd[r]:
            copy.wait_recv()
        for p in range(lev_count):
            part_in = incoming(r)[pl.ds(p * wave_count, wave_count)].astype(jnp.float32)
            gathered[p] = part_in[:, :local_n].reshape(block_n, LANES)
            if r == 0:
                value = part_in[:, local_n:].reshape(wave_count * 8, LANES)
                rest_sum = value if p == 0 else rest_sum + value
        if r == 0:
            rest_in[...] = rest_sum

        def solve(s, carry):
            rest = rest_in[pl.ds(s, wave_count, stride=8), :]
            lasts = None
            for g in range(groups):
                j = g * 8 + s
                rows = pl.ds(j, wave_count, stride=local_n)
                low, high = gathered[0, rows, :], gathered[1, rows, :]
                sides = [jnp.where(lane < half, low, high),
                         pltpu.roll(jnp.where(lane < half, high, low), half, 1)]
                stacked = []
                for c in range(part_count):
                    shift = g * step + (r * part_count + c) * extra
                    moved = pltpu.roll(rest, LANES - shift, 1) if shift else rest
                    stacked.append(jnp.concatenate([sides[c], moved], axis=1)[:, :depth])
                stacked = jnp.concatenate(stacked, axis=0).astype(jnp.bfloat16)
                result = f32_dot(stacked, tables[j], NN)
                for c in range(part_count):
                    strided[c, rows, :] = result[c * wave_count:(c + 1) * wave_count, :LANES]
                last = result[:, LANES:]
                lasts = last if lasts is None else lasts + last
            total = lasts[:wave_count]
            for c in range(1, part_count):
                total += pltpu.roll(lasts[c * wave_count:(c + 1) * wave_count], c * extra, 1)
            rest_out[pl.ds(s, wave_count, stride=8), :] = total
            return carry

        lax.fori_loop(0, 8, solve, 0, unroll=2)
        pieces = [strided[c].reshape(wave_count, local_n, LANES) for c in range(part_count)]
        pieces.append(rest_out[...].reshape(wave_count, 8, LANES))
        back_out[r] = jnp.concatenate(pieces, axis=1).astype(jnp.bfloat16)
        back.append([])
        for w, s in wave_peers:
            copy = pltpu.make_async_remote_copy(
                src_ref=back_out.at[r, w], dst_ref=back_in.at[r, wave],
                send_sem=back_send.at[r, s], recv_sem=back_recv.at[r, s],
                device_id=(w, lev), device_id_type=MESH,
            )
            copy.start()
            back[r].append(copy)
        back_in[r, wave] = back_out[r, wave]

    relays = [[] for _ in range(row_count)]
    other = lax.rem(lev + 1, lev_count)

    def relay(r, spot, index):
        copy = pltpu.make_async_remote_copy(
            src_ref=back_in.at[r, spot], dst_ref=relayed.at[r, spot],
            send_sem=relay_send.at[r, index], recv_sem=relay_recv.at[r, index],
            device_id=(wave, other), device_id_type=MESH,
        )
        copy.start()
        relays[r].append(copy)

    heat_flat = heat_in.reshape(row_count, fields, total_n)
    div_flat = div_out.reshape(row_count, fields, total_n)
    temp_flat = temp_out.reshape(row_count, fields, total_n)

    def finish(r, wire, block):
        value = wire[r].astype(jnp.float32)
        sides = [value[:, c * local_n:(c + 1) * local_n].reshape(block_n, LANES)
                 for c in range(part_count)]
        folded = value[:, part_count * local_n:].reshape(wave_count * 8, LANES)
        turn = part_count * extra
        rest = [(pltpu.roll(folded, LANES - g * turn, 1) if g else folded)
                .reshape(wave_count, 1, 8, LANES) for g in range(groups)]
        sides.append(jnp.concatenate(rest, axis=1).reshape(block_n, LANES))
        packed = jnp.concatenate(sides, axis=1).astype(jnp.bfloat16)
        result = f32_dot(weights[...], packed, NT)
        spots = pl.ds(pl.multiple_of(block * block_n, LANES), block_n)
        inside = block * block_n + grid_of((1, block_n), 1) >= orders_in[:, r:r + 1]
        div_flat[r, :, spots] = jnp.where(inside, result[:fields], 0.0).astype(jnp.bfloat16)
        coupled = result[fields:].astype(jnp.bfloat16).astype(jnp.float32)
        warmed = heat_flat[r, :, spots].astype(jnp.float32) - coupled
        temp_flat[r, :, spots] = jnp.where(inside, warmed, 0.0).astype(jnp.bfloat16)

    loads[6].wait()
    for r in range(row_count):
        relay(r, wave, 0)
        for (w, s), copy in zip(arrivals, back[r]):
            copy.wait_recv()
            relay(r, w, s)
        finish(r, back_in, lev)
        if r:
            for copy in relays[r - 1]:
                copy.wait_recv()
            finish(r - 1, relayed, other)
    for copy in relays[-1]:
        copy.wait_recv()
    finish(row_count - 1, relayed, other)
    for group in (*fwd, *back, *relays):
        for copy in group:
            copy.wait_send()


def by_kernel(spin, source, heat, matrices, coupler, strengths, orders):
    lev_count, wave_count = lax.axis_size("lev"), lax.axis_size("wave")
    row_count, part_count, lev_local, total_n = source.shape
    block_n = total_n // lev_count
    local_n = block_n // wave_count
    layer_count = lev_local * lev_count
    fields = lev_local * part_count
    sources = wave_count * lev_count
    depth = -(-layer_count // 16) * 16
    anywhere, vmem = pl.BlockSpec(memory_space=pl.ANY), pl.BlockSpec(memory_space=pltpu.VMEM)
    shape = (row_count, lev_local, part_count, total_n)
    bf16, f32 = jnp.bfloat16, jnp.float32
    field = jax.ShapeDtypeStruct(shape, bf16)
    dma = pltpu.SemaphoreType.DMA
    back_rows = part_count * local_n + 8
    wire = pltpu.VMEM((row_count, wave_count, back_rows, LANES), bf16)
    outs = pl.pallas_call(
        functools.partial(step_kernel, wave_count, lev_count),
        out_shape=(field,) * 3,
        in_specs=[anywhere] * 7,
        out_specs=(vmem,) * 3,
        scratch_shapes=[
            pltpu.VMEM(shape, bf16), pltpu.VMEM(shape, bf16), pltpu.VMEM(shape, bf16),
            pltpu.VMEM(matrices.shape[1:], bf16), pltpu.VMEM(coupler.shape, bf16),
            pltpu.VMEM((1, layer_count), f32), pltpu.VMEM((1, row_count), jnp.int32),
            pltpu.VMEM((sources, local_n + 8, LANES), bf16),
            pltpu.VMEM((row_count - 1, sources, local_n, LANES), bf16),
            pltpu.VMEM((sources, local_n + 8, LANES), bf16),
            pltpu.VMEM((row_count - 1, sources, local_n, LANES), bf16),
            pltpu.VMEM((lev_count, block_n, LANES), f32),
            pltpu.VMEM((wave_count * 8, LANES), f32),
            pltpu.VMEM((local_n, depth, 2 * LANES), bf16),
            pltpu.VMEM((part_count, block_n, LANES), f32),
            pltpu.VMEM((wave_count * 8, LANES), f32),
            pltpu.VMEM((2 * fields, 3 * LANES), bf16),
            wire, wire, wire,
            dma((7,)),
            dma((row_count, sources)), dma((row_count, sources)),
            dma((row_count, wave_count)), dma((row_count, wave_count)),
            dma((row_count, wave_count)), dma((row_count, wave_count)),
        ],
        compiler_params=pltpu.CompilerParams(
            collective_id=0, has_side_effects=True, vmem_limit_bytes=48 * 2**20
        ),
    )(
        spin.transpose(0, 2, 1, 3), source.transpose(0, 2, 1, 3), heat.transpose(0, 2, 1, 3),
        matrices[0], coupler, strengths.reshape(1, layer_count), orders.reshape(1, row_count),
    )
    return tuple(out.transpose(0, 2, 1, 3) for out in outs)


def kernel_fits(source_shape, lev_count, wave_count):
    row_count, part_count, lev_local, total_n = source_shape
    block_n = total_n // lev_count
    extra = lev_local * lev_count - LANES
    return (
        lev_count == 2
        and part_count == 2
        and row_count > 1
        and wave_count > 1
        and wave_count % 8 == 0
        and block_n % LANES == 0
        and total_n % (2 * LANES) == 0
        and block_n % (8 * wave_count) == 0
        and extra > 0
        and extra * row_count * part_count * (block_n // (8 * wave_count)) <= LANES
    )


def on_device(
    spin_tendency,
    spreading_source,
    heat_source,
    helmholtz_inverses,
    heat_spreading_coupler,
    smoothing_strengths,
    azimuthal_order_list,
):
    lev_count, wave_count = lax.axis_size("lev"), lax.axis_size("wave")
    lev_index = lax.axis_index("lev")
    lev_local, total_n = spreading_source.shape[2:]
    empty_placeholder = jnp.zeros((), jnp.bfloat16)
    if kernel_fits(spreading_source.shape, lev_count, wave_count):
        return by_kernel(
            spin_tendency, spreading_source, heat_source, helmholtz_inverses,
            heat_spreading_coupler, smoothing_strengths, azimuthal_order_list,
        )
    spreading_updated, coupled_out = exchange_by_collectives(
        spreading_source, helmholtz_inverses, heat_spreading_coupler
    )
    heat_updated = (heat_source.astype(jnp.float32) - coupled_out.astype(jnp.float32)).astype(
        jnp.bfloat16
    )
    level_gain = lax.dynamic_slice_in_dim(smoothing_strengths, lev_index * lev_local, lev_local)
    damping = damping_table(level_gain, jnp.arange(total_n, dtype=jnp.int32), total_n)
    spin_updated = (spin_tendency.astype(jnp.float32) * damping[None, None]).astype(jnp.bfloat16)
    interior_slice = (
        jnp.arange(total_n, dtype=jnp.int32)[None, :] >= azimuthal_order_list[:, None]
    )[:, None, None, :]
    return (
        jnp.where(interior_slice, spin_updated, empty_placeholder),
        jnp.where(interior_slice, spreading_updated, empty_placeholder),
        jnp.where(interior_slice, heat_updated, empty_placeholder),
    )


def solution(mesh):
    return jax.shard_map(
        on_device,
        mesh=mesh,
        in_specs=(
            P("wave", None, "lev", None),
            P("wave", None, "lev", None),
            P("wave", None, "lev", None),
            P("lev", "wave", None, None),
            P(),
            P(),
            P("wave"),
        ),
        out_specs=(
            P("wave", None, "lev", None),
            P("wave", None, "lev", None),
            P("wave", None, "lev", None),
        ),
        check_vma=False,
    )
```

```python
import functools
import jax
import jax.numpy as jnp
from jax import lax
from jax.experimental import pallas as pl
from jax.experimental.pallas import tpu as pltpu
from jax.sharding import PartitionSpec as P

LANES = 128
MESH = pl.DeviceIdType.MESH
NN = (((1,), (0,)), ((), ()))
NT = (((1,), (1,)), ((), ()))


def damping_table(level_gain, wavenumbers, total_n):
    scaled = (wavenumbers * (wavenumbers + 1)).astype(jnp.float32) / jnp.float32(
        (total_n - 1) * total_n
    )
    return 1.0 / (1.0 + level_gain[:, None] * scaled[None, :] ** 2)


def exchange_by_collectives(spreading_source, helmholtz_inverses, heat_spreading_coupler):
    lev_count = lax.axis_size("lev")
    row_count, part_count, lev_local, total_n = spreading_source.shape
    block_n = total_n // lev_count
    layer_count = lev_local * lev_count
    flat_rows = row_count * part_count
    wave_count = lax.axis_size("wave")
    local_n = block_n // wave_count
    rhs_div = lax.all_to_all(spreading_source, "lev", split_axis=3, concat_axis=2, tiled=True)
    outgoing = rhs_div.reshape(flat_rows, layer_count, wave_count, local_n).transpose(2, 3, 0, 1)
    outgoing = outgoing.reshape(wave_count, local_n, flat_rows * layer_count)
    columns = lax.all_to_all(outgoing, "wave", split_axis=0, concat_axis=0, tiled=True)
    columns = columns.reshape(wave_count, local_n, flat_rows, layer_count)
    solved_columns = jnp.einsum(
        "jkp,wjcp->wjck", helmholtz_inverses[0], columns, preferred_element_type=jnp.float32
    ).astype(jnp.bfloat16)
    solved_columns = solved_columns.reshape(wave_count, local_n, flat_rows * layer_count)
    returned = lax.all_to_all(solved_columns, "wave", split_axis=0, concat_axis=0, tiled=True)
    answer_fields = returned.reshape(block_n, flat_rows, layer_count).transpose(1, 2, 0)
    coupled = jnp.einsum(
        "om,dms->dos", heat_spreading_coupler, answer_fields, preferred_element_type=jnp.float32
    ).astype(jnp.bfloat16)
    both = jnp.stack([answer_fields, coupled])
    both = lax.all_to_all(both, "lev", split_axis=2, concat_axis=3, tiled=True)
    both = both.reshape(2, row_count, part_count, lev_local, total_n)
    spreading_updated, coupled_out = both[0], both[1]
    return spreading_updated, coupled_out


def f32_dot(left, right, dims):
    return lax.dot_general(left, right, dims, preferred_element_type=jnp.float32)


def grid_of(shape, axis):
    return lax.broadcasted_iota(jnp.int32, shape, axis)


def ones_where(condition, dtype=jnp.bfloat16):
    return jnp.where(condition, 1.0, 0.0).astype(dtype)


def step_kernel(
    wave_count, lev_count, spin, source, heat, matrices, coupler, strengths, orders,
    vort_out, div_out, temp_out,
    spin_in, source_in, heat_in, mats_in, coupler_in, strengths_in, orders_in,
    first_out, next_out, first_in, next_in, gathered, rest_in, tables, strided, rest_out,
    weights, back_out, back_in, relayed,
    load_sem, fwd_send, fwd_recv, back_send, back_recv, relay_send, relay_recv,
):
    wave, lev = lax.axis_index("wave"), lax.axis_index("lev")
    row_count, lev_local, part_count, total_n = source.shape
    block_n = total_n // lev_count
    local_n = block_n // wave_count
    groups = local_n // 8
    layer_count = lev_local * lev_count
    fields = lev_local * part_count
    half = LANES // part_count
    short = lev_local - half
    extra = layer_count - LANES
    depth = tables.shape[1]
    sources = wave_count * lev_count

    loads = []
    for i, (src, dst) in enumerate(
        ((source, source_in), (matrices, mats_in), (coupler, coupler_in), (strengths, strengths_in),
         (orders, orders_in), (spin, spin_in), (heat, heat_in))
    ):
        copy = pltpu.make_async_copy(src, dst, load_sem.at[i])
        copy.start()
        loads.append(copy)

    order = sorted(range(wave_count), key=lambda s: abs(2 * s - wave_count))
    peers = [(lax.rem(wave + s, wave_count), lax.rem(lev + t, lev_count), s * lev_count + t)
             for s in order for t in range(lev_count) if s or t]
    wave_peers = [(lax.rem(wave + s, wave_count), s) for s in order if s]
    arrivals = [(lax.rem(wave + wave_count - s, wave_count), s) for s in order if s]
    barrier = pltpu.get_barrier_semaphore()
    for w, q, _ in peers:
        pl.semaphore_signal(barrier, inc=1, device_id=(w, q), device_id_type=MESH)

    wide = 2 * LANES
    out_row, in_row = grid_of((wide, fields), 0), grid_of((wide, fields), 1)
    level, part = in_row // part_count, in_row % part_count
    main_spot = lax.rem(part + lev, part_count) * half + level
    eye = ones_where(grid_of((wide, wide), 0) == grid_of((wide, wide), 1))
    loads[0].wait()
    flat = source_in.reshape(row_count, fields, total_n)
    mains, rest = [], None
    for r in range(row_count):
        rest_spot = LANES + (r * part_count + part) * extra + lev * short + level - half
        spot = jnp.where(level < half, main_spot, rest_spot)
        picked = f32_dot(ones_where(out_row == spot), flat[r], NN)
        mains.append(picked[:LANES].astype(jnp.bfloat16))
        rest = picked[LANES:] if rest is None else rest + picked[LANES:]
    mains[0] = jnp.concatenate([mains[0], rest.astype(jnp.bfloat16)], axis=0)
    step = row_count * part_count * extra
    for r in range(row_count):
        turned = jnp.concatenate(
            [f32_dot(eye, mains[r][:, k:k + wide], NT) for k in range(0, total_n, wide)], axis=0
        )
        main = turned[:, :LANES].reshape(sources, local_n, LANES)
        if r:
            next_out[r - 1] = main.astype(jnp.bfloat16)
            continue
        tail = turned[:, LANES:].reshape(sources, groups, 8, LANES)
        folded = tail[:, 0].reshape(sources * 8, LANES)
        for g in range(1, groups):
            folded += pltpu.roll(tail[:, g].reshape(sources * 8, LANES), g * step, 1)
        first_out[...] = jnp.concatenate(
            [main, folded.reshape(sources, 8, LANES)], axis=1
        ).astype(jnp.bfloat16)

    pl.semaphore_wait(barrier, sources - 1)
    mine = lev * wave_count + wave

    def outgoing(r):
        return first_out if r == 0 else next_out.at[r - 1]

    def incoming(r):
        return first_in if r == 0 else next_in.at[r - 1]

    fwd = []
    for r in range(row_count):
        fwd.append([])
        for w, q, i in peers:
            copy = pltpu.make_async_remote_copy(
                src_ref=outgoing(r).at[q * wave_count + w], dst_ref=incoming(r).at[mine],
                send_sem=fwd_send.at[r, i], recv_sem=fwd_recv.at[r, i],
                device_id=(w, q), device_id_type=MESH,
            )
            copy.start()
            fwd[r].append(copy)
    for r in range(row_count):
        incoming(r)[mine] = outgoing(r)[mine]

    loads[1].wait()
    deep, flat_level = grid_of((depth, layer_count), 0), grid_of((depth, layer_count), 1)
    owner, place = flat_level // lev_local, flat_level % lev_local
    spot = jnp.where(place < half, owner * half + place, LANES + owner * short + place - half)
    ordered = ones_where(deep == spot)
    lanes = grid_of((depth, LANES), 1)
    zeros = jnp.zeros((depth, LANES - extra), jnp.float32)

    def prepare(s, carry):
        for g in range(groups):
            j = g * 8 + s
            turned = f32_dot(ordered, mats_in[j], NT)
            last = jnp.concatenate([turned[:, LANES:], zeros], axis=1)
            if g:
                last = pltpu.roll(last, g * part_count * extra, 1)
            tables[j] = jnp.concatenate([turned[:, :LANES], last], axis=1).astype(jnp.bfloat16)
        return carry

    lax.fori_loop(0, 8, prepare, 0)

    loads[2].wait()
    row, col = grid_of((fields, layer_count), 0), grid_of((fields, layer_count), 1)
    chosen = ones_where(col == lev * lev_local + row // part_count)
    coupled_rows = f32_dot(chosen, coupler_in[...], NN)
    tops = jnp.concatenate([chosen.astype(jnp.float32), coupled_rows], axis=0)
    tops_part = lax.rem(grid_of(tops.shape, 0), part_count)
    keeps = [jnp.where(tops_part == c, tops, 0.0) for c in range(part_count)]
    pieces = [k[:, :LANES] for k in keeps] + [k[:, LANES:] for k in keeps]
    pieces.append(jnp.zeros((2 * fields, LANES - part_count * extra), jnp.float32))
    weights[...] = jnp.concatenate(pieces, axis=1).astype(jnp.bfloat16)

    for copy in loads[3:6]:
        copy.wait()
    row, col = grid_of((fields, layer_count), 0), grid_of((fields, layer_count), 1)
    gain = jnp.sum(
        jnp.where(col == lev * lev_local + row // part_count, strengths_in[...], 0.0),
        axis=1, keepdims=True,
    )
    n = grid_of((1, total_n), 1)
    scaled = (n * (n + 1)).astype(jnp.float32) / jnp.float32((total_n - 1) * total_n)
    damping = 1.0 / (1.0 + gain * scaled ** 2)
    spin_flat = spin_in.reshape(row_count, fields, total_n)
    vort_flat = vort_out.reshape(row_count, fields, total_n)
    for r in range(row_count):
        value = (spin_flat[r].astype(jnp.float32) * damping)
        value = jnp.where(n >= orders_in[:, r:r + 1], value, 0.0)
        vort_flat[r] = value.astype(jnp.bfloat16)

    lane = grid_of((wave_count, LANES), 1)
    back = []
    for r in range(row_count):
        for copy in fwd[r]:
            copy.wait_recv()
        for p in range(lev_count):
            part_in = incoming(r)[pl.ds(p * wave_count, wave_count)].astype(jnp.float32)
            gathered[p] = part_in[:, :local_n].reshape(block_n, LANES)
            if r == 0:
                value = part_in[:, local_n:].reshape(wave_count * 8, LANES)
                rest_sum = value if p == 0 else rest_sum + value
        if r == 0:
            rest_in[...] = rest_sum

        def solve(s, carry):
            rest = rest_in[pl.ds(s, wave_count, stride=8), :]
            lasts = None
            for g in range(groups):
                j = g * 8 + s
                rows = pl.ds(j, wave_count, stride=local_n)
                low, high = gathered[0, rows, :], gathered[1, rows, :]
                sides = [jnp.where(lane < half, low, high),
                         pltpu.roll(jnp.where(lane < half, high, low), half, 1)]
                stacked = []
                for c in range(part_count):
                    shift = g * step + (r * part_count + c) * extra
                    moved = pltpu.roll(rest, LANES - shift, 1) if shift else rest
                    stacked.append(jnp.concatenate([sides[c], moved], axis=1)[:, :depth])
                stacked = jnp.concatenate(stacked, axis=0).astype(jnp.bfloat16)
                result = f32_dot(stacked, tables[j], NN)
                for c in range(part_count):
                    strided[c, rows, :] = result[c * wave_count:(c + 1) * wave_count, :LANES]
                last = result[:, LANES:]
                lasts = last if lasts is None else lasts + last
            total = lasts[:wave_count]
            for c in range(1, part_count):
                total += pltpu.roll(lasts[c * wave_count:(c + 1) * wave_count], c * extra, 1)
            rest_out[pl.ds(s, wave_count, stride=8), :] = total
            return carry

        lax.fori_loop(0, 8, solve, 0, unroll=2)
        pieces = [strided[c].reshape(wave_count, local_n, LANES) for c in range(part_count)]
        pieces.append(rest_out[...].reshape(wave_count, 8, LANES))
        back_out[r] = jnp.concatenate(pieces, axis=1).astype(jnp.bfloat16)
        back.append([])
        for w, s in wave_peers:
            copy = pltpu.make_async_remote_copy(
                src_ref=back_out.at[r, w], dst_ref=back_in.at[r, wave],
                send_sem=back_send.at[r, s], recv_sem=back_recv.at[r, s],
                device_id=(w, lev), device_id_type=MESH,
            )
            copy.start()
            back[r].append(copy)
        back_in[r, wave] = back_out[r, wave]

    relays = [[] for _ in range(row_count)]
    other = lax.rem(lev + 1, lev_count)

    def relay(r, spot, index):
        copy = pltpu.make_async_remote_copy(
            src_ref=back_in.at[r, spot], dst_ref=relayed.at[r, spot],
            send_sem=relay_send.at[r, index], recv_sem=relay_recv.at[r, index],
            device_id=(wave, other), device_id_type=MESH,
        )
        copy.start()
        relays[r].append(copy)

    heat_flat = heat_in.reshape(row_count, fields, total_n)
    div_flat = div_out.reshape(row_count, fields, total_n)
    temp_flat = temp_out.reshape(row_count, fields, total_n)

    def finish(r, wire, block):
        value = wire[r].astype(jnp.float32)
        sides = [value[:, c * local_n:(c + 1) * local_n].reshape(block_n, LANES)
                 for c in range(part_count)]
        folded = value[:, part_count * local_n:].reshape(wave_count * 8, LANES)
        turn = part_count * extra
        rest = [(pltpu.roll(folded, LANES - g * turn, 1) if g else folded)
                .reshape(wave_count, 1, 8, LANES) for g in range(groups)]
        sides.append(jnp.concatenate(rest, axis=1).reshape(block_n, LANES))
        packed = jnp.concatenate(sides, axis=1).astype(jnp.bfloat16)
        result = f32_dot(weights[...], packed, NT)
        spots = pl.ds(pl.multiple_of(block * block_n, LANES), block_n)
        inside = block * block_n + grid_of((1, block_n), 1) >= orders_in[:, r:r + 1]
        div_flat[r, :, spots] = jnp.where(inside, result[:fields], 0.0).astype(jnp.bfloat16)
        coupled = result[fields:].astype(jnp.bfloat16).astype(jnp.float32)
        warmed = heat_flat[r, :, spots].astype(jnp.float32) - coupled
        temp_flat[r, :, spots] = jnp.where(inside, warmed, 0.0).astype(jnp.bfloat16)

    loads[6].wait()
    for r in range(row_count):
        relay(r, wave, 0)
        for (w, s), copy in zip(arrivals, back[r]):
            copy.wait_recv()
            relay(r, w, s)
        finish(r, back_in, lev)
        if r:
            for copy in relays[r - 1]:
                copy.wait_recv()
            finish(r - 1, relayed, other)
    for copy in relays[-1]:
        copy.wait_recv()
    finish(row_count - 1, relayed, other)
    for group in (*fwd, *back, *relays):
        for copy in group:
            copy.wait_send()


def store_kernel(*refs):
    count = (len(refs) - 1) // 2
    copies = [
        pltpu.make_async_copy(refs[i], refs[count + i], refs[-1].at[i]) for i in range(count)
    ]
    for copy in copies:
        copy.start()
    for copy in copies:
        copy.wait()


def by_kernel(spin, source, heat, matrices, coupler, strengths, orders):
    lev_count, wave_count = lax.axis_size("lev"), lax.axis_size("wave")
    row_count, part_count, lev_local, total_n = source.shape
    block_n = total_n // lev_count
    local_n = block_n // wave_count
    layer_count = lev_local * lev_count
    fields = lev_local * part_count
    sources = wave_count * lev_count
    depth = -(-layer_count // 16) * 16
    anywhere, vmem = pl.BlockSpec(memory_space=pltpu.HBM), pl.BlockSpec(memory_space=pltpu.VMEM)
    shape = (row_count, lev_local, part_count, total_n)
    bf16, f32 = jnp.bfloat16, jnp.float32
    field = jax.ShapeDtypeStruct(shape, bf16)
    dma = pltpu.SemaphoreType.DMA
    back_rows = part_count * local_n + 8
    wire = pltpu.VMEM((row_count, wave_count, back_rows, LANES), bf16)
    outs = pl.pallas_call(
        functools.partial(step_kernel, wave_count, lev_count),
        out_shape=(field,) * 3,
        in_specs=[anywhere] * 7,
        out_specs=(vmem,) * 3,
        scratch_shapes=[
            pltpu.VMEM(shape, bf16), pltpu.VMEM(shape, bf16), pltpu.VMEM(shape, bf16),
            pltpu.VMEM(matrices.shape[1:], bf16), pltpu.VMEM(coupler.shape, bf16),
            pltpu.VMEM((1, layer_count), f32), pltpu.VMEM((1, row_count), jnp.int32),
            pltpu.VMEM((sources, local_n + 8, LANES), bf16),
            pltpu.VMEM((row_count - 1, sources, local_n, LANES), bf16),
            pltpu.VMEM((sources, local_n + 8, LANES), bf16),
            pltpu.VMEM((row_count - 1, sources, local_n, LANES), bf16),
            pltpu.VMEM((lev_count, block_n, LANES), f32),
            pltpu.VMEM((wave_count * 8, LANES), f32),
            pltpu.VMEM((local_n, depth, 2 * LANES), bf16),
            pltpu.VMEM((part_count, block_n, LANES), f32),
            pltpu.VMEM((wave_count * 8, LANES), f32),
            pltpu.VMEM((2 * fields, 3 * LANES), bf16),
            wire, wire, wire,
            dma((7,)),
            dma((row_count, sources)), dma((row_count, sources)),
            dma((row_count, wave_count)), dma((row_count, wave_count)),
            dma((row_count, wave_count)), dma((row_count, wave_count)),
        ],
        compiler_params=pltpu.CompilerParams(
            collective_id=0, has_side_effects=True, vmem_limit_bytes=48 * 2**20
        ),
    )(
        *(
            pltpu.with_memory_space_constraint(value, pltpu.HBM)
            for value in (
                spin.transpose(0, 2, 1, 3), source.transpose(0, 2, 1, 3), heat.transpose(0, 2, 1, 3),
                matrices[0], coupler, strengths.reshape(1, layer_count), orders.reshape(1, row_count),
            )
        )
    )
    outs = pl.pallas_call(
        store_kernel, out_shape=(field,) * 3, in_specs=[vmem] * 3, out_specs=(anywhere,) * 3,
        scratch_shapes=[dma((3,))],
        compiler_params=pltpu.CompilerParams(vmem_limit_bytes=4 * 2**20),
    )(*outs)
    return tuple(out.transpose(0, 2, 1, 3) for out in outs)


def kernel_fits(source_shape, lev_count, wave_count):
    row_count, part_count, lev_local, total_n = source_shape
    block_n = total_n // lev_count
    extra = lev_local * lev_count - LANES
    return (
        lev_count == 2
        and part_count == 2
        and row_count > 1
        and wave_count > 1
        and wave_count % 8 == 0
        and block_n % LANES == 0
        and total_n % (2 * LANES) == 0
        and block_n % (8 * wave_count) == 0
        and extra > 0
        and extra * row_count * part_count * (block_n // (8 * wave_count)) <= LANES
    )


def on_device(
    spin_tendency,
    spreading_source,
    heat_source,
    helmholtz_inverses,
    heat_spreading_coupler,
    smoothing_strengths,
    azimuthal_order_list,
):
    lev_count, wave_count = lax.axis_size("lev"), lax.axis_size("wave")
    lev_index = lax.axis_index("lev")
    lev_local, total_n = spreading_source.shape[2:]
    empty_placeholder = jnp.zeros((), jnp.bfloat16)
    if kernel_fits(spreading_source.shape, lev_count, wave_count):
        return by_kernel(
            spin_tendency, spreading_source, heat_source, helmholtz_inverses,
            heat_spreading_coupler, smoothing_strengths, azimuthal_order_list,
        )
    spreading_updated, coupled_out = exchange_by_collectives(
        spreading_source, helmholtz_inverses, heat_spreading_coupler
    )
    heat_updated = (heat_source.astype(jnp.float32) - coupled_out.astype(jnp.float32)).astype(
        jnp.bfloat16
    )
    level_gain = lax.dynamic_slice_in_dim(smoothing_strengths, lev_index * lev_local, lev_local)
    damping = damping_table(level_gain, jnp.arange(total_n, dtype=jnp.int32), total_n)
    spin_updated = (spin_tendency.astype(jnp.float32) * damping[None, None]).astype(jnp.bfloat16)
    interior_slice = (
        jnp.arange(total_n, dtype=jnp.int32)[None, :] >= azimuthal_order_list[:, None]
    )[:, None, None, :]
    return (
        jnp.where(interior_slice, spin_updated, empty_placeholder),
        jnp.where(interior_slice, spreading_updated, empty_placeholder),
        jnp.where(interior_slice, heat_updated, empty_placeholder),
    )


def solution(mesh):
    return jax.shard_map(
        on_device,
        mesh=mesh,
        in_specs=(
            P("wave", None, "lev", None),
            P("wave", None, "lev", None),
            P("wave", None, "lev", None),
            P("lev", "wave", None, None),
            P(),
            P(),
            P("wave"),
        ),
        out_specs=(
            P("wave", None, "lev", None),
            P("wave", None, "lev", None),
            P("wave", None, "lev", None),
        ),
        check_vma=False,
    )
```

```python
import functools
import jax
import jax.numpy as jnp
from jax import lax
from jax.experimental import pallas as pl
from jax.experimental.pallas import tpu as pltpu
from jax.sharding import PartitionSpec as P

LANES = 128
MESH = pl.DeviceIdType.MESH
NN = (((1,), (0,)), ((), ()))
NT = (((1,), (1,)), ((), ()))


def damping_table(level_gain, wavenumbers, total_n):
    scaled = (wavenumbers * (wavenumbers + 1)).astype(jnp.float32) / jnp.float32(
        (total_n - 1) * total_n
    )
    return 1.0 / (1.0 + level_gain[:, None] * scaled[None, :] ** 2)


def exchange_by_collectives(spreading_source, helmholtz_inverses, heat_spreading_coupler):
    lev_count = lax.axis_size("lev")
    row_count, part_count, lev_local, total_n = spreading_source.shape
    block_n = total_n // lev_count
    layer_count = lev_local * lev_count
    flat_rows = row_count * part_count
    wave_count = lax.axis_size("wave")
    local_n = block_n // wave_count
    rhs_div = lax.all_to_all(spreading_source, "lev", split_axis=3, concat_axis=2, tiled=True)
    outgoing = rhs_div.reshape(flat_rows, layer_count, wave_count, local_n).transpose(2, 3, 0, 1)
    outgoing = outgoing.reshape(wave_count, local_n, flat_rows * layer_count)
    columns = lax.all_to_all(outgoing, "wave", split_axis=0, concat_axis=0, tiled=True)
    columns = columns.reshape(wave_count, local_n, flat_rows, layer_count)
    solved_columns = jnp.einsum(
        "jkp,wjcp->wjck", helmholtz_inverses[0], columns, preferred_element_type=jnp.float32
    ).astype(jnp.bfloat16)
    solved_columns = solved_columns.reshape(wave_count, local_n, flat_rows * layer_count)
    returned = lax.all_to_all(solved_columns, "wave", split_axis=0, concat_axis=0, tiled=True)
    answer_fields = returned.reshape(block_n, flat_rows, layer_count).transpose(1, 2, 0)
    coupled = jnp.einsum(
        "om,dms->dos", heat_spreading_coupler, answer_fields, preferred_element_type=jnp.float32
    ).astype(jnp.bfloat16)
    both = jnp.stack([answer_fields, coupled])
    both = lax.all_to_all(both, "lev", split_axis=2, concat_axis=3, tiled=True)
    both = both.reshape(2, row_count, part_count, lev_local, total_n)
    spreading_updated, coupled_out = both[0], both[1]
    return spreading_updated, coupled_out


def f32_dot(left, right, dims):
    return lax.dot_general(left, right, dims, preferred_element_type=jnp.float32)


def grid_of(shape, axis):
    return lax.broadcasted_iota(jnp.int32, shape, axis)


def ones_where(condition, dtype=jnp.bfloat16):
    return jnp.where(condition, 1.0, 0.0).astype(dtype)


def flipped(value, mask):
    out, bit = value, 1
    while bit <= mask:
        if mask & bit:
            out = out + bit * (1 - 2 * lax.rem(lax.div(value, bit), 2))
        bit *= 2
    return out


def step_kernel(
    wave_count, lev_count, spin, source, heat, matrices, coupler, strengths, orders,
    vort_out, div_out, temp_out,
    spin_in, source_in, heat_in, mats_in, coupler_in, strengths_in, orders_in,
    first_out, next_out, first_in, next_in, gathered, rest_in, tables, strided, rest_out,
    weights, back_out, back_in, relayed,
    load_sem, fwd_send, fwd_recv, back_send, back_recv, relay_send, relay_recv,
):
    wave, lev = lax.axis_index("wave"), lax.axis_index("lev")
    row_count, lev_local, part_count, total_n = source.shape
    block_n = total_n // lev_count
    local_n = block_n // wave_count
    groups = local_n // 8
    layer_count = lev_local * lev_count
    fields = lev_local * part_count
    half = LANES // part_count
    short = lev_local - half
    extra = layer_count - LANES
    depth = tables.shape[1]
    sources = wave_count * lev_count
    wide = 2 * LANES
    cells = [(h, g) for h in range(2) for g in range(groups)]
    fwd_step = row_count * part_count * short
    back_step = part_count * extra
    rest_step = row_count * part_count * extra

    loads = []
    small = [(matrices, mats_in), (coupler, coupler_in), (strengths, strengths_in),
             (orders, orders_in), (spin, spin_in), (heat, heat_in)]
    for i, (src, dst) in enumerate(
        [(source.at[r], source_in.at[r]) for r in range(row_count)] + small
    ):
        copy = pltpu.make_async_copy(src, dst, load_sem.at[i])
        copy.start()
        loads.append(copy)
    source_loads, loads = loads[:row_count], loads[row_count:]

    peer = [flipped(wave, mask) for mask in range(wave_count)]
    other = lax.rem(lev + 1, lev_count)
    far_first = range(wave_count - 1, -1, -1)
    barrier = pltpu.get_barrier_semaphore()
    for mask in far_first:
        for t, q in enumerate((lev, other)):
            if mask or t:
                pl.semaphore_signal(
                    barrier, inc=1, device_id=(peer[mask], q), device_id_type=MESH
                )

    out_row, in_row = grid_of((wide, fields), 0), grid_of((wide, fields), 1)
    level, part = in_row // part_count, in_row % part_count
    main_spot = lax.rem(part + lev, part_count) * half + level
    main_pick = ones_where(
        (out_row == main_spot)[:LANES] & (level < half)[:LANES]
    )
    rest_picks = [
        ones_where(
            (out_row == (r * part_count + part) * short + level - half)[:LANES]
            & (level >= half)[:LANES]
        )
        for r in range(row_count)
    ]
    eye = ones_where(grid_of((wide, wide), 0) == grid_of((wide, wide), 1))
    flat = source_in.reshape(row_count, fields, total_n)
    mine = lev * wave_count + wave

    def turn(rows):
        return jnp.concatenate(
            [f32_dot(eye, rows[:, k:k + wide], NT) for k in range(0, total_n, wide)], axis=0
        )

    def by_rows(ref):
        return ref.reshape(*ref.shape[:-3], ref.shape[-3] * 2, LANES)

    outgoing, incoming = [first_out, next_out], [first_in, next_in]
    fwd = []

    def send(r):
        fwd.append([])
        for mask in far_first:
            for t, q in enumerate((lev, other)):
                if not (mask or t):
                    continue
                copy = pltpu.make_async_remote_copy(
                    src_ref=outgoing[r].at[q * wave_count + peer[mask]],
                    dst_ref=incoming[r].at[mine],
                    send_sem=fwd_send.at[r, mask, t], recv_sem=fwd_recv.at[r, mask, t],
                    device_id=(peer[mask], q), device_id_type=MESH,
                )
                copy.start()
                fwd[r].append(copy)
        incoming[r][mine] = outgoing[r][mine]

    for copy in source_loads:
        copy.wait()
    main = f32_dot(main_pick, flat[0], NN)
    rest = f32_dot(rest_picks[0], flat[0], NN)
    for r in range(1, row_count):
        rest += f32_dot(rest_picks[r], flat[r], NN)
    turned = turn(jnp.concatenate([main, rest], axis=0).astype(jnp.bfloat16))
    tail = turned[:, LANES:].reshape(sources, groups, 8, LANES)
    folded = tail[:, 0].reshape(sources * 8, LANES)
    for g in range(1, groups):
        folded += pltpu.roll(tail[:, g].reshape(sources * 8, LANES), g * fwd_step, 1)
    swung = pltpu.roll(folded, half, 1).reshape(sources, 8, LANES)
    folded = folded.reshape(sources, 8, LANES)[:, :4] + swung[:, 4:]
    by_rows(first_out)[:, :local_n] = (
        turned[:, :LANES].reshape(sources, local_n, LANES).astype(jnp.bfloat16)
    )
    by_rows(first_out)[:, local_n:] = folded.astype(jnp.bfloat16)
    pl.semaphore_wait(barrier, sources - 1)
    send(0)
    for r in range(1, row_count):
        turned = turn(f32_dot(main_pick, flat[r], NN).astype(jnp.bfloat16))
        by_rows(next_out)[...] = turned.reshape(sources, local_n, LANES).astype(jnp.bfloat16)
        send(r)

    loads[0].wait()
    deep, flat_level = grid_of((depth, layer_count), 0), grid_of((depth, layer_count), 1)
    owner, place = flat_level // lev_local, flat_level % lev_local
    spot = jnp.where(place < half, owner * half + place, LANES + owner * short + place - half)
    ordered = ones_where(deep == spot)
    zeros = jnp.zeros((depth, LANES - extra), jnp.float32)

    def prepare(t, carry):
        for h, g in cells:
            j = g * 8 + h * 4 + t
            turned = f32_dot(ordered, mats_in[j], NT)
            last = jnp.concatenate([turned[:, LANES:], zeros], axis=1)
            shift = h * half + g * back_step
            if shift:
                last = pltpu.roll(last, shift, 1)
            tables[j] = jnp.concatenate([turned[:, :LANES], last], axis=1).astype(jnp.bfloat16)
        return carry

    lax.fori_loop(0, 4, prepare, 0)

    come, go = grid_of((lev_count * LANES, wide), 0), grid_of((lev_count * LANES, wide), 1)
    p, lane = come // LANES, come % LANES
    h, lane = lane // half, lane % half
    g, lane = lane // fwd_step, lane % fwd_step
    target = h * LANES + g * rest_step + lane // short * extra + p * short + lane % short
    spread = ones_where((go == target) & (g < groups))

    loads[1].wait()
    row, col = grid_of((fields, layer_count), 0), grid_of((fields, layer_count), 1)
    chosen = ones_where(col == lev * lev_local + row // part_count)
    coupled_rows = f32_dot(chosen, coupler_in[...], NN)
    tops = jnp.concatenate([chosen.astype(jnp.float32), coupled_rows], axis=0)
    tops_part = lax.rem(grid_of(tops.shape, 0), part_count)
    keeps = [jnp.where(tops_part == c, tops, 0.0) for c in range(part_count)]
    pieces = [k[:, :LANES] for k in keeps] + [k[:, LANES:] for k in keeps]
    pieces.append(jnp.zeros((2 * fields, LANES - part_count * extra), jnp.float32))
    weights[...] = jnp.concatenate(pieces, axis=1).astype(jnp.bfloat16)

    for copy in loads[2:5]:
        copy.wait()
    gain = jnp.sum(
        jnp.where(col == lev * lev_local + row // part_count, strengths_in[...], 0.0),
        axis=1, keepdims=True,
    )
    n = grid_of((1, total_n), 1)
    scaled = (n * (n + 1)).astype(jnp.float32) / jnp.float32((total_n - 1) * total_n)
    damping = 1.0 / (1.0 + gain * scaled ** 2)
    spin_flat = spin_in.reshape(row_count, fields, total_n)
    vort_flat = vort_out.reshape(row_count, fields, total_n)
    for r in range(row_count):
        value = (spin_flat[r].astype(jnp.float32) * damping)
        value = jnp.where(n >= orders_in[:, r:r + 1], value, 0.0)
        vort_flat[r] = value.astype(jnp.bfloat16)

    lane = grid_of((wave_count, LANES), 1)
    back = []

    def solve_chunk(r):
        rows_in = by_rows(incoming[r])
        for q in range(lev_count):
            main = rows_in[pl.ds(q * wave_count, wave_count), :local_n]
            gathered[q] = main.astype(jnp.float32).reshape(block_n, LANES)
        if r == 0:
            rests = [
                rows_in[pl.ds(q * wave_count, wave_count), local_n:]
                .astype(jnp.float32).reshape(wave_count * 4, LANES)
                for q in range(lev_count)
            ]
            value = jnp.concatenate(rests, axis=1).astype(jnp.bfloat16)
            value = f32_dot(value, spread, NN)
            for h in range(2):
                rest_in[h] = value[:, h * LANES:(h + 1) * LANES]

        def solve(t, carry):
            every = pl.ds(t, wave_count, stride=4)
            lasts = None
            for h, g in cells:
                j = g * 8 + h * 4 + t
                rest = rest_in[h, every, :]
                rows = pl.ds(j, wave_count, stride=local_n)
                low, high = gathered[0, rows, :], gathered[1, rows, :]
                sides = [jnp.where(lane < half, low, high),
                         pltpu.roll(jnp.where(lane < half, high, low), half, 1)]
                stacked = []
                for c in range(part_count):
                    shift = g * rest_step + (r * part_count + c) * extra
                    moved = pltpu.roll(rest, LANES - shift, 1) if shift else rest
                    stacked.append(jnp.concatenate([sides[c], moved], axis=1)[:, :depth])
                stacked = jnp.concatenate(stacked, axis=0).astype(jnp.bfloat16)
                result = f32_dot(stacked, tables[j], NN)
                for c in range(part_count):
                    strided[c, rows, :] = result[c * wave_count:(c + 1) * wave_count, :LANES]
                last = result[:, LANES:]
                lasts = last if lasts is None else lasts + last
            total = lasts[:wave_count]
            for c in range(1, part_count):
                total += pltpu.roll(lasts[c * wave_count:(c + 1) * wave_count], c * extra, 1)
            rest_out[every, :] = total
            return carry

        lax.fori_loop(0, 4, solve, 0)
        rows_out = by_rows(back_out)
        for c in range(part_count):
            rows_out[r, :, c * local_n:(c + 1) * local_n] = (
                strided[c].reshape(wave_count, local_n, LANES).astype(jnp.bfloat16)
            )
        rows_out[r, :, part_count * local_n:] = (
            rest_out[...].reshape(wave_count, 4, LANES).astype(jnp.bfloat16)
        )
        back.append({})
        for mask in far_first[:-1]:
            copy = pltpu.make_async_remote_copy(
                src_ref=back_out.at[r, peer[mask]], dst_ref=back_in.at[r, wave],
                send_sem=back_send.at[r, mask], recv_sem=back_recv.at[r, mask],
                device_id=(peer[mask], lev), device_id_type=MESH,
            )
            copy.start()
            back[r][mask] = copy
        back_in[r, wave] = back_out[r, wave]

    relays = [[] for _ in range(row_count)]

    def relay(r, masks):
        for mask in masks:
            if mask:
                back[r][mask].wait_recv()
            copy = pltpu.make_async_remote_copy(
                src_ref=(back_in if mask else back_out).at[r, peer[mask]],
                dst_ref=relayed.at[r, peer[mask]],
                send_sem=relay_send.at[r, mask], recv_sem=relay_recv.at[r, mask],
                device_id=(wave, other), device_id_type=MESH,
            )
            copy.start()
            relays[r].append(copy)

    heat_flat = heat_in.reshape(row_count, fields, total_n)
    div_flat = div_out.reshape(row_count, fields, total_n)
    temp_flat = temp_out.reshape(row_count, fields, total_n)

    def finish(r, wire, block):
        rows_in = by_rows(wire)
        sides = [
            rows_in[r, :, c * local_n:(c + 1) * local_n].astype(jnp.float32).reshape(block_n, LANES)
            for c in range(part_count)
        ]
        folded = rows_in[r, :, part_count * local_n:].astype(jnp.float32)
        swung = pltpu.roll(folded.reshape(wave_count * 4, LANES), half, 1)
        folded = jnp.concatenate([folded, swung.reshape(wave_count, 4, LANES)], axis=1)
        folded = folded.reshape(wave_count * 8, LANES)
        rest = [(pltpu.roll(folded, LANES - g * back_step, 1) if g else folded)
                .reshape(wave_count, 1, 8, LANES) for g in range(groups)]
        sides.append(jnp.concatenate(rest, axis=1).reshape(block_n, LANES))
        packed = jnp.concatenate(sides, axis=1).astype(jnp.bfloat16)
        result = f32_dot(weights[...], packed, NT)
        spots = pl.ds(pl.multiple_of(block * block_n, LANES), block_n)
        inside = block * block_n + grid_of((1, block_n), 1) >= orders_in[:, r:r + 1]
        div_flat[r, :, spots] = jnp.where(inside, result[:fields], 0.0).astype(jnp.bfloat16)
        coupled = result[fields:].astype(jnp.bfloat16).astype(jnp.float32)
        warmed = heat_flat[r, :, spots].astype(jnp.float32) - coupled
        temp_flat[r, :, spots] = jnp.where(inside, warmed, 0.0).astype(jnp.bfloat16)

    loads[5].wait()
    near, mid, far = range(4), range(4, wave_count // 2), range(wave_count // 2, wave_count)
    for r in range(row_count):
        for copy in fwd[r]:
            copy.wait_recv()
        solve_chunk(r)
        relay(r, near)
    for copy in (c for group in fwd for c in group):
        copy.wait_send()
    relay(0, mid)
    relay(0, far)
    relay(1, mid)
    finish(0, back_in, lev)
    relay(1, far)
    finish(1, back_in, lev)
    for group in back:
        for copy in group.values():
            copy.wait_send()
    for copy in relays[0]:
        copy.wait_send()
        copy.wait_recv()
    finish(0, relayed, other)
    for copy in relays[1]:
        copy.wait_send()
        copy.wait_recv()
    finish(1, relayed, other)


def store_kernel(*refs):
    count = (len(refs) - 1) // 2
    copies = [
        pltpu.make_async_copy(refs[i], refs[count + i], refs[-1].at[i]) for i in range(count)
    ]
    for copy in copies:
        copy.start()
    for copy in copies:
        copy.wait()


def by_kernel(spin, source, heat, matrices, coupler, strengths, orders):
    lev_count, wave_count = lax.axis_size("lev"), lax.axis_size("wave")
    row_count, part_count, lev_local, total_n = source.shape
    block_n = total_n // lev_count
    local_n = block_n // wave_count
    layer_count = lev_local * lev_count
    fields = lev_local * part_count
    sources = wave_count * lev_count
    depth = -(-layer_count // 16) * 16
    anywhere, vmem = pl.BlockSpec(memory_space=pltpu.HBM), pl.BlockSpec(memory_space=pltpu.VMEM)
    shape = (row_count, lev_local, part_count, total_n)
    bf16, f32 = jnp.bfloat16, jnp.float32
    field = jax.ShapeDtypeStruct(shape, bf16)
    dma = pltpu.SemaphoreType.DMA
    main_pairs, rest_pairs = local_n // 2, 2
    wire = pltpu.VMEM((row_count, wave_count, part_count * main_pairs + rest_pairs, 2, LANES), bf16)
    first = pltpu.VMEM((sources, main_pairs + rest_pairs, 2, LANES), bf16)
    following = pltpu.VMEM((sources, main_pairs, 2, LANES), bf16)
    fwd_sems, back_sems = dma((row_count, wave_count, lev_count)), dma((row_count, wave_count))
    outs = pl.pallas_call(
        functools.partial(step_kernel, wave_count, lev_count),
        out_shape=(field,) * 3,
        in_specs=[anywhere] * 7,
        out_specs=(vmem,) * 3,
        scratch_shapes=[
            pltpu.VMEM(shape, bf16), pltpu.VMEM(shape, bf16), pltpu.VMEM(shape, bf16),
            pltpu.VMEM(matrices.shape[1:], bf16), pltpu.VMEM(coupler.shape, bf16),
            pltpu.VMEM((1, layer_count), f32), pltpu.VMEM((1, row_count), jnp.int32),
            first, following, first, following,
            pltpu.VMEM((lev_count, block_n, LANES), f32),
            pltpu.VMEM((2, wave_count * 4, LANES), f32),
            pltpu.VMEM((local_n, depth, 2 * LANES), bf16),
            pltpu.VMEM((part_count, block_n, LANES), f32),
            pltpu.VMEM((wave_count * 4, LANES), f32),
            pltpu.VMEM((2 * fields, 3 * LANES), bf16),
            wire, wire, wire,
            dma((row_count + 6,)),
            fwd_sems, fwd_sems, back_sems, back_sems, back_sems, back_sems,
        ],
        compiler_params=pltpu.CompilerParams(
            collective_id=0, has_side_effects=True, vmem_limit_bytes=48 * 2**20
        ),
    )(
        *(
            pltpu.with_memory_space_constraint(value, pltpu.HBM)
            for value in (
                spin.transpose(0, 2, 1, 3), source.transpose(0, 2, 1, 3), heat.transpose(0, 2, 1, 3),
                matrices[0], coupler, strengths.reshape(1, layer_count), orders.reshape(1, row_count),
            )
        )
    )
    outs = pl.pallas_call(
        store_kernel, out_shape=(field,) * 3, in_specs=[vmem] * 3, out_specs=(anywhere,) * 3,
        scratch_shapes=[dma((3,))],
        compiler_params=pltpu.CompilerParams(vmem_limit_bytes=4 * 2**20),
    )(*outs)
    return tuple(out.transpose(0, 2, 1, 3) for out in outs)


def kernel_fits(source_shape, lev_count, wave_count):
    row_count, part_count, lev_local, total_n = source_shape
    block_n = total_n // lev_count
    extra = lev_local * lev_count - LANES
    half = LANES // 2
    groups = block_n // (8 * wave_count)
    return (
        lev_count == 2
        and part_count == 2
        and row_count == 2
        and wave_count > 8
        and wave_count & (wave_count - 1) == 0
        and wave_count % 8 == 0
        and block_n % LANES == 0
        and total_n % (2 * LANES) == 0
        and block_n % (8 * wave_count) == 0
        and extra > 0
        and extra * row_count * part_count * groups <= LANES
        and (lev_local - half) * row_count * part_count * groups <= half
        and extra * part_count * groups <= half
    )


def on_device(
    spin_tendency,
    spreading_source,
    heat_source,
    helmholtz_inverses,
    heat_spreading_coupler,
    smoothing_strengths,
    azimuthal_order_list,
):
    lev_count, wave_count = lax.axis_size("lev"), lax.axis_size("wave")
    lev_index = lax.axis_index("lev")
    lev_local, total_n = spreading_source.shape[2:]
    empty_placeholder = jnp.zeros((), jnp.bfloat16)
    if kernel_fits(spreading_source.shape, lev_count, wave_count):
        return by_kernel(
            spin_tendency, spreading_source, heat_source, helmholtz_inverses,
            heat_spreading_coupler, smoothing_strengths, azimuthal_order_list,
        )
    spreading_updated, coupled_out = exchange_by_collectives(
        spreading_source, helmholtz_inverses, heat_spreading_coupler
    )
    heat_updated = (heat_source.astype(jnp.float32) - coupled_out.astype(jnp.float32)).astype(
        jnp.bfloat16
    )
    level_gain = lax.dynamic_slice_in_dim(smoothing_strengths, lev_index * lev_local, lev_local)
    damping = damping_table(level_gain, jnp.arange(total_n, dtype=jnp.int32), total_n)
    spin_updated = (spin_tendency.astype(jnp.float32) * damping[None, None]).astype(jnp.bfloat16)
    interior_slice = (
        jnp.arange(total_n, dtype=jnp.int32)[None, :] >= azimuthal_order_list[:, None]
    )[:, None, None, :]
    return (
        jnp.where(interior_slice, spin_updated, empty_placeholder),
        jnp.where(interior_slice, spreading_updated, empty_placeholder),
        jnp.where(interior_slice, heat_updated, empty_placeholder),
    )


def solution(mesh):
    return jax.shard_map(
        on_device,
        mesh=mesh,
        in_specs=(
            P("wave", None, "lev", None),
            P("wave", None, "lev", None),
            P("wave", None, "lev", None),
            P("lev", "wave", None, None),
            P(),
            P(),
            P("wave"),
        ),
        out_specs=(
            P("wave", None, "lev", None),
            P("wave", None, "lev", None),
            P("wave", None, "lev", None),
        ),
        check_vma=False,
    )
```

```python
import functools
import jax
import jax.numpy as jnp
from jax import lax
from jax.experimental import pallas as pl
from jax.experimental.pallas import tpu as pltpu
from jax.sharding import PartitionSpec as P

LANES = 128
MESH = pl.DeviceIdType.MESH
NN = (((1,), (0,)), ((), ()))
NT = (((1,), (1,)), ((), ()))


def damping_table(level_gain, wavenumbers, total_n):
    scaled = (wavenumbers * (wavenumbers + 1)).astype(jnp.float32) / jnp.float32(
        (total_n - 1) * total_n
    )
    return 1.0 / (1.0 + level_gain[:, None] * scaled[None, :] ** 2)


def exchange_by_collectives(spreading_source, helmholtz_inverses, heat_spreading_coupler):
    lev_count = lax.axis_size("lev")
    row_count, part_count, lev_local, total_n = spreading_source.shape
    block_n = total_n // lev_count
    layer_count = lev_local * lev_count
    flat_rows = row_count * part_count
    wave_count = lax.axis_size("wave")
    local_n = block_n // wave_count
    rhs_div = lax.all_to_all(spreading_source, "lev", split_axis=3, concat_axis=2, tiled=True)
    outgoing = rhs_div.reshape(flat_rows, layer_count, wave_count, local_n).transpose(2, 3, 0, 1)
    outgoing = outgoing.reshape(wave_count, local_n, flat_rows * layer_count)
    columns = lax.all_to_all(outgoing, "wave", split_axis=0, concat_axis=0, tiled=True)
    columns = columns.reshape(wave_count, local_n, flat_rows, layer_count)
    solved_columns = jnp.einsum(
        "jkp,wjcp->wjck", helmholtz_inverses[0], columns, preferred_element_type=jnp.float32
    ).astype(jnp.bfloat16)
    solved_columns = solved_columns.reshape(wave_count, local_n, flat_rows * layer_count)
    returned = lax.all_to_all(solved_columns, "wave", split_axis=0, concat_axis=0, tiled=True)
    answer_fields = returned.reshape(block_n, flat_rows, layer_count).transpose(1, 2, 0)
    coupled = jnp.einsum(
        "om,dms->dos", heat_spreading_coupler, answer_fields, preferred_element_type=jnp.float32
    ).astype(jnp.bfloat16)
    both = jnp.stack([answer_fields, coupled])
    both = lax.all_to_all(both, "lev", split_axis=2, concat_axis=3, tiled=True)
    both = both.reshape(2, row_count, part_count, lev_local, total_n)
    spreading_updated, coupled_out = both[0], both[1]
    return spreading_updated, coupled_out


def f32_dot(left, right, dims):
    return lax.dot_general(left, right, dims, preferred_element_type=jnp.float32)


def grid_of(shape, axis):
    return lax.broadcasted_iota(jnp.int32, shape, axis)


def ones_where(condition, dtype=jnp.bfloat16):
    return jnp.where(condition, 1.0, 0.0).astype(dtype)


def flipped(value, mask):
    out, bit = value, 1
    while bit <= mask:
        if mask & bit:
            out = out + bit * (1 - 2 * lax.rem(lax.div(value, bit), 2))
        bit *= 2
    return out


def step_kernel(
    wave_count, lev_count, spin, source, heat, matrices, coupler, strengths, orders,
    vort_out, div_out, temp_out,
    spin_in, source_in, heat_in, mats_in, coupler_in, strengths_in, orders_in,
    first_out, next_out, first_in, next_in, gathered, rest_in, tables, strided, rest_out,
    weights, back_out, back_in, relayed,
    load_sem, fwd_send, fwd_recv, back_send, back_recv, relay_send, relay_recv,
):
    wave, lev = lax.axis_index("wave"), lax.axis_index("lev")
    row_count, lev_local, part_count, total_n = source.shape
    block_n = total_n // lev_count
    local_n = block_n // wave_count
    groups = local_n // 8
    layer_count = lev_local * lev_count
    fields = lev_local * part_count
    half = LANES // part_count
    short = lev_local - half
    extra = layer_count - LANES
    depth = tables.shape[1]
    sources = wave_count * lev_count
    wide = 2 * LANES
    cells = [(h, g) for h in range(2) for g in range(groups)]
    fwd_step = row_count * part_count * short
    back_step = part_count * extra
    rest_step = row_count * part_count * extra

    loads = []
    small = [(matrices, mats_in), (coupler, coupler_in), (strengths, strengths_in),
             (orders, orders_in), (spin, spin_in), (heat, heat_in)]
    for i, (src, dst) in enumerate(
        [(source, source_in), *small]
    ):
        copy = pltpu.make_async_copy(src, dst, load_sem.at[i])
        copy.start()
        loads.append(copy)
    source_load, loads = loads[0], loads[1:]

    peer = [flipped(wave, mask) for mask in range(wave_count)]
    other = lax.rem(lev + 1, lev_count)
    outward = [*range(1, wave_count), 0]
    barrier = pltpu.get_barrier_semaphore()
    for mask in outward:
        for t, q in enumerate((lev, other)):
            if mask or t:
                pl.semaphore_signal(
                    barrier, inc=1, device_id=(peer[mask], q), device_id_type=MESH
                )

    out_row, in_row = grid_of((wide, fields), 0), grid_of((wide, fields), 1)
    level, part = in_row // part_count, in_row % part_count
    main_spot = lax.rem(part + lev, part_count) * half + level
    main_pick = ones_where(
        (out_row == main_spot)[:LANES] & (level < half)[:LANES]
    )
    rest_picks = [
        ones_where(
            (out_row == (r * part_count + part) * short + level - half)[:LANES]
            & (level >= half)[:LANES]
        )
        for r in range(row_count)
    ]
    eye = ones_where(grid_of((wide, wide), 0) == grid_of((wide, wide), 1))
    flat = source_in.reshape(row_count, fields, total_n)
    mine = lev * wave_count + wave

    def turn(rows):
        return jnp.concatenate(
            [f32_dot(eye, rows[:, k:k + wide], NT) for k in range(0, total_n, wide)], axis=0
        )

    def by_rows(ref):
        return ref.reshape(*ref.shape[:-3], ref.shape[-3] * 2, LANES)

    outgoing, incoming = [first_out, next_out], [first_in, next_in]

    def await_bytes(ref, sem):
        pltpu.make_async_copy(ref, ref, sem).wait()

    def send(r):
        for mask in outward:
            for t, q in enumerate((lev, other)):
                if not (mask or t):
                    continue
                copy = pltpu.make_async_remote_copy(
                    src_ref=outgoing[r].at[q * wave_count + peer[mask]],
                    dst_ref=incoming[r].at[mine],
                    send_sem=fwd_send.at[r], recv_sem=fwd_recv.at[r],
                    device_id=(peer[mask], q), device_id_type=MESH,
                )
                copy.start()
        incoming[r][mine] = outgoing[r][mine]

    source_load.wait()
    main = f32_dot(main_pick, flat[0], NN)
    rest = f32_dot(rest_picks[0], flat[0], NN)
    for r in range(1, row_count):
        rest += f32_dot(rest_picks[r], flat[r], NN)
    turned = turn(jnp.concatenate([main, rest], axis=0).astype(jnp.bfloat16))
    tail = turned[:, LANES:].reshape(sources, groups, 8, LANES)
    folded = tail[:, 0].reshape(sources * 8, LANES)
    for g in range(1, groups):
        folded += pltpu.roll(tail[:, g].reshape(sources * 8, LANES), g * fwd_step, 1)
    swung = pltpu.roll(folded, half, 1).reshape(sources, 8, LANES)
    folded = folded.reshape(sources, 8, LANES)[:, :4] + swung[:, 4:]
    by_rows(first_out)[:, :local_n] = (
        turned[:, :LANES].reshape(sources, local_n, LANES).astype(jnp.bfloat16)
    )
    by_rows(first_out)[:, local_n:] = folded.astype(jnp.bfloat16)
    pl.semaphore_wait(barrier, sources - 1)
    send(0)
    for r in range(1, row_count):
        turned = turn(f32_dot(main_pick, flat[r], NN).astype(jnp.bfloat16))
        by_rows(next_out)[...] = turned.reshape(sources, local_n, LANES).astype(jnp.bfloat16)
        send(r)

    loads[0].wait()
    deep, flat_level = grid_of((depth, layer_count), 0), grid_of((depth, layer_count), 1)
    owner, place = flat_level // lev_local, flat_level % lev_local
    spot = jnp.where(place < half, owner * half + place, LANES + owner * short + place - half)
    ordered = ones_where(deep == spot)
    zeros = jnp.zeros((depth, LANES - extra), jnp.float32)

    def prepare(t, carry):
        for h, g in cells:
            j = g * 8 + h * 4 + t
            turned = f32_dot(ordered, mats_in[j], NT)
            last = jnp.concatenate([turned[:, LANES:], zeros], axis=1)
            shift = h * half + g * back_step
            if shift:
                last = pltpu.roll(last, shift, 1)
            tables[j] = jnp.concatenate([turned[:, :LANES], last], axis=1).astype(jnp.bfloat16)
        return carry

    lax.fori_loop(0, 4, prepare, 0)

    come, go = grid_of((lev_count * LANES, wide), 0), grid_of((lev_count * LANES, wide), 1)
    p, lane = come // LANES, come % LANES
    h, lane = lane // half, lane % half
    g, lane = lane // fwd_step, lane % fwd_step
    target = h * LANES + g * rest_step + lane // short * extra + p * short + lane % short
    spread = ones_where((go == target) & (g < groups))

    loads[1].wait()
    row, col = grid_of((fields, layer_count), 0), grid_of((fields, layer_count), 1)
    chosen = ones_where(col == lev * lev_local + row // part_count)
    coupled_rows = f32_dot(chosen, coupler_in[...], NN)
    tops = jnp.concatenate([chosen.astype(jnp.float32), coupled_rows], axis=0)
    tops_part = lax.rem(grid_of(tops.shape, 0), part_count)
    keeps = [jnp.where(tops_part == c, tops, 0.0) for c in range(part_count)]
    pieces = [k[:, :LANES] for k in keeps] + [k[:, LANES:] for k in keeps]
    pieces.append(jnp.zeros((2 * fields, LANES - part_count * extra), jnp.float32))
    weights[...] = jnp.concatenate(pieces, axis=1).astype(jnp.bfloat16)

    for copy in loads[2:5]:
        copy.wait()
    gain = jnp.sum(
        jnp.where(col == lev * lev_local + row // part_count, strengths_in[...], 0.0),
        axis=1, keepdims=True,
    )
    n = grid_of((1, total_n), 1)
    scaled = (n * (n + 1)).astype(jnp.float32) / jnp.float32((total_n - 1) * total_n)
    damping = 1.0 / (1.0 + gain * scaled ** 2)
    spin_flat = spin_in.reshape(row_count, fields, total_n)
    vort_flat = vort_out.reshape(row_count, fields, total_n)
    for r in range(row_count):
        value = (spin_flat[r].astype(jnp.float32) * damping)
        value = jnp.where(n >= orders_in[:, r:r + 1], value, 0.0)
        vort_flat[r] = value.astype(jnp.bfloat16)

    lane = grid_of((wave_count, LANES), 1)
    cuts = [1, 4, 8, 12, 16] if wave_count == 16 else [1, 4, 8, wave_count]
    parties = [range(a, b) for a, b in zip(cuts, cuts[1:])]
    group_of = {mask: i for i, party in enumerate(parties) for mask in party}

    def solve_chunk(r):
        rows_in = by_rows(incoming[r])
        for q in range(lev_count):
            main = rows_in[pl.ds(q * wave_count, wave_count), :local_n]
            gathered[q] = main.astype(jnp.float32).reshape(block_n, LANES)
        if r == 0:
            rests = [
                rows_in[pl.ds(q * wave_count, wave_count), local_n:]
                .astype(jnp.float32).reshape(wave_count * 4, LANES)
                for q in range(lev_count)
            ]
            value = jnp.concatenate(rests, axis=1).astype(jnp.bfloat16)
            value = f32_dot(value, spread, NN)
            for h in range(2):
                rest_in[h] = value[:, h * LANES:(h + 1) * LANES]

        def solve(t, carry):
            every = pl.ds(t, wave_count, stride=4)
            lasts = None
            for h, g in cells:
                j = g * 8 + h * 4 + t
                rest = rest_in[h, every, :]
                rows = pl.ds(j, wave_count, stride=local_n)
                low, high = gathered[0, rows, :], gathered[1, rows, :]
                sides = [jnp.where(lane < half, low, high),
                         pltpu.roll(jnp.where(lane < half, high, low), half, 1)]
                stacked = []
                for c in range(part_count):
                    shift = g * rest_step + (r * part_count + c) * extra
                    moved = pltpu.roll(rest, LANES - shift, 1) if shift else rest
                    stacked.append(jnp.concatenate([sides[c], moved], axis=1)[:, :depth])
                stacked = jnp.concatenate(stacked, axis=0).astype(jnp.bfloat16)
                result = f32_dot(stacked, tables[j], NN)
                for c in range(part_count):
                    strided[c, rows, :] = result[c * wave_count:(c + 1) * wave_count, :LANES]
                last = result[:, LANES:]
                lasts = last if lasts is None else lasts + last
            total = lasts[:wave_count]
            for c in range(1, part_count):
                total += pltpu.roll(lasts[c * wave_count:(c + 1) * wave_count], c * extra, 1)
            rest_out[every, :] = total
            return carry

        lax.fori_loop(0, 4, solve, 0)
        rows_out = by_rows(back_out)
        for c in range(part_count):
            rows_out[r, :, c * local_n:(c + 1) * local_n] = (
                strided[c].reshape(wave_count, local_n, LANES).astype(jnp.bfloat16)
            )
        rows_out[r, :, part_count * local_n:] = (
            rest_out[...].reshape(wave_count, 4, LANES).astype(jnp.bfloat16)
        )
        for mask in outward[:-1]:
            copy = pltpu.make_async_remote_copy(
                src_ref=back_out.at[r, peer[mask]], dst_ref=back_in.at[r, wave],
                send_sem=back_send.at[r], recv_sem=back_recv.at[r, group_of[mask]],
                device_id=(peer[mask], lev), device_id_type=MESH,
            )
            copy.start()
        back_in[r, wave] = back_out[r, wave]

    def relay(r, masks):
        if masks[0]:
            await_bytes(back_in.at[r, pl.ds(0, len(masks))], back_recv.at[r, group_of[masks[0]]])
        for mask in masks:
            pltpu.make_async_remote_copy(
                src_ref=(back_in if mask else back_out).at[r, peer[mask]],
                dst_ref=relayed.at[r, peer[mask]],
                send_sem=relay_send.at[r], recv_sem=relay_recv.at[r],
                device_id=(wave, other), device_id_type=MESH,
            ).start()

    heat_flat = heat_in.reshape(row_count, fields, total_n)
    div_flat = div_out.reshape(row_count, fields, total_n)
    temp_flat = temp_out.reshape(row_count, fields, total_n)

    def finish(r, wire, block):
        rows_in = by_rows(wire)
        sides = [
            rows_in[r, :, c * local_n:(c + 1) * local_n].astype(jnp.float32).reshape(block_n, LANES)
            for c in range(part_count)
        ]
        folded = rows_in[r, :, part_count * local_n:].astype(jnp.float32)
        swung = pltpu.roll(folded.reshape(wave_count * 4, LANES), half, 1)
        folded = jnp.concatenate([folded, swung.reshape(wave_count, 4, LANES)], axis=1)
        folded = folded.reshape(wave_count * 8, LANES)
        rest = [(pltpu.roll(folded, LANES - g * back_step, 1) if g else folded)
                .reshape(wave_count, 1, 8, LANES) for g in range(groups)]
        sides.append(jnp.concatenate(rest, axis=1).reshape(block_n, LANES))
        packed = jnp.concatenate(sides, axis=1).astype(jnp.bfloat16)
        result = f32_dot(weights[...], packed, NT)
        spots = pl.ds(pl.multiple_of(block * block_n, LANES), block_n)
        inside = block * block_n + grid_of((1, block_n), 1) >= orders_in[:, r:r + 1]
        div_flat[r, :, spots] = jnp.where(inside, result[:fields], 0.0).astype(jnp.bfloat16)
        coupled = result[fields:].astype(jnp.bfloat16).astype(jnp.float32)
        warmed = heat_flat[r, :, spots].astype(jnp.float32) - coupled
        temp_flat[r, :, spots] = jnp.where(inside, warmed, 0.0).astype(jnp.bfloat16)

    loads[5].wait()
    for r in range(row_count):
        await_bytes(incoming[r].at[pl.ds(0, sources - 1)], fwd_recv.at[r])
        solve_chunk(r)
        relay(r, [0])
    lagging, leading = list(parties), list(parties)
    relay(0, lagging.pop(0))
    relay(0, lagging.pop(0))
    while lagging:
        relay(0, lagging.pop(0))
        relay(1, leading.pop(0))
    for r in range(row_count):
        await_bytes(outgoing[r].at[pl.ds(0, sources - 1)], fwd_send.at[r])
    finish(0, back_in, lev)
    while leading:
        relay(1, leading.pop(0))
    finish(1, back_in, lev)
    for r in range(row_count):
        await_bytes(back_out.at[r, pl.ds(0, wave_count - 1)], back_send.at[r])
    for r in range(row_count):
        await_bytes(relayed.at[r], relay_recv.at[r])
        finish(r, relayed, other)
    for r in range(row_count):
        await_bytes(relayed.at[r], relay_send.at[r])


def store_kernel(*refs):
    count = (len(refs) - 1) // 2
    copies = [
        pltpu.make_async_copy(refs[i], refs[count + i], refs[-1].at[i]) for i in range(count)
    ]
    for copy in copies:
        copy.start()
    for copy in copies:
        copy.wait()


def by_kernel(spin, source, heat, matrices, coupler, strengths, orders):
    lev_count, wave_count = lax.axis_size("lev"), lax.axis_size("wave")
    row_count, part_count, lev_local, total_n = source.shape
    block_n = total_n // lev_count
    local_n = block_n // wave_count
    layer_count = lev_local * lev_count
    fields = lev_local * part_count
    sources = wave_count * lev_count
    depth = -(-layer_count // 16) * 16
    anywhere, vmem = pl.BlockSpec(memory_space=pltpu.HBM), pl.BlockSpec(memory_space=pltpu.VMEM)
    shape = (row_count, lev_local, part_count, total_n)
    bf16, f32 = jnp.bfloat16, jnp.float32
    field = jax.ShapeDtypeStruct(shape, bf16)
    dma = pltpu.SemaphoreType.DMA
    main_pairs, rest_pairs = local_n // 2, 2
    wire = pltpu.VMEM((row_count, wave_count, part_count * main_pairs + rest_pairs, 2, LANES), bf16)
    first = pltpu.VMEM((sources, main_pairs + rest_pairs, 2, LANES), bf16)
    following = pltpu.VMEM((sources, main_pairs, 2, LANES), bf16)
    each = dma((row_count,))
    outs = pl.pallas_call(
        functools.partial(step_kernel, wave_count, lev_count),
        out_shape=(field,) * 3,
        in_specs=[anywhere] * 7,
        out_specs=(vmem,) * 3,
        scratch_shapes=[
            pltpu.VMEM(shape, bf16), pltpu.VMEM(shape, bf16), pltpu.VMEM(shape, bf16),
            pltpu.VMEM(matrices.shape[1:], bf16), pltpu.VMEM(coupler.shape, bf16),
            pltpu.VMEM((1, layer_count), f32), pltpu.VMEM((1, row_count), jnp.int32),
            first, following, first, following,
            pltpu.VMEM((lev_count, block_n, LANES), f32),
            pltpu.VMEM((2, wave_count * 4, LANES), f32),
            pltpu.VMEM((local_n, depth, 2 * LANES), bf16),
            pltpu.VMEM((part_count, block_n, LANES), f32),
            pltpu.VMEM((wave_count * 4, LANES), f32),
            pltpu.VMEM((2 * fields, 3 * LANES), bf16),
            wire, wire, wire,
            dma((7,)), each, each, each, dma((row_count, 4)), each, each,
        ],
        compiler_params=pltpu.CompilerParams(
            collective_id=0, has_side_effects=True, vmem_limit_bytes=48 * 2**20
        ),
    )(
        *(
            pltpu.with_memory_space_constraint(value, pltpu.HBM)
            for value in (
                spin.transpose(0, 2, 1, 3), source.transpose(0, 2, 1, 3), heat.transpose(0, 2, 1, 3),
                matrices[0], coupler, strengths.reshape(1, layer_count), orders.reshape(1, row_count),
            )
        )
    )
    outs = pl.pallas_call(
        store_kernel, out_shape=(field,) * 3, in_specs=[vmem] * 3, out_specs=(anywhere,) * 3,
        scratch_shapes=[dma((3,))],
        compiler_params=pltpu.CompilerParams(vmem_limit_bytes=4 * 2**20),
    )(*outs)
    return tuple(out.transpose(0, 2, 1, 3) for out in outs)


def kernel_fits(source_shape, lev_count, wave_count):
    row_count, part_count, lev_local, total_n = source_shape
    block_n = total_n // lev_count
    extra = lev_local * lev_count - LANES
    half = LANES // 2
    groups = block_n // (8 * wave_count)
    return (
        lev_count == 2
        and part_count == 2
        and row_count == 2
        and wave_count > 8
        and wave_count & (wave_count - 1) == 0
        and wave_count % 8 == 0
        and block_n % LANES == 0
        and total_n % (2 * LANES) == 0
        and block_n % (8 * wave_count) == 0
        and extra > 0
        and extra * row_count * part_count * groups <= LANES
        and (lev_local - half) * row_count * part_count * groups <= half
        and extra * part_count * groups <= half
    )


def on_device(
    spin_tendency,
    spreading_source,
    heat_source,
    helmholtz_inverses,
    heat_spreading_coupler,
    smoothing_strengths,
    azimuthal_order_list,
):
    lev_count, wave_count = lax.axis_size("lev"), lax.axis_size("wave")
    lev_index = lax.axis_index("lev")
    lev_local, total_n = spreading_source.shape[2:]
    empty_placeholder = jnp.zeros((), jnp.bfloat16)
    if kernel_fits(spreading_source.shape, lev_count, wave_count):
        return by_kernel(
            spin_tendency, spreading_source, heat_source, helmholtz_inverses,
            heat_spreading_coupler, smoothing_strengths, azimuthal_order_list,
        )
    spreading_updated, coupled_out = exchange_by_collectives(
        spreading_source, helmholtz_inverses, heat_spreading_coupler
    )
    heat_updated = (heat_source.astype(jnp.float32) - coupled_out.astype(jnp.float32)).astype(
        jnp.bfloat16
    )
    level_gain = lax.dynamic_slice_in_dim(smoothing_strengths, lev_index * lev_local, lev_local)
    damping = damping_table(level_gain, jnp.arange(total_n, dtype=jnp.int32), total_n)
    spin_updated = (spin_tendency.astype(jnp.float32) * damping[None, None]).astype(jnp.bfloat16)
    interior_slice = (
        jnp.arange(total_n, dtype=jnp.int32)[None, :] >= azimuthal_order_list[:, None]
    )[:, None, None, :]
    return (
        jnp.where(interior_slice, spin_updated, empty_placeholder),
        jnp.where(interior_slice, spreading_updated, empty_placeholder),
        jnp.where(interior_slice, heat_updated, empty_placeholder),
    )


def solution(mesh):
    return jax.shard_map(
        on_device,
        mesh=mesh,
        in_specs=(
            P("wave", None, "lev", None),
            P("wave", None, "lev", None),
            P("wave", None, "lev", None),
            P("lev", "wave", None, None),
            P(),
            P(),
            P("wave"),
        ),
        out_specs=(
            P("wave", None, "lev", None),
            P("wave", None, "lev", None),
            P("wave", None, "lev", None),
        ),
        check_vma=False,
    )
```

```python
import functools
import jax
import jax.numpy as jnp
from jax import lax
from jax.experimental import pallas as pl
from jax.experimental.pallas import tpu as pltpu
from jax.sharding import PartitionSpec as P

LANES = 128
MESH = pl.DeviceIdType.MESH
NN = (((1,), (0,)), ((), ()))
NT = (((1,), (1,)), ((), ()))


def damping_table(level_gain, wavenumbers, total_n):
    scaled = (wavenumbers * (wavenumbers + 1)).astype(jnp.float32) / jnp.float32(
        (total_n - 1) * total_n
    )
    return 1.0 / (1.0 + level_gain[:, None] * scaled[None, :] ** 2)


def exchange_by_collectives(spreading_source, helmholtz_inverses, heat_spreading_coupler):
    lev_count = lax.axis_size("lev")
    row_count, part_count, lev_local, total_n = spreading_source.shape
    block_n = total_n // lev_count
    layer_count = lev_local * lev_count
    flat_rows = row_count * part_count
    wave_count = lax.axis_size("wave")
    local_n = block_n // wave_count
    rhs_div = lax.all_to_all(spreading_source, "lev", split_axis=3, concat_axis=2, tiled=True)
    outgoing = rhs_div.reshape(flat_rows, layer_count, wave_count, local_n).transpose(2, 3, 0, 1)
    outgoing = outgoing.reshape(wave_count, local_n, flat_rows * layer_count)
    columns = lax.all_to_all(outgoing, "wave", split_axis=0, concat_axis=0, tiled=True)
    columns = columns.reshape(wave_count, local_n, flat_rows, layer_count)
    solved_columns = jnp.einsum(
        "jkp,wjcp->wjck", helmholtz_inverses[0], columns, preferred_element_type=jnp.float32
    ).astype(jnp.bfloat16)
    solved_columns = solved_columns.reshape(wave_count, local_n, flat_rows * layer_count)
    returned = lax.all_to_all(solved_columns, "wave", split_axis=0, concat_axis=0, tiled=True)
    answer_fields = returned.reshape(block_n, flat_rows, layer_count).transpose(1, 2, 0)
    coupled = jnp.einsum(
        "om,dms->dos", heat_spreading_coupler, answer_fields, preferred_element_type=jnp.float32
    ).astype(jnp.bfloat16)
    both = jnp.stack([answer_fields, coupled])
    both = lax.all_to_all(both, "lev", split_axis=2, concat_axis=3, tiled=True)
    both = both.reshape(2, row_count, part_count, lev_local, total_n)
    spreading_updated, coupled_out = both[0], both[1]
    return spreading_updated, coupled_out


def f32_dot(left, right, dims):
    return lax.dot_general(left, right, dims, preferred_element_type=jnp.float32)


def grid_of(shape, axis):
    return lax.broadcasted_iota(jnp.int32, shape, axis)


def ones_where(condition, dtype=jnp.bfloat16):
    return jnp.where(condition, 1.0, 0.0).astype(dtype)


def flipped(value, mask):
    out, bit = value, 1
    while bit <= mask:
        if mask & bit:
            out = out + bit * (1 - 2 * lax.rem(lax.div(value, bit), 2))
        bit *= 2
    return out


def step_kernel(
    wave_count, lev_count, spin, source, heat, matrices, coupler, strengths, orders,
    vort_out, div_out, temp_out,
    spin_in, source_in, heat_in, mats_in, coupler_in, strengths_in, orders_in,
    first_out, next_out, first_in, next_in, gathered, rest_in, tables, strided, rest_out,
    weights, back_out, back_in, relayed,
    load_sem, fwd_send, fwd_recv, back_send, back_recv, relay_send, relay_recv,
):
    wave, lev = lax.axis_index("wave"), lax.axis_index("lev")
    row_count, lev_local, part_count, total_n = source.shape
    block_n = total_n // lev_count
    local_n = block_n // wave_count
    groups = local_n // 8
    layer_count = lev_local * lev_count
    fields = lev_local * part_count
    half = LANES // part_count
    short = lev_local - half
    extra = layer_count - LANES
    depth = tables.shape[1]
    sources = wave_count * lev_count
    wide = 2 * LANES
    cells = [(h, g) for h in range(2) for g in range(groups)]
    fwd_step = row_count * part_count * short
    back_step = part_count * extra
    rest_step = row_count * part_count * extra

    loads = []
    small = [(matrices, mats_in), (coupler, coupler_in), (strengths, strengths_in),
             (orders, orders_in), (spin, spin_in), (heat, heat_in)]
    for i, (src, dst) in enumerate(
        [(source, source_in), *small]
    ):
        copy = pltpu.make_async_copy(src, dst, load_sem.at[i])
        copy.start()
        loads.append(copy)
    source_load, loads = loads[0], loads[1:]

    middle = wave_count // 2
    block = lax.rem(wave, 4)
    across = middle * (1 - lax.div(wave, middle))
    flips = [flipped(wave, mask) for mask in range(wave_count)]
    peer = flips[:middle]
    peer += [across + i // 4 * 4 + flipped(block, i % 4) for i in range(middle)]
    rank = [*range(middle), *(lax.div(lax.rem(wave, middle), 4) * 4 + i % 4 for i in range(middle))]
    other = lax.rem(lev + 1, lev_count)
    outward = [*range(1, wave_count), 0]
    barrier = pltpu.get_barrier_semaphore()
    for mask in reversed(range(wave_count)):
        for t, q in enumerate((lev, other)):
            if mask or t:
                pl.semaphore_signal(
                    barrier, inc=1, device_id=(peer[mask], q), device_id_type=MESH
                )

    out_row, in_row = grid_of((wide, fields), 0), grid_of((wide, fields), 1)
    level, part = in_row // part_count, in_row % part_count
    main_spot = lax.rem(part + lev, part_count) * half + level
    main_pick = ones_where(
        (out_row == main_spot)[:LANES] & (level < half)[:LANES]
    )
    rest_picks = [
        ones_where(
            (out_row == (r * part_count + part) * short + level - half)[:LANES]
            & (level >= half)[:LANES]
        )
        for r in range(row_count)
    ]
    eye = ones_where(grid_of((wide, wide), 0) == grid_of((wide, wide), 1))
    flat = source_in.reshape(row_count, fields, total_n)
    mine = lev * wave_count + wave

    def turn(rows):
        return jnp.concatenate(
            [f32_dot(eye, rows[:, k:k + wide], NT) for k in range(0, total_n, wide)], axis=0
        )

    def by_rows(ref):
        return ref.reshape(*ref.shape[:-3], ref.shape[-3] * 2, LANES)

    outgoing, incoming = [first_out, next_out], [first_in, next_in]

    def await_bytes(ref, sem):
        pltpu.make_async_copy(ref, ref, sem).wait()

    def send(r, masks):
        for mask in masks:
            for t, q in enumerate((lev, other)):
                if not (mask or t):
                    continue
                copy = pltpu.make_async_remote_copy(
                    src_ref=outgoing[r].at[q * wave_count + flips[mask]],
                    dst_ref=incoming[r].at[mine],
                    send_sem=fwd_send.at[r], recv_sem=fwd_recv.at[r],
                    device_id=(flips[mask], q), device_id_type=MESH,
                )
                copy.start()

    source_load.wait()
    main = f32_dot(main_pick, flat[0], NN)
    rest = f32_dot(rest_picks[0], flat[0], NN)
    for r in range(1, row_count):
        rest += f32_dot(rest_picks[r], flat[r], NN)
    turned = turn(jnp.concatenate([main, rest], axis=0).astype(jnp.bfloat16))
    tail = turned[:, LANES:].reshape(sources, groups, 8, LANES)
    folded = tail[:, 0].reshape(sources * 8, LANES)
    for g in range(1, groups):
        folded += pltpu.roll(tail[:, g].reshape(sources * 8, LANES), g * fwd_step, 1)
    swung = pltpu.roll(folded, half, 1).reshape(sources, 8, LANES)
    folded = folded.reshape(sources, 8, LANES)[:, :4] + swung[:, 4:]
    by_rows(first_out)[:, :local_n] = (
        turned[:, :LANES].reshape(sources, local_n, LANES).astype(jnp.bfloat16)
    )
    by_rows(first_out)[:, local_n:] = folded.astype(jnp.bfloat16)
    pl.semaphore_wait(barrier, sources - 1)
    send(0, outward)
    incoming[0][mine] = outgoing[0][mine]
    for r in range(1, row_count):
        turned = turn(f32_dot(main_pick, flat[r], NN).astype(jnp.bfloat16))
        by_rows(next_out)[...] = turned.reshape(sources, local_n, LANES).astype(jnp.bfloat16)
        send(r, range(middle))
        incoming[r][mine] = outgoing[r][mine]

    loads[0].wait()
    deep, flat_level = grid_of((depth, layer_count), 0), grid_of((depth, layer_count), 1)
    owner, place = flat_level // lev_local, flat_level % lev_local
    spot = jnp.where(place < half, owner * half + place, LANES + owner * short + place - half)
    ordered = ones_where(deep == spot)
    zeros = jnp.zeros((depth, LANES - extra), jnp.float32)

    def prepare(t, carry):
        for h, g in cells:
            j = g * 8 + h * 4 + t
            turned = f32_dot(ordered, mats_in[j], NT)
            last = jnp.concatenate([turned[:, LANES:], zeros], axis=1)
            shift = h * half + g * back_step
            if shift:
                last = pltpu.roll(last, shift, 1)
            tables[j] = jnp.concatenate([turned[:, :LANES], last], axis=1).astype(jnp.bfloat16)
        return carry

    lax.fori_loop(0, 4, prepare, 0)

    come, go = grid_of((lev_count * LANES, wide), 0), grid_of((lev_count * LANES, wide), 1)
    p, lane = come // LANES, come % LANES
    h, lane = lane // half, lane % half
    g, lane = lane // fwd_step, lane % fwd_step
    target = h * LANES + g * rest_step + lane // short * extra + p * short + lane % short
    spread = ones_where((go == target) & (g < groups))

    loads[1].wait()
    row, col = grid_of((fields, layer_count), 0), grid_of((fields, layer_count), 1)
    chosen = ones_where(col == lev * lev_local + row // part_count)
    coupled_rows = f32_dot(chosen, coupler_in[...], NN)
    tops = jnp.concatenate([chosen.astype(jnp.float32), coupled_rows], axis=0)
    tops_part = lax.rem(grid_of(tops.shape, 0), part_count)
    keeps = [jnp.where(tops_part == c, tops, 0.0) for c in range(part_count)]
    pieces = [k[:, :LANES] for k in keeps] + [k[:, LANES:] for k in keeps]
    pieces.append(jnp.zeros((2 * fields, LANES - part_count * extra), jnp.float32))
    weights[...] = jnp.concatenate(pieces, axis=1).astype(jnp.bfloat16)

    for copy in loads[2:5]:
        copy.wait()
    gain = jnp.sum(
        jnp.where(col == lev * lev_local + row // part_count, strengths_in[...], 0.0),
        axis=1, keepdims=True,
    )
    n = grid_of((1, total_n), 1)
    scaled = (n * (n + 1)).astype(jnp.float32) / jnp.float32((total_n - 1) * total_n)
    damping = 1.0 / (1.0 + gain * scaled ** 2)
    spin_flat = spin_in.reshape(row_count, fields, total_n)
    vort_flat = vort_out.reshape(row_count, fields, total_n)
    for r in range(row_count):
        value = (spin_flat[r].astype(jnp.float32) * damping)
        value = jnp.where(n >= orders_in[:, r:r + 1], value, 0.0)
        vort_flat[r] = value.astype(jnp.bfloat16)

    send(1, range(middle, wave_count))

    lane = grid_of((wave_count, LANES), 1)
    parties = [range(1, 4), *([i] for i in range(4, wave_count))]
    group_of = {i: g for g, party in enumerate(parties) for i in party}

    def hand_over(ref, r, spot, target):
        pltpu.make_async_remote_copy(
            src_ref=ref, dst_ref=relayed.at[r, spot],
            send_sem=relay_send.at[r], recv_sem=relay_recv.at[r],
            device_id=(target, other), device_id_type=MESH,
        ).start()

    def give_back(r, masks):
        for mask in masks:
            copy = pltpu.make_async_remote_copy(
                src_ref=back_out.at[r, peer[mask]], dst_ref=back_in.at[r, wave],
                send_sem=back_send.at[r], recv_sem=back_recv.at[
                    r, group_of[mask] if mask < middle else group_of[middle] + rank[mask]
                ],
                device_id=(peer[mask], lev), device_id_type=MESH,
            )
            copy.start()
            if mask in parties[0]:
                hand_over(back_out.at[r, peer[mask]], r, wave, peer[mask])

    def relay(r, masks):
        if masks[0]:
            await_bytes(back_in.at[r, pl.ds(0, len(masks))], back_recv.at[r, group_of[masks[0]]])
        for mask in masks:
            hand_over((back_in if mask else back_out).at[r, peer[mask]], r, peer[mask], wave)

    def solve_chunk(r):
        rows_in = by_rows(incoming[r])
        for q in range(lev_count):
            main = rows_in[pl.ds(q * wave_count, wave_count), :local_n]
            gathered[q] = main.astype(jnp.float32).reshape(block_n, LANES)
        if r == 0:
            rests = [
                rows_in[pl.ds(q * wave_count, wave_count), local_n:]
                .astype(jnp.float32).reshape(wave_count * 4, LANES)
                for q in range(lev_count)
            ]
            value = jnp.concatenate(rests, axis=1).astype(jnp.bfloat16)
            value = f32_dot(value, spread, NN)
            for h in range(2):
                rest_in[h] = value[:, h * LANES:(h + 1) * LANES]

        def solve(t, carry):
            every = pl.ds(t, wave_count, stride=4)
            lasts = None
            for h, g in cells:
                j = g * 8 + h * 4 + t
                rest = rest_in[h, every, :]
                rows = pl.ds(j, wave_count, stride=local_n)
                low, high = gathered[0, rows, :], gathered[1, rows, :]
                sides = [jnp.where(lane < half, low, high),
                         pltpu.roll(jnp.where(lane < half, high, low), half, 1)]
                stacked = []
                for c in range(part_count):
                    shift = g * rest_step + (r * part_count + c) * extra
                    moved = pltpu.roll(rest, LANES - shift, 1) if shift else rest
                    stacked.append(jnp.concatenate([sides[c], moved], axis=1)[:, :depth])
                stacked = jnp.concatenate(stacked, axis=0).astype(jnp.bfloat16)
                result = f32_dot(stacked, tables[j], NN)
                for c in range(part_count):
                    strided[c, rows, :] = result[c * wave_count:(c + 1) * wave_count, :LANES]
                last = result[:, LANES:]
                lasts = last if lasts is None else lasts + last
            total = lasts[:wave_count]
            for c in range(1, part_count):
                total += pltpu.roll(lasts[c * wave_count:(c + 1) * wave_count], c * extra, 1)
            rest_out[every, :] = total
            return carry

        lax.fori_loop(0, 4, solve, 0, unroll=4)
        rows_out = by_rows(back_out)
        for c in range(part_count):
            rows_out[r, :, c * local_n:(c + 1) * local_n] = (
                strided[c].reshape(wave_count, local_n, LANES).astype(jnp.bfloat16)
            )
        rows_out[r, :, part_count * local_n:] = (
            rest_out[...].reshape(wave_count, 4, LANES).astype(jnp.bfloat16)
        )
        relay(r, [0])
        give_back(r, range(1, wave_count if r == 0 else middle + 4))
        back_in[r, wave] = back_out[r, wave]

    heat_flat = heat_in.reshape(row_count, fields, total_n)
    div_flat = div_out.reshape(row_count, fields, total_n)
    temp_flat = temp_out.reshape(row_count, fields, total_n)

    def finish(r, wire, block):
        rows_in = by_rows(wire)
        sides = [
            rows_in[r, :, c * local_n:(c + 1) * local_n].astype(jnp.float32).reshape(block_n, LANES)
            for c in range(part_count)
        ]
        folded = rows_in[r, :, part_count * local_n:].astype(jnp.float32)
        swung = pltpu.roll(folded.reshape(wave_count * 4, LANES), half, 1)
        folded = jnp.concatenate([folded, swung.reshape(wave_count, 4, LANES)], axis=1)
        folded = folded.reshape(wave_count * 8, LANES)
        rest = [(pltpu.roll(folded, LANES - g * back_step, 1) if g else folded)
                .reshape(wave_count, 1, 8, LANES) for g in range(groups)]
        sides.append(jnp.concatenate(rest, axis=1).reshape(block_n, LANES))
        packed = jnp.concatenate(sides, axis=1).astype(jnp.bfloat16)
        result = f32_dot(weights[...], packed, NT)
        spots = pl.ds(pl.multiple_of(block * block_n, LANES), block_n)
        inside = block * block_n + grid_of((1, block_n), 1) >= orders_in[:, r:r + 1]
        div_flat[r, :, spots] = jnp.where(inside, result[:fields], 0.0).astype(jnp.bfloat16)
        coupled = result[fields:].astype(jnp.bfloat16).astype(jnp.float32)
        warmed = heat_flat[r, :, spots].astype(jnp.float32) - coupled
        temp_flat[r, :, spots] = jnp.where(inside, warmed, 0.0).astype(jnp.bfloat16)

    loads[5].wait()
    for r in range(row_count):
        await_bytes(incoming[r].at[pl.ds(0, sources - 1)], fwd_recv.at[r])
        solve_chunk(r)
    for party in parties[1:]:
        relay(0, party)
        place = party[0] - middle
        if place > 0 and place % 2 and middle + 4 + place // 2 < wave_count:
            give_back(1, [middle + 4 + place // 2])
    for r in range(row_count):
        await_bytes(outgoing[r].at[pl.ds(0, sources - 1)], fwd_send.at[r])
    await_bytes(back_in.at[0, pl.ds(0, len(parties[0]))], back_recv.at[0, 0])
    finish(0, back_in, lev)
    for party in parties[1:]:
        relay(1, party)
    await_bytes(back_in.at[1, pl.ds(0, len(parties[0]))], back_recv.at[1, 0])
    finish(1, back_in, lev)
    for r in range(row_count):
        await_bytes(back_out.at[r, pl.ds(0, wave_count - 1)], back_send.at[r])
    for r in range(row_count):
        await_bytes(relayed.at[r], relay_recv.at[r])
        finish(r, relayed, other)
    for r in range(row_count):
        await_bytes(relayed.at[r], relay_send.at[r])


def store_kernel(*refs):
    count = (len(refs) - 1) // 2
    copies = [
        pltpu.make_async_copy(refs[i], refs[count + i], refs[-1].at[i]) for i in range(count)
    ]
    for copy in copies:
        copy.start()
    for copy in copies:
        copy.wait()


def by_kernel(spin, source, heat, matrices, coupler, strengths, orders):
    lev_count, wave_count = lax.axis_size("lev"), lax.axis_size("wave")
    row_count, part_count, lev_local, total_n = source.shape
    block_n = total_n // lev_count
    local_n = block_n // wave_count
    layer_count = lev_local * lev_count
    fields = lev_local * part_count
    sources = wave_count * lev_count
    depth = -(-layer_count // 16) * 16
    anywhere, vmem = pl.BlockSpec(memory_space=pltpu.HBM), pl.BlockSpec(memory_space=pltpu.VMEM)
    shape = (row_count, lev_local, part_count, total_n)
    bf16, f32 = jnp.bfloat16, jnp.float32
    field = jax.ShapeDtypeStruct(shape, bf16)
    dma = pltpu.SemaphoreType.DMA
    main_pairs, rest_pairs = local_n // 2, 2
    wire = pltpu.VMEM((row_count, wave_count, part_count * main_pairs + rest_pairs, 2, LANES), bf16)
    first = pltpu.VMEM((sources, main_pairs + rest_pairs, 2, LANES), bf16)
    following = pltpu.VMEM((sources, main_pairs, 2, LANES), bf16)
    each = dma((row_count,))
    outs = pl.pallas_call(
        functools.partial(step_kernel, wave_count, lev_count),
        out_shape=(field,) * 3,
        in_specs=[anywhere] * 7,
        out_specs=(vmem,) * 3,
        scratch_shapes=[
            pltpu.VMEM(shape, bf16), pltpu.VMEM(shape, bf16), pltpu.VMEM(shape, bf16),
            pltpu.VMEM(matrices.shape[1:], bf16), pltpu.VMEM(coupler.shape, bf16),
            pltpu.VMEM((1, layer_count), f32), pltpu.VMEM((1, row_count), jnp.int32),
            first, following, first, following,
            pltpu.VMEM((lev_count, block_n, LANES), f32),
            pltpu.VMEM((2, wave_count * 4, LANES), f32),
            pltpu.VMEM((local_n, depth, 2 * LANES), bf16),
            pltpu.VMEM((part_count, block_n, LANES), f32),
            pltpu.VMEM((wave_count * 4, LANES), f32),
            pltpu.VMEM((2 * fields, 3 * LANES), bf16),
            wire, wire, wire,
            dma((7,)), each, each, each, dma((row_count, wave_count - 3)), each, each,
        ],
        compiler_params=pltpu.CompilerParams(
            collective_id=0, has_side_effects=True, vmem_limit_bytes=48 * 2**20
        ),
    )(
        *(
            pltpu.with_memory_space_constraint(value, pltpu.HBM)
            for value in (
                spin.transpose(0, 2, 1, 3), source.transpose(0, 2, 1, 3), heat.transpose(0, 2, 1, 3),
                matrices[0], coupler, strengths.reshape(1, layer_count), orders.reshape(1, row_count),
            )
        )
    )
    outs = pl.pallas_call(
        store_kernel, out_shape=(field,) * 3, in_specs=[vmem] * 3, out_specs=(anywhere,) * 3,
        scratch_shapes=[dma((3,))],
        compiler_params=pltpu.CompilerParams(vmem_limit_bytes=4 * 2**20),
    )(*outs)
    return tuple(out.transpose(0, 2, 1, 3) for out in outs)


def kernel_fits(source_shape, lev_count, wave_count):
    row_count, part_count, lev_local, total_n = source_shape
    block_n = total_n // lev_count
    extra = lev_local * lev_count - LANES
    half = LANES // 2
    groups = block_n // (8 * wave_count)
    return (
        lev_count == 2
        and part_count == 2
        and row_count == 2
        and wave_count > 8
        and wave_count & (wave_count - 1) == 0
        and wave_count % 8 == 0
        and block_n % LANES == 0
        and total_n % (2 * LANES) == 0
        and block_n % (8 * wave_count) == 0
        and extra > 0
        and extra * row_count * part_count * groups <= LANES
        and (lev_local - half) * row_count * part_count * groups <= half
        and extra * part_count * groups <= half
    )


def on_device(
    spin_tendency,
    spreading_source,
    heat_source,
    helmholtz_inverses,
    heat_spreading_coupler,
    smoothing_strengths,
    azimuthal_order_list,
):
    lev_count, wave_count = lax.axis_size("lev"), lax.axis_size("wave")
    lev_index = lax.axis_index("lev")
    lev_local, total_n = spreading_source.shape[2:]
    empty_placeholder = jnp.zeros((), jnp.bfloat16)
    if kernel_fits(spreading_source.shape, lev_count, wave_count):
        return by_kernel(
            spin_tendency, spreading_source, heat_source, helmholtz_inverses,
            heat_spreading_coupler, smoothing_strengths, azimuthal_order_list,
        )
    spreading_updated, coupled_out = exchange_by_collectives(
        spreading_source, helmholtz_inverses, heat_spreading_coupler
    )
    heat_updated = (heat_source.astype(jnp.float32) - coupled_out.astype(jnp.float32)).astype(
        jnp.bfloat16
    )
    level_gain = lax.dynamic_slice_in_dim(smoothing_strengths, lev_index * lev_local, lev_local)
    damping = damping_table(level_gain, jnp.arange(total_n, dtype=jnp.int32), total_n)
    spin_updated = (spin_tendency.astype(jnp.float32) * damping[None, None]).astype(jnp.bfloat16)
    interior_slice = (
        jnp.arange(total_n, dtype=jnp.int32)[None, :] >= azimuthal_order_list[:, None]
    )[:, None, None, :]
    return (
        jnp.where(interior_slice, spin_updated, empty_placeholder),
        jnp.where(interior_slice, spreading_updated, empty_placeholder),
        jnp.where(interior_slice, heat_updated, empty_placeholder),
    )


def solution(mesh):
    return jax.shard_map(
        on_device,
        mesh=mesh,
        in_specs=(
            P("wave", None, "lev", None),
            P("wave", None, "lev", None),
            P("wave", None, "lev", None),
            P("lev", "wave", None, None),
            P(),
            P(),
            P("wave"),
        ),
        out_specs=(
            P("wave", None, "lev", None),
            P("wave", None, "lev", None),
            P("wave", None, "lev", None),
        ),
        check_vma=False,
    )
```

```python
import functools
import jax
import jax.numpy as jnp
from jax import lax
from jax.experimental import pallas as pl
from jax.experimental.pallas import tpu as pltpu
from jax.sharding import PartitionSpec as P

LANES = 128
MESH = pl.DeviceIdType.MESH
NN = (((1,), (0,)), ((), ()))
NT = (((1,), (1,)), ((), ()))


def damping_table(level_gain, wavenumbers, total_n):
    scaled = (wavenumbers * (wavenumbers + 1)).astype(jnp.float32) / jnp.float32(
        (total_n - 1) * total_n
    )
    return 1.0 / (1.0 + level_gain[:, None] * scaled[None, :] ** 2)


def exchange_by_collectives(spreading_source, helmholtz_inverses, heat_spreading_coupler):
    lev_count = lax.axis_size("lev")
    row_count, part_count, lev_local, total_n = spreading_source.shape
    block_n = total_n // lev_count
    layer_count = lev_local * lev_count
    flat_rows = row_count * part_count
    wave_count = lax.axis_size("wave")
    local_n = block_n // wave_count
    rhs_div = lax.all_to_all(spreading_source, "lev", split_axis=3, concat_axis=2, tiled=True)
    outgoing = rhs_div.reshape(flat_rows, layer_count, wave_count, local_n).transpose(2, 3, 0, 1)
    outgoing = outgoing.reshape(wave_count, local_n, flat_rows * layer_count)
    columns = lax.all_to_all(outgoing, "wave", split_axis=0, concat_axis=0, tiled=True)
    columns = columns.reshape(wave_count, local_n, flat_rows, layer_count)
    solved_columns = jnp.einsum(
        "jkp,wjcp->wjck", helmholtz_inverses[0], columns, preferred_element_type=jnp.float32
    ).astype(jnp.bfloat16)
    solved_columns = solved_columns.reshape(wave_count, local_n, flat_rows * layer_count)
    returned = lax.all_to_all(solved_columns, "wave", split_axis=0, concat_axis=0, tiled=True)
    answer_fields = returned.reshape(block_n, flat_rows, layer_count).transpose(1, 2, 0)
    coupled = jnp.einsum(
        "om,dms->dos", heat_spreading_coupler, answer_fields, preferred_element_type=jnp.float32
    ).astype(jnp.bfloat16)
    both = jnp.stack([answer_fields, coupled])
    both = lax.all_to_all(both, "lev", split_axis=2, concat_axis=3, tiled=True)
    both = both.reshape(2, row_count, part_count, lev_local, total_n)
    spreading_updated, coupled_out = both[0], both[1]
    return spreading_updated, coupled_out


def f32_dot(left, right, dims):
    return lax.dot_general(left, right, dims, preferred_element_type=jnp.float32)


def grid_of(shape, axis):
    return lax.broadcasted_iota(jnp.int32, shape, axis)


def ones_where(condition, dtype=jnp.bfloat16):
    return jnp.where(condition, 1.0, 0.0).astype(dtype)


def flipped(value, mask):
    out, bit = value, 1
    while bit <= mask:
        if mask & bit:
            out = out + bit * (1 - 2 * lax.rem(lax.div(value, bit), 2))
        bit *= 2
    return out


def step_kernel(
    wave_count, lev_count, spin, source, heat, matrices, coupler, strengths, orders,
    vort_out, div_out, temp_out,
    spin_in, source_in, heat_in, mats_in, coupler_in, strengths_in, orders_in,
    first_out, next_out, first_in, next_in, first_lev, next_lev, gathered, rest_in, tables, strided, rest_out,
    weights, back_out, back_in, relayed,
    load_sem, fwd_send, fwd_recv, lev_recv, pass_send, back_send, back_recv, relay_send, relay_recv,
):
    wave, lev = lax.axis_index("wave"), lax.axis_index("lev")
    row_count, lev_local, part_count, total_n = source.shape
    block_n = total_n // lev_count
    local_n = block_n // wave_count
    groups = local_n // 8
    layer_count = lev_local * lev_count
    fields = lev_local * part_count
    half = LANES // part_count
    short = lev_local - half
    extra = layer_count - LANES
    depth = tables.shape[1]
    sources = wave_count * lev_count
    wide = 2 * LANES
    cells = [(h, g) for h in range(2) for g in range(groups)]
    fwd_step = row_count * part_count * short
    back_step = part_count * extra
    rest_step = row_count * part_count * extra

    loads = []
    small = [(matrices, mats_in), (coupler, coupler_in), (strengths, strengths_in),
             (orders, orders_in), (spin, spin_in), (heat, heat_in)]
    for i, (src, dst) in enumerate(
        [(source, source_in), *small]
    ):
        copy = pltpu.make_async_copy(src, dst, load_sem.at[i])
        copy.start()
        loads.append(copy)
    source_load, loads = loads[0], loads[1:]

    middle = wave_count // 2
    block = lax.rem(wave, 4)
    across = middle * (1 - lax.div(wave, middle))
    flips = [flipped(wave, mask) for mask in range(wave_count)]
    peer = flips[:middle]
    peer += [across + i // 4 * 4 + flipped(block, i % 4) for i in range(middle)]
    rank = [*range(middle), *(lax.div(lax.rem(wave, middle), 4) * 4 + i % 4 for i in range(middle))]
    other = lax.rem(lev + 1, lev_count)
    outward = [*range(1, wave_count), 0]
    barrier = pltpu.get_barrier_semaphore()
    for mask in reversed(range(wave_count)):
        for t, q in enumerate((lev, other)):
            if mask or t:
                pl.semaphore_signal(
                    barrier, inc=1, device_id=(peer[mask], q), device_id_type=MESH
                )

    out_row, in_row = grid_of((wide, fields), 0), grid_of((wide, fields), 1)
    level, part = in_row // part_count, in_row % part_count
    main_spot = lax.rem(part + lev, part_count) * half + level
    main_pick = ones_where(
        (out_row == main_spot)[:LANES] & (level < half)[:LANES]
    )
    rest_picks = [
        ones_where(
            (out_row == (r * part_count + part) * short + level - half)[:LANES]
            & (level >= half)[:LANES]
        )
        for r in range(row_count)
    ]
    eye = ones_where(grid_of((wide, wide), 0) == grid_of((wide, wide), 1))
    flat = source_in.reshape(row_count, fields, total_n)
    mine = lev * wave_count + wave

    def turn(rows):
        return jnp.concatenate(
            [f32_dot(eye, rows[:, k:k + wide], NT) for k in range(0, total_n, wide)], axis=0
        )

    def by_rows(ref):
        return ref.reshape(*ref.shape[:-3], ref.shape[-3] * 2, LANES)

    outgoing, incoming = [first_out, next_out], [first_in, next_in]

    def await_bytes(ref, sem):
        pltpu.make_async_copy(ref, ref, sem).wait()

    crossing = [first_lev, next_lev]
    home = middle - across
    planes = [across + i for i in range(0, middle, 4)]
    planes += [home + lax.rem(lax.rem(wave - block - home, middle) + i, middle)
               for i in range(4, middle, 4)]
    planes += [wave - block]

    def cross(r):
        for i, plane in enumerate(planes):
            pltpu.make_async_remote_copy(
                src_ref=outgoing[r].at[pl.ds(other * wave_count + plane, 4)],
                dst_ref=crossing[r].at[pl.ds(plane, 4)],
                send_sem=fwd_send.at[r], recv_sem=lev_recv.at[r, i],
                device_id=(wave, other), device_id_type=MESH,
            ).start()

    def send(r, masks):
        for mask in masks:
            pltpu.make_async_remote_copy(
                src_ref=outgoing[r].at[lev * wave_count + flips[mask]],
                dst_ref=incoming[r].at[mine],
                send_sem=fwd_send.at[r], recv_sem=fwd_recv.at[r],
                device_id=(flips[mask], lev), device_id_type=MESH,
            ).start()

    def pass_on(r, which):
        for i in which:
            plane = planes[i]
            await_bytes(crossing[r].at[pl.ds(0, 4)], lev_recv.at[r, i])
            last = i == len(planes) - 1
            for k in range(1 if last else 0, 4):
                target = plane + flipped(block, k)
                pltpu.make_async_remote_copy(
                    src_ref=crossing[r].at[target],
                    dst_ref=incoming[r].at[other * wave_count + wave],
                    send_sem=pass_send.at[r], recv_sem=fwd_recv.at[r],
                    device_id=(target, lev), device_id_type=MESH,
                ).start()
            if last:
                incoming[r][other * wave_count + wave] = crossing[r][wave]

    source_load.wait()
    main = f32_dot(main_pick, flat[0], NN)
    rest = f32_dot(rest_picks[0], flat[0], NN)
    for r in range(1, row_count):
        rest += f32_dot(rest_picks[r], flat[r], NN)
    turned = turn(jnp.concatenate([main, rest], axis=0).astype(jnp.bfloat16))
    tail = turned[:, LANES:].reshape(sources, groups, 8, LANES)
    folded = tail[:, 0].reshape(sources * 8, LANES)
    for g in range(1, groups):
        folded += pltpu.roll(tail[:, g].reshape(sources * 8, LANES), g * fwd_step, 1)
    swung = pltpu.roll(folded, half, 1).reshape(sources, 8, LANES)
    folded = folded.reshape(sources, 8, LANES)[:, :4] + swung[:, 4:]
    by_rows(first_out)[:, :local_n] = (
        turned[:, :LANES].reshape(sources, local_n, LANES).astype(jnp.bfloat16)
    )
    by_rows(first_out)[:, local_n:] = folded.astype(jnp.bfloat16)
    pl.semaphore_wait(barrier, sources - 1)
    cross(0)
    send(0, range(1, wave_count))
    incoming[0][mine] = outgoing[0][mine]
    for r in range(1, row_count):
        turned = turn(f32_dot(main_pick, flat[r], NN).astype(jnp.bfloat16))
        by_rows(next_out)[...] = turned.reshape(sources, local_n, LANES).astype(jnp.bfloat16)
        send(r, range(1, middle))
        incoming[r][mine] = outgoing[r][mine]

    loads[0].wait()
    deep, flat_level = grid_of((depth, layer_count), 0), grid_of((depth, layer_count), 1)
    owner, place = flat_level // lev_local, flat_level % lev_local
    spot = jnp.where(place < half, owner * half + place, LANES + owner * short + place - half)
    ordered = ones_where(deep == spot)
    zeros = jnp.zeros((depth, LANES - extra), jnp.float32)

    def prepare(t, carry):
        for h, g in cells:
            j = g * 8 + h * 4 + t
            turned = f32_dot(ordered, mats_in[j], NT)
            last = jnp.concatenate([turned[:, LANES:], zeros], axis=1)
            shift = h * half + g * back_step
            if shift:
                last = pltpu.roll(last, shift, 1)
            tables[j] = jnp.concatenate([turned[:, :LANES], last], axis=1).astype(jnp.bfloat16)
        return carry

    lax.fori_loop(0, 4, prepare, 0)
    cross(1)
    pass_on(0, range(2))
    send(1, range(middle, wave_count))
    pass_on(0, range(2, len(planes)))

    come, go = grid_of((lev_count * LANES, wide), 0), grid_of((lev_count * LANES, wide), 1)
    p, lane = come // LANES, come % LANES
    h, lane = lane // half, lane % half
    g, lane = lane // fwd_step, lane % fwd_step
    target = h * LANES + g * rest_step + lane // short * extra + p * short + lane % short
    spread = ones_where((go == target) & (g < groups))

    loads[1].wait()
    row, col = grid_of((fields, layer_count), 0), grid_of((fields, layer_count), 1)
    chosen = ones_where(col == lev * lev_local + row // part_count)
    coupled_rows = f32_dot(chosen, coupler_in[...], NN)
    tops = jnp.concatenate([chosen.astype(jnp.float32), coupled_rows], axis=0)
    tops_part = lax.rem(grid_of(tops.shape, 0), part_count)
    keeps = [jnp.where(tops_part == c, tops, 0.0) for c in range(part_count)]
    pieces = [k[:, :LANES] for k in keeps] + [k[:, LANES:] for k in keeps]
    pieces.append(jnp.zeros((2 * fields, LANES - part_count * extra), jnp.float32))
    weights[...] = jnp.concatenate(pieces, axis=1).astype(jnp.bfloat16)

    for copy in loads[2:5]:
        copy.wait()
    gain = jnp.sum(
        jnp.where(col == lev * lev_local + row // part_count, strengths_in[...], 0.0),
        axis=1, keepdims=True,
    )
    n = grid_of((1, total_n), 1)
    scaled = (n * (n + 1)).astype(jnp.float32) / jnp.float32((total_n - 1) * total_n)
    damping = 1.0 / (1.0 + gain * scaled ** 2)
    spin_flat = spin_in.reshape(row_count, fields, total_n)
    vort_flat = vort_out.reshape(row_count, fields, total_n)
    for r in range(row_count):
        value = (spin_flat[r].astype(jnp.float32) * damping)
        value = jnp.where(n >= orders_in[:, r:r + 1], value, 0.0)
        vort_flat[r] = value.astype(jnp.bfloat16)

    pass_on(1, range(len(planes)))
    lane = grid_of((wave_count, LANES), 1)
    parties = [range(1, 4), *([i] for i in range(4, wave_count))]
    group_of = {i: g for g, party in enumerate(parties) for i in party}

    def hand_over(ref, r, spot, target):
        pltpu.make_async_remote_copy(
            src_ref=ref, dst_ref=relayed.at[r, spot],
            send_sem=relay_send.at[r], recv_sem=relay_recv.at[r],
            device_id=(target, other), device_id_type=MESH,
        ).start()

    def give_back(r, masks):
        for mask in masks:
            copy = pltpu.make_async_remote_copy(
                src_ref=back_out.at[r, peer[mask]], dst_ref=back_in.at[r, wave],
                send_sem=back_send.at[r], recv_sem=back_recv.at[
                    r, group_of[mask] if mask < middle else group_of[middle] + rank[mask]
                ],
                device_id=(peer[mask], lev), device_id_type=MESH,
            )
            copy.start()
            if mask in parties[0]:
                hand_over(back_out.at[r, peer[mask]], r, wave, peer[mask])

    def relay(r, masks):
        if masks[0]:
            await_bytes(back_in.at[r, pl.ds(0, len(masks))], back_recv.at[r, group_of[masks[0]]])
        for mask in masks:
            hand_over((back_in if mask else back_out).at[r, peer[mask]], r, peer[mask], wave)

    def solve_chunk(r):
        rows_in = by_rows(incoming[r])
        for q in range(lev_count):
            main = rows_in[pl.ds(q * wave_count, wave_count), :local_n]
            gathered[q] = main.astype(jnp.float32).reshape(block_n, LANES)
        if r == 0:
            rests = [
                rows_in[pl.ds(q * wave_count, wave_count), local_n:]
                .astype(jnp.float32).reshape(wave_count * 4, LANES)
                for q in range(lev_count)
            ]
            value = jnp.concatenate(rests, axis=1).astype(jnp.bfloat16)
            value = f32_dot(value, spread, NN)
            for h in range(2):
                rest_in[h] = value[:, h * LANES:(h + 1) * LANES]

        def solve(t, carry):
            every = pl.ds(t, wave_count, stride=4)
            lasts = None
            for h, g in cells:
                j = g * 8 + h * 4 + t
                rest = rest_in[h, every, :]
                rows = pl.ds(j, wave_count, stride=local_n)
                low, high = gathered[0, rows, :], gathered[1, rows, :]
                sides = [jnp.where(lane < half, low, high),
                         pltpu.roll(jnp.where(lane < half, high, low), half, 1)]
                stacked = []
                for c in range(part_count):
                    shift = g * rest_step + (r * part_count + c) * extra
                    moved = pltpu.roll(rest, LANES - shift, 1) if shift else rest
                    stacked.append(jnp.concatenate([sides[c], moved], axis=1)[:, :depth])
                stacked = jnp.concatenate(stacked, axis=0).astype(jnp.bfloat16)
                result = f32_dot(stacked, tables[j], NN)
                for c in range(part_count):
                    strided[c, rows, :] = result[c * wave_count:(c + 1) * wave_count, :LANES]
                last = result[:, LANES:]
                lasts = last if lasts is None else lasts + last
            total = lasts[:wave_count]
            for c in range(1, part_count):
                total += pltpu.roll(lasts[c * wave_count:(c + 1) * wave_count], c * extra, 1)
            rest_out[every, :] = total
            return carry

        lax.fori_loop(0, 4, solve, 0, unroll=4)
        rows_out = by_rows(back_out)
        for c in range(part_count):
            rows_out[r, :, c * local_n:(c + 1) * local_n] = (
                strided[c].reshape(wave_count, local_n, LANES).astype(jnp.bfloat16)
            )
        rows_out[r, :, part_count * local_n:] = (
            rest_out[...].reshape(wave_count, 4, LANES).astype(jnp.bfloat16)
        )
        relay(r, [0])
        give_back(r, range(1, wave_count if r == 0 else middle + 4))
        back_in[r, wave] = back_out[r, wave]

    heat_flat = heat_in.reshape(row_count, fields, total_n)
    div_flat = div_out.reshape(row_count, fields, total_n)
    temp_flat = temp_out.reshape(row_count, fields, total_n)

    def finish(r, wire, block):
        rows_in = by_rows(wire)
        sides = [
            rows_in[r, :, c * local_n:(c + 1) * local_n].astype(jnp.float32).reshape(block_n, LANES)
            for c in range(part_count)
        ]
        folded = rows_in[r, :, part_count * local_n:].astype(jnp.float32)
        swung = pltpu.roll(folded.reshape(wave_count * 4, LANES), half, 1)
        folded = jnp.concatenate([folded, swung.reshape(wave_count, 4, LANES)], axis=1)
        folded = folded.reshape(wave_count * 8, LANES)
        rest = [(pltpu.roll(folded, LANES - g * back_step, 1) if g else folded)
                .reshape(wave_count, 1, 8, LANES) for g in range(groups)]
        sides.append(jnp.concatenate(rest, axis=1).reshape(block_n, LANES))
        packed = jnp.concatenate(sides, axis=1).astype(jnp.bfloat16)
        result = f32_dot(weights[...], packed, NT)
        spots = pl.ds(pl.multiple_of(block * block_n, LANES), block_n)
        inside = block * block_n + grid_of((1, block_n), 1) >= orders_in[:, r:r + 1]
        div_flat[r, :, spots] = jnp.where(inside, result[:fields], 0.0).astype(jnp.bfloat16)
        coupled = result[fields:].astype(jnp.bfloat16).astype(jnp.float32)
        warmed = heat_flat[r, :, spots].astype(jnp.float32) - coupled
        temp_flat[r, :, spots] = jnp.where(inside, warmed, 0.0).astype(jnp.bfloat16)

    loads[5].wait()
    for r in range(row_count):
        await_bytes(incoming[r].at[pl.ds(0, sources - 2)], fwd_recv.at[r])
        solve_chunk(r)
    for party in parties[1:]:
        relay(0, party)
        place = party[0] - middle
        if place > 0 and place % 2 and middle + 4 + place // 2 < wave_count:
            give_back(1, [middle + 4 + place // 2])
    for r in range(row_count):
        await_bytes(outgoing[r].at[pl.ds(0, sources - 1)], fwd_send.at[r])
        await_bytes(crossing[r].at[pl.ds(0, wave_count - 1)], pass_send.at[r])
    await_bytes(back_in.at[0, pl.ds(0, len(parties[0]))], back_recv.at[0, 0])
    finish(0, back_in, lev)
    for party in parties[1:]:
        relay(1, party)
    await_bytes(back_in.at[1, pl.ds(0, len(parties[0]))], back_recv.at[1, 0])
    finish(1, back_in, lev)
    for r in range(row_count):
        await_bytes(back_out.at[r, pl.ds(0, wave_count - 1)], back_send.at[r])
    for r in range(row_count):
        await_bytes(relayed.at[r], relay_recv.at[r])
        finish(r, relayed, other)
    for r in range(row_count):
        await_bytes(relayed.at[r], relay_send.at[r])


def store_kernel(*refs):
    count = (len(refs) - 1) // 2
    copies = [
        pltpu.make_async_copy(refs[i], refs[count + i], refs[-1].at[i]) for i in range(count)
    ]
    for copy in copies:
        copy.start()
    for copy in copies:
        copy.wait()


def by_kernel(spin, source, heat, matrices, coupler, strengths, orders):
    lev_count, wave_count = lax.axis_size("lev"), lax.axis_size("wave")
    row_count, part_count, lev_local, total_n = source.shape
    block_n = total_n // lev_count
    local_n = block_n // wave_count
    layer_count = lev_local * lev_count
    fields = lev_local * part_count
    sources = wave_count * lev_count
    depth = -(-layer_count // 16) * 16
    anywhere, vmem = pl.BlockSpec(memory_space=pltpu.HBM), pl.BlockSpec(memory_space=pltpu.VMEM)
    shape = (row_count, lev_local, part_count, total_n)
    bf16, f32 = jnp.bfloat16, jnp.float32
    field = jax.ShapeDtypeStruct(shape, bf16)
    dma = pltpu.SemaphoreType.DMA
    main_pairs, rest_pairs = local_n // 2, 2
    wire = pltpu.VMEM((row_count, wave_count, part_count * main_pairs + rest_pairs, 2, LANES), bf16)

    def first(count):
        return pltpu.VMEM((count, main_pairs + rest_pairs, 2, LANES), bf16)

    def following(count):
        return pltpu.VMEM((count, main_pairs, 2, LANES), bf16)

    each = dma((row_count,))
    outs = pl.pallas_call(
        functools.partial(step_kernel, wave_count, lev_count),
        out_shape=(field,) * 3,
        in_specs=[anywhere] * 7,
        out_specs=(vmem,) * 3,
        scratch_shapes=[
            pltpu.VMEM(shape, bf16), pltpu.VMEM(shape, bf16), pltpu.VMEM(shape, bf16),
            pltpu.VMEM(matrices.shape[1:], bf16), pltpu.VMEM(coupler.shape, bf16),
            pltpu.VMEM((1, layer_count), f32), pltpu.VMEM((1, row_count), jnp.int32),
            first(sources), following(sources), first(sources), following(sources),
            first(wave_count), following(wave_count),
            pltpu.VMEM((lev_count, block_n, LANES), f32),
            pltpu.VMEM((2, wave_count * 4, LANES), f32),
            pltpu.VMEM((local_n, depth, 2 * LANES), bf16),
            pltpu.VMEM((part_count, block_n, LANES), f32),
            pltpu.VMEM((wave_count * 4, LANES), f32),
            pltpu.VMEM((2 * fields, 3 * LANES), bf16),
            wire, wire, wire,
            dma((7,)), each, each, dma((row_count, wave_count // 4)), each,
            each, dma((row_count, wave_count - 3)), each, each,
        ],
        compiler_params=pltpu.CompilerParams(
            collective_id=0, has_side_effects=True, vmem_limit_bytes=48 * 2**20
        ),
    )(
        *(
            pltpu.with_memory_space_constraint(value, pltpu.HBM)
            for value in (
                spin.transpose(0, 2, 1, 3), source.transpose(0, 2, 1, 3), heat.transpose(0, 2, 1, 3),
                matrices[0], coupler, strengths.reshape(1, layer_count), orders.reshape(1, row_count),
            )
        )
    )
    outs = pl.pallas_call(
        store_kernel, out_shape=(field,) * 3, in_specs=[vmem] * 3, out_specs=(anywhere,) * 3,
        scratch_shapes=[dma((3,))],
        compiler_params=pltpu.CompilerParams(vmem_limit_bytes=4 * 2**20),
    )(*outs)
    return tuple(out.transpose(0, 2, 1, 3) for out in outs)


def kernel_fits(source_shape, lev_count, wave_count):
    row_count, part_count, lev_local, total_n = source_shape
    block_n = total_n // lev_count
    extra = lev_local * lev_count - LANES
    half = LANES // 2
    groups = block_n // (8 * wave_count)
    return (
        lev_count == 2
        and part_count == 2
        and row_count == 2
        and wave_count > 8
        and wave_count & (wave_count - 1) == 0
        and wave_count % 8 == 0
        and block_n % LANES == 0
        and total_n % (2 * LANES) == 0
        and block_n % (8 * wave_count) == 0
        and extra > 0
        and extra * row_count * part_count * groups <= LANES
        and (lev_local - half) * row_count * part_count * groups <= half
        and extra * part_count * groups <= half
    )


def on_device(
    spin_tendency,
    spreading_source,
    heat_source,
    helmholtz_inverses,
    heat_spreading_coupler,
    smoothing_strengths,
    azimuthal_order_list,
):
    lev_count, wave_count = lax.axis_size("lev"), lax.axis_size("wave")
    lev_index = lax.axis_index("lev")
    lev_local, total_n = spreading_source.shape[2:]
    empty_placeholder = jnp.zeros((), jnp.bfloat16)
    if kernel_fits(spreading_source.shape, lev_count, wave_count):
        return by_kernel(
            spin_tendency, spreading_source, heat_source, helmholtz_inverses,
            heat_spreading_coupler, smoothing_strengths, azimuthal_order_list,
        )
    spreading_updated, coupled_out = exchange_by_collectives(
        spreading_source, helmholtz_inverses, heat_spreading_coupler
    )
    heat_updated = (heat_source.astype(jnp.float32) - coupled_out.astype(jnp.float32)).astype(
        jnp.bfloat16
    )
    level_gain = lax.dynamic_slice_in_dim(smoothing_strengths, lev_index * lev_local, lev_local)
    damping = damping_table(level_gain, jnp.arange(total_n, dtype=jnp.int32), total_n)
    spin_updated = (spin_tendency.astype(jnp.float32) * damping[None, None]).astype(jnp.bfloat16)
    interior_slice = (
        jnp.arange(total_n, dtype=jnp.int32)[None, :] >= azimuthal_order_list[:, None]
    )[:, None, None, :]
    return (
        jnp.where(interior_slice, spin_updated, empty_placeholder),
        jnp.where(interior_slice, spreading_updated, empty_placeholder),
        jnp.where(interior_slice, heat_updated, empty_placeholder),
    )


def solution(mesh):
    return jax.shard_map(
        on_device,
        mesh=mesh,
        in_specs=(
            P("wave", None, "lev", None),
            P("wave", None, "lev", None),
            P("wave", None, "lev", None),
            P("lev", "wave", None, None),
            P(),
            P(),
            P("wave"),
        ),
        out_specs=(
            P("wave", None, "lev", None),
            P("wave", None, "lev", None),
            P("wave", None, "lev", None),
        ),
        check_vma=False,
    )
```

```python
import functools
import jax
import jax.numpy as jnp
from jax import lax
from jax.experimental import pallas as pl
from jax.experimental.pallas import tpu as pltpu
from jax.sharding import PartitionSpec as P

LANES = 128
MESH = pl.DeviceIdType.MESH
NN = (((1,), (0,)), ((), ()))
NT = (((1,), (1,)), ((), ()))


def damping_table(level_gain, wavenumbers, total_n):
    scaled = (wavenumbers * (wavenumbers + 1)).astype(jnp.float32) / jnp.float32(
        (total_n - 1) * total_n
    )
    return 1.0 / (1.0 + level_gain[:, None] * scaled[None, :] ** 2)


def exchange_by_collectives(spreading_source, helmholtz_inverses, heat_spreading_coupler):
    lev_count = lax.axis_size("lev")
    row_count, part_count, lev_local, total_n = spreading_source.shape
    block_n = total_n // lev_count
    layer_count = lev_local * lev_count
    flat_rows = row_count * part_count
    wave_count = lax.axis_size("wave")
    local_n = block_n // wave_count
    rhs_div = lax.all_to_all(spreading_source, "lev", split_axis=3, concat_axis=2, tiled=True)
    outgoing = rhs_div.reshape(flat_rows, layer_count, wave_count, local_n).transpose(2, 3, 0, 1)
    outgoing = outgoing.reshape(wave_count, local_n, flat_rows * layer_count)
    columns = lax.all_to_all(outgoing, "wave", split_axis=0, concat_axis=0, tiled=True)
    columns = columns.reshape(wave_count, local_n, flat_rows, layer_count)
    solved_columns = jnp.einsum(
        "jkp,wjcp->wjck", helmholtz_inverses[0], columns, preferred_element_type=jnp.float32
    ).astype(jnp.bfloat16)
    solved_columns = solved_columns.reshape(wave_count, local_n, flat_rows * layer_count)
    returned = lax.all_to_all(solved_columns, "wave", split_axis=0, concat_axis=0, tiled=True)
    answer_fields = returned.reshape(block_n, flat_rows, layer_count).transpose(1, 2, 0)
    coupled = jnp.einsum(
        "om,dms->dos", heat_spreading_coupler, answer_fields, preferred_element_type=jnp.float32
    ).astype(jnp.bfloat16)
    both = jnp.stack([answer_fields, coupled])
    both = lax.all_to_all(both, "lev", split_axis=2, concat_axis=3, tiled=True)
    both = both.reshape(2, row_count, part_count, lev_local, total_n)
    spreading_updated, coupled_out = both[0], both[1]
    return spreading_updated, coupled_out


def f32_dot(left, right, dims):
    return lax.dot_general(left, right, dims, preferred_element_type=jnp.float32)


def grid_of(shape, axis):
    return lax.broadcasted_iota(jnp.int32, shape, axis)


def ones_where(condition, dtype=jnp.bfloat16):
    return jnp.where(condition, 1.0, 0.0).astype(dtype)


def flipped(value, mask):
    out, bit = value, 1
    while bit <= mask:
        if mask & bit:
            out = out + bit * (1 - 2 * lax.rem(lax.div(value, bit), 2))
        bit *= 2
    return out


def by_rows(ref):
    return ref.reshape(*ref.shape[:-3], ref.shape[-3] * 2, LANES)


def block_values(wire, weights, heat_flat, orders, r, block, block_n, step):
    wave_count = wire.shape[1]
    local_n = block_n // wave_count
    groups = local_n // 8
    fields = heat_flat.shape[1]
    rows_in = by_rows(wire)
    parts = (rows_in.shape[2] - 4) // local_n
    sides = [
        rows_in[r, :, c * local_n:(c + 1) * local_n].astype(jnp.float32).reshape(block_n, LANES)
        for c in range(parts)
    ]
    folded = rows_in[r, :, parts * local_n:].astype(jnp.float32)
    swung = pltpu.roll(folded.reshape(wave_count * 4, LANES), LANES // 2, 1)
    folded = jnp.concatenate([folded, swung.reshape(wave_count, 4, LANES)], axis=1)
    folded = folded.reshape(wave_count * 8, LANES)
    rest = [(pltpu.roll(folded, LANES - g * step, 1) if g else folded)
            .reshape(wave_count, 1, 8, LANES) for g in range(groups)]
    sides.append(jnp.concatenate(rest, axis=1).reshape(block_n, LANES))
    packed = jnp.concatenate(sides, axis=1).astype(jnp.bfloat16)
    result = f32_dot(weights[...], packed, NT)
    spots = pl.ds(pl.multiple_of(block * block_n, LANES), block_n)
    inside = block * block_n + grid_of((1, block_n), 1) >= orders[:, r:r + 1]
    coupled = result[fields:].astype(jnp.bfloat16).astype(jnp.float32)
    warmed = heat_flat[r, :, spots].astype(jnp.float32) - coupled
    return (
        jnp.where(inside, result[:fields], 0.0).astype(jnp.bfloat16),
        jnp.where(inside, warmed, 0.0).astype(jnp.bfloat16),
    )


def step_kernel(
    wave_count, lev_count, spin, source, heat, matrices, coupler, strengths, orders,
    vort_out, div_out, temp_out, relayed, weights, heat_in, orders_in,
    spin_in, source_in, mats_in, coupler_in, strengths_in,
    first_out, next_out, first_in, next_in, first_lev, next_lev, gathered, rest_in, tables, strided, rest_out,
    back_out, back_in,
    load_sem, fwd_send, fwd_recv, lev_recv, pass_send, back_send, back_recv, relay_send, relay_recv,
):
    wave, lev = lax.axis_index("wave"), lax.axis_index("lev")
    row_count, lev_local, part_count, total_n = source.shape
    block_n = total_n // lev_count
    local_n = block_n // wave_count
    groups = local_n // 8
    layer_count = lev_local * lev_count
    fields = lev_local * part_count
    half = LANES // part_count
    short = lev_local - half
    extra = layer_count - LANES
    depth = tables.shape[1]
    sources = wave_count * lev_count
    wide = 2 * LANES
    cells = [(h, g) for h in range(2) for g in range(groups)]
    fwd_step = row_count * part_count * short
    back_step = part_count * extra
    rest_step = row_count * part_count * extra

    loads = []
    small = [(matrices, mats_in), (coupler, coupler_in), (strengths, strengths_in),
             (orders, orders_in), (spin, spin_in), (heat, heat_in)]
    for i, (src, dst) in enumerate(
        [(source, source_in), *small]
    ):
        copy = pltpu.make_async_copy(src, dst, load_sem.at[i])
        copy.start()
        loads.append(copy)
    source_load, loads = loads[0], loads[1:]

    middle = wave_count // 2
    block = lax.rem(wave, 4)
    across = middle * (1 - lax.div(wave, middle))
    flips = [flipped(wave, mask) for mask in range(wave_count)]
    peer = flips[:middle]
    peer += [across + i // 4 * 4 + flipped(block, i % 4) for i in range(middle)]
    rank = [*range(middle), *(lax.div(lax.rem(wave, middle), 4) * 4 + i % 4 for i in range(middle))]
    other = lax.rem(lev + 1, lev_count)
    outward = [*range(1, wave_count), 0]
    barrier = pltpu.get_barrier_semaphore()
    for mask in reversed(range(wave_count)):
        for t, q in enumerate((lev, other)):
            if mask or t:
                pl.semaphore_signal(
                    barrier, inc=1, device_id=(peer[mask], q), device_id_type=MESH
                )

    out_row, in_row = grid_of((wide, fields), 0), grid_of((wide, fields), 1)
    level, part = in_row // part_count, in_row % part_count
    main_spot = lax.rem(part + lev, part_count) * half + level
    main_pick = ones_where(
        (out_row == main_spot)[:LANES] & (level < half)[:LANES]
    )
    rest_picks = [
        ones_where(
            (out_row == (r * part_count + part) * short + level - half)[:LANES]
            & (level >= half)[:LANES]
        )
        for r in range(row_count)
    ]
    eye = ones_where(grid_of((wide, wide), 0) == grid_of((wide, wide), 1))
    flat = source_in.reshape(row_count, fields, total_n)
    mine = lev * wave_count + wave

    def turn(rows):
        return jnp.concatenate(
            [f32_dot(eye, rows[:, k:k + wide], NT) for k in range(0, total_n, wide)], axis=0
        )

    outgoing, incoming = [first_out, next_out], [first_in, next_in]

    def await_bytes(ref, sem):
        pltpu.make_async_copy(ref, ref, sem).wait()

    crossing = [first_lev, next_lev]
    home = middle - across
    planes = [across + i for i in range(0, middle, 4)]
    planes += [home + lax.rem(lax.rem(wave - block - home, middle) + i, middle)
               for i in range(4, middle, 4)]
    planes += [wave - block]

    def cross(r):
        for i, plane in enumerate(planes):
            pltpu.make_async_remote_copy(
                src_ref=outgoing[r].at[pl.ds(other * wave_count + plane, 4)],
                dst_ref=crossing[r].at[pl.ds(plane, 4)],
                send_sem=fwd_send.at[r], recv_sem=lev_recv.at[r, i],
                device_id=(wave, other), device_id_type=MESH,
            ).start()

    def send(r, masks):
        for mask in masks:
            pltpu.make_async_remote_copy(
                src_ref=outgoing[r].at[lev * wave_count + flips[mask]],
                dst_ref=incoming[r].at[mine],
                send_sem=fwd_send.at[r], recv_sem=fwd_recv.at[r],
                device_id=(flips[mask], lev), device_id_type=MESH,
            ).start()

    def pass_on(r, which):
        for i in which:
            plane = planes[i]
            await_bytes(crossing[r].at[pl.ds(0, 4)], lev_recv.at[r, i])
            last = i == len(planes) - 1
            for k in range(1 if last else 0, 4):
                target = plane + flipped(block, k)
                pltpu.make_async_remote_copy(
                    src_ref=crossing[r].at[target],
                    dst_ref=incoming[r].at[other * wave_count + wave],
                    send_sem=pass_send.at[r], recv_sem=fwd_recv.at[r],
                    device_id=(target, lev), device_id_type=MESH,
                ).start()
            if last:
                incoming[r][other * wave_count + wave] = crossing[r][wave]

    source_load.wait()
    main = f32_dot(main_pick, flat[0], NN)
    rest = f32_dot(rest_picks[0], flat[0], NN)
    for r in range(1, row_count):
        rest += f32_dot(rest_picks[r], flat[r], NN)
    turned = turn(jnp.concatenate([main, rest], axis=0).astype(jnp.bfloat16))
    tail = turned[:, LANES:].reshape(sources, groups, 8, LANES)
    folded = tail[:, 0].reshape(sources * 8, LANES)
    for g in range(1, groups):
        folded += pltpu.roll(tail[:, g].reshape(sources * 8, LANES), g * fwd_step, 1)
    swung = pltpu.roll(folded, half, 1).reshape(sources, 8, LANES)
    folded = folded.reshape(sources, 8, LANES)[:, :4] + swung[:, 4:]
    by_rows(first_out)[:, :local_n] = (
        turned[:, :LANES].reshape(sources, local_n, LANES).astype(jnp.bfloat16)
    )
    by_rows(first_out)[:, local_n:] = folded.astype(jnp.bfloat16)
    pl.semaphore_wait(barrier, sources - 1)
    cross(0)
    send(0, range(1, wave_count))
    incoming[0][mine] = outgoing[0][mine]
    for r in range(1, row_count):
        turned = turn(f32_dot(main_pick, flat[r], NN).astype(jnp.bfloat16))
        by_rows(next_out)[...] = turned.reshape(sources, local_n, LANES).astype(jnp.bfloat16)
        send(r, range(1, middle))
        incoming[r][mine] = outgoing[r][mine]

    loads[0].wait()
    deep, flat_level = grid_of((depth, layer_count), 0), grid_of((depth, layer_count), 1)
    owner, place = flat_level // lev_local, flat_level % lev_local
    spot = jnp.where(place < half, owner * half + place, LANES + owner * short + place - half)
    ordered = ones_where(deep == spot)
    zeros = jnp.zeros((depth, LANES - extra), jnp.float32)

    def prepare(t, carry):
        for h, g in cells:
            j = g * 8 + h * 4 + t
            turned = f32_dot(ordered, mats_in[j], NT)
            last = jnp.concatenate([turned[:, LANES:], zeros], axis=1)
            shift = h * half + g * back_step
            if shift:
                last = pltpu.roll(last, shift, 1)
            tables[j] = jnp.concatenate([turned[:, :LANES], last], axis=1).astype(jnp.bfloat16)
        return carry

    lax.fori_loop(0, 4, prepare, 0)
    cross(1)
    pass_on(0, range(2))

    @pl.when(wave >= middle)
    def _():
        send(1, range(middle, wave_count))

    pass_on(0, range(2, len(planes)))

    come, go = grid_of((lev_count * LANES, wide), 0), grid_of((lev_count * LANES, wide), 1)
    p, lane = come // LANES, come % LANES
    h, lane = lane // half, lane % half
    g, lane = lane // fwd_step, lane % fwd_step
    target = h * LANES + g * rest_step + lane // short * extra + p * short + lane % short
    spread = ones_where((go == target) & (g < groups))

    loads[1].wait()
    row, col = grid_of((fields, layer_count), 0), grid_of((fields, layer_count), 1)
    chosen = ones_where(col == lev * lev_local + row // part_count)
    coupled_rows = f32_dot(chosen, coupler_in[...], NN)
    tops = jnp.concatenate([chosen.astype(jnp.float32), coupled_rows], axis=0)
    tops_part = lax.rem(grid_of(tops.shape, 0), part_count)
    keeps = [jnp.where(tops_part == c, tops, 0.0) for c in range(part_count)]
    pieces = [k[:, :LANES] for k in keeps] + [k[:, LANES:] for k in keeps]
    pieces.append(jnp.zeros((2 * fields, LANES - part_count * extra), jnp.float32))
    weights[...] = jnp.concatenate(pieces, axis=1).astype(jnp.bfloat16)

    for copy in loads[2:5]:
        copy.wait()
    gain = jnp.sum(
        jnp.where(col == lev * lev_local + row // part_count, strengths_in[...], 0.0),
        axis=1, keepdims=True,
    )
    n = grid_of((1, total_n), 1)
    scaled = (n * (n + 1)).astype(jnp.float32) / jnp.float32((total_n - 1) * total_n)
    damping = 1.0 / (1.0 + gain * scaled ** 2)
    spin_flat = spin_in.reshape(row_count, fields, total_n)
    vort_flat = vort_out.reshape(row_count, fields, total_n)
    for r in range(row_count):
        value = (spin_flat[r].astype(jnp.float32) * damping)
        value = jnp.where(n >= orders_in[:, r:r + 1], value, 0.0)
        vort_flat[r] = value.astype(jnp.bfloat16)


    @pl.when(wave < middle)
    def _():
        send(1, range(middle, wave_count))

    pass_on(1, range(len(planes)))
    lane = grid_of((wave_count, LANES), 1)
    parties = [range(1, 4), *([i] for i in range(4, wave_count))]
    group_of = {i: g for g, party in enumerate(parties) for i in party}

    def hand_over(ref, r, spot, target):
        pltpu.make_async_remote_copy(
            src_ref=ref, dst_ref=relayed.at[r, spot],
            send_sem=relay_send.at[r], recv_sem=relay_recv.at[r],
            device_id=(target, other), device_id_type=MESH,
        ).start()

    def give_back(r, masks):
        for mask in masks:
            copy = pltpu.make_async_remote_copy(
                src_ref=back_out.at[r, peer[mask]], dst_ref=back_in.at[r, wave],
                send_sem=back_send.at[r], recv_sem=back_recv.at[
                    r, group_of[mask] if mask < middle else group_of[middle] + rank[mask]
                ],
                device_id=(peer[mask], lev), device_id_type=MESH,
            )
            copy.start()
            if mask in parties[0]:
                hand_over(back_out.at[r, peer[mask]], r, wave, peer[mask])

    def relay(r, masks):
        if masks[0]:
            await_bytes(back_in.at[r, pl.ds(0, len(masks))], back_recv.at[r, group_of[masks[0]]])
        for mask in masks:
            hand_over((back_in if mask else back_out).at[r, peer[mask]], r, peer[mask], wave)

    def solve_chunk(r):
        rows_in = by_rows(incoming[r])
        for q in range(lev_count):
            main = rows_in[pl.ds(q * wave_count, wave_count), :local_n]
            gathered[q] = main.astype(jnp.float32).reshape(block_n, LANES)
        if r == 0:
            rests = [
                rows_in[pl.ds(q * wave_count, wave_count), local_n:]
                .astype(jnp.float32).reshape(wave_count * 4, LANES)
                for q in range(lev_count)
            ]
            value = jnp.concatenate(rests, axis=1).astype(jnp.bfloat16)
            value = f32_dot(value, spread, NN)
            for h in range(2):
                rest_in[h] = value[:, h * LANES:(h + 1) * LANES]

        def solve(t, carry):
            every = pl.ds(t, wave_count, stride=4)
            lasts = None
            for h, g in cells:
                j = g * 8 + h * 4 + t
                rest = rest_in[h, every, :]
                rows = pl.ds(j, wave_count, stride=local_n)
                low, high = gathered[0, rows, :], gathered[1, rows, :]
                sides = [jnp.where(lane < half, low, high),
                         pltpu.roll(jnp.where(lane < half, high, low), half, 1)]
                stacked = []
                for c in range(part_count):
                    shift = g * rest_step + (r * part_count + c) * extra
                    moved = pltpu.roll(rest, LANES - shift, 1) if shift else rest
                    stacked.append(jnp.concatenate([sides[c], moved], axis=1)[:, :depth])
                stacked = jnp.concatenate(stacked, axis=0).astype(jnp.bfloat16)
                result = f32_dot(stacked, tables[j], NN)
                for c in range(part_count):
                    strided[c, rows, :] = result[c * wave_count:(c + 1) * wave_count, :LANES]
                last = result[:, LANES:]
                lasts = last if lasts is None else lasts + last
            total = lasts[:wave_count]
            for c in range(1, part_count):
                total += pltpu.roll(lasts[c * wave_count:(c + 1) * wave_count], c * extra, 1)
            rest_out[every, :] = total
            return carry

        lax.fori_loop(0, 4, solve, 0, unroll=4)
        rows_out = by_rows(back_out)
        for c in range(part_count):
            rows_out[r, :, c * local_n:(c + 1) * local_n] = (
                strided[c].reshape(wave_count, local_n, LANES).astype(jnp.bfloat16)
            )
        rows_out[r, :, part_count * local_n:] = (
            rest_out[...].reshape(wave_count, 4, LANES).astype(jnp.bfloat16)
        )
        relay(r, [0])
        give_back(r, range(1, wave_count if r == 0 else middle))
        back_in[r, wave] = back_out[r, wave]

    heat_flat = heat_in.reshape(row_count, fields, total_n)
    div_flat = div_out.reshape(row_count, fields, total_n)
    temp_flat = temp_out.reshape(row_count, fields, total_n)

    def finish(r, wire, block):
        spots = pl.ds(pl.multiple_of(block * block_n, LANES), block_n)
        div_flat[r, :, spots], temp_flat[r, :, spots] = block_values(
            wire, weights, heat_flat, orders_in, r, block, block_n, back_step
        )

    loads[5].wait()
    for r in range(row_count):
        await_bytes(incoming[r].at[pl.ds(0, sources - 2)], fwd_recv.at[r])
        solve_chunk(r)
    m = middle
    paced = {4: [m, m + 1], 5: [m + 2, m + 3], 7: [m + 4], m: [m + 5], m + 1: [m + 6],
             m + 2: range(m + 7, wave_count)}
    for party in parties[1:]:
        relay(0, party)
        if party[0] in paced:
            give_back(1, paced[party[0]])
    for r in range(row_count):
        await_bytes(outgoing[r].at[pl.ds(0, sources - 1)], fwd_send.at[r])
        await_bytes(crossing[r].at[pl.ds(0, wave_count - 1)], pass_send.at[r])
    await_bytes(back_in.at[0, pl.ds(0, len(parties[0]))], back_recv.at[0, 0])
    finish(0, back_in, lev)
    for party in parties[1:]:
        relay(1, party)
    await_bytes(back_in.at[1, pl.ds(0, len(parties[0]))], back_recv.at[1, 0])
    finish(1, back_in, lev)
    for r in range(row_count):
        await_bytes(back_out.at[r, pl.ds(0, wave_count - 1)], back_send.at[r])
    for r in range(row_count):
        await_bytes(relayed.at[r], relay_recv.at[r])
        if r + 1 < row_count:
            finish(r, relayed, other)
    for r in range(row_count):
        await_bytes(relayed.at[r], relay_send.at[r])


def store_kernel(
    lev_count, step, vort, div, temp, wire, weights, heat, orders, vort_out, div_out, temp_out,
    div_last, temp_last, sems,
):
    row_count, lev_local, part_count, total_n = vort.shape
    block_n = total_n // lev_count
    last = row_count - 1
    lev = lax.axis_index("lev")
    mine, others = (
        pl.ds(pl.multiple_of(block * block_n, LANES), block_n)
        for block in (lev, lax.rem(lev + 1, lev_count))
    )
    pairs = [(vort, vort_out)]
    for src, dst in ((div, div_out), (temp, temp_out)):
        pairs += [(src.at[r], dst.at[r]) for r in range(last)]
        pairs.append((src.at[last, :, :, mine], dst.at[last, :, :, mine]))
    late = [(div_last, div_out.at[last, :, :, others]), (temp_last, temp_out.at[last, :, :, others])]
    copies = [
        pltpu.make_async_copy(src, dst, sems.at[i]) for i, (src, dst) in enumerate(pairs + late)
    ]
    for copy in copies[:len(pairs)]:
        copy.start()
    fields = lev_local * part_count
    values = block_values(
        wire, weights, heat.reshape(row_count, fields, total_n), orders, last,
        lax.rem(lev + 1, lev_count), block_n, step,
    )
    for ref, value in zip((div_last, temp_last), values):
        ref.reshape(fields, block_n)[...] = value
    for copy in copies[len(pairs):]:
        copy.start()
    for copy in copies:
        copy.wait()


def by_kernel(spin, source, heat, matrices, coupler, strengths, orders):
    lev_count, wave_count = lax.axis_size("lev"), lax.axis_size("wave")
    row_count, part_count, lev_local, total_n = source.shape
    block_n = total_n // lev_count
    local_n = block_n // wave_count
    layer_count = lev_local * lev_count
    fields = lev_local * part_count
    sources = wave_count * lev_count
    depth = -(-layer_count // 16) * 16
    anywhere, vmem = pl.BlockSpec(memory_space=pltpu.HBM), pl.BlockSpec(memory_space=pltpu.VMEM)
    shape = (row_count, lev_local, part_count, total_n)
    bf16, f32 = jnp.bfloat16, jnp.float32
    field = jax.ShapeDtypeStruct(shape, bf16)
    dma = pltpu.SemaphoreType.DMA
    main_pairs, rest_pairs = local_n // 2, 2
    wire_shape = (row_count, wave_count, part_count * main_pairs + rest_pairs, 2, LANES)
    wire = pltpu.VMEM(wire_shape, bf16)

    def first(count):
        return pltpu.VMEM((count, main_pairs + rest_pairs, 2, LANES), bf16)

    def following(count):
        return pltpu.VMEM((count, main_pairs, 2, LANES), bf16)

    each = dma((row_count,))
    outs = pl.pallas_call(
        functools.partial(step_kernel, wave_count, lev_count),
        out_shape=(
            field, field, field, jax.ShapeDtypeStruct(wire_shape, bf16),
            jax.ShapeDtypeStruct((2 * fields, 3 * LANES), bf16), field,
            jax.ShapeDtypeStruct((1, row_count), jnp.int32),
        ),
        in_specs=[anywhere] * 7,
        out_specs=(vmem,) * 7,
        scratch_shapes=[
            pltpu.VMEM(shape, bf16), pltpu.VMEM(shape, bf16),
            pltpu.VMEM(matrices.shape[1:], bf16), pltpu.VMEM(coupler.shape, bf16),
            pltpu.VMEM((1, layer_count), f32),
            first(sources), following(sources), first(sources), following(sources),
            first(wave_count), following(wave_count),
            pltpu.VMEM((lev_count, block_n, LANES), f32),
            pltpu.VMEM((2, wave_count * 4, LANES), f32),
            pltpu.VMEM((local_n, depth, 2 * LANES), bf16),
            pltpu.VMEM((part_count, block_n, LANES), f32),
            pltpu.VMEM((wave_count * 4, LANES), f32),
            wire, wire,
            dma((7,)), each, each, dma((row_count, wave_count // 4)), each,
            each, dma((row_count, wave_count - 3)), each, each,
        ],
        compiler_params=pltpu.CompilerParams(
            collective_id=0, has_side_effects=True, vmem_limit_bytes=48 * 2**20
        ),
    )(
        *(
            pltpu.with_memory_space_constraint(value, pltpu.HBM)
            for value in (
                spin.transpose(0, 2, 1, 3), source.transpose(0, 2, 1, 3), heat.transpose(0, 2, 1, 3),
                matrices[0], coupler, strengths.reshape(1, layer_count), orders.reshape(1, row_count),
            )
        )
    )
    extra = layer_count - LANES
    last_block = pltpu.VMEM((lev_local, part_count, block_n), bf16)
    outs = pl.pallas_call(
        functools.partial(store_kernel, lev_count, part_count * extra),
        out_shape=(field,) * 3, in_specs=[vmem] * 7, out_specs=(anywhere,) * 3,
        scratch_shapes=[last_block, last_block, dma((2 * row_count + 3,))],
        compiler_params=pltpu.CompilerParams(vmem_limit_bytes=8 * 2**20),
    )(*outs)
    return tuple(out.transpose(0, 2, 1, 3) for out in outs)


def kernel_fits(source_shape, lev_count, wave_count):
    row_count, part_count, lev_local, total_n = source_shape
    block_n = total_n // lev_count
    extra = lev_local * lev_count - LANES
    half = LANES // 2
    groups = block_n // (8 * wave_count)
    return (
        lev_count == 2
        and part_count == 2
        and row_count == 2
        and wave_count > 8
        and wave_count & (wave_count - 1) == 0
        and wave_count % 8 == 0
        and block_n % LANES == 0
        and total_n % (2 * LANES) == 0
        and block_n % (8 * wave_count) == 0
        and extra > 0
        and extra * row_count * part_count * groups <= LANES
        and (lev_local - half) * row_count * part_count * groups <= half
        and extra * part_count * groups <= half
    )


def on_device(
    spin_tendency,
    spreading_source,
    heat_source,
    helmholtz_inverses,
    heat_spreading_coupler,
    smoothing_strengths,
    azimuthal_order_list,
):
    lev_count, wave_count = lax.axis_size("lev"), lax.axis_size("wave")
    lev_index = lax.axis_index("lev")
    lev_local, total_n = spreading_source.shape[2:]
    empty_placeholder = jnp.zeros((), jnp.bfloat16)
    if kernel_fits(spreading_source.shape, lev_count, wave_count):
        return by_kernel(
            spin_tendency, spreading_source, heat_source, helmholtz_inverses,
            heat_spreading_coupler, smoothing_strengths, azimuthal_order_list,
        )
    spreading_updated, coupled_out = exchange_by_collectives(
        spreading_source, helmholtz_inverses, heat_spreading_coupler
    )
    heat_updated = (heat_source.astype(jnp.float32) - coupled_out.astype(jnp.float32)).astype(
        jnp.bfloat16
    )
    level_gain = lax.dynamic_slice_in_dim(smoothing_strengths, lev_index * lev_local, lev_local)
    damping = damping_table(level_gain, jnp.arange(total_n, dtype=jnp.int32), total_n)
    spin_updated = (spin_tendency.astype(jnp.float32) * damping[None, None]).astype(jnp.bfloat16)
    interior_slice = (
        jnp.arange(total_n, dtype=jnp.int32)[None, :] >= azimuthal_order_list[:, None]
    )[:, None, None, :]
    return (
        jnp.where(interior_slice, spin_updated, empty_placeholder),
        jnp.where(interior_slice, spreading_updated, empty_placeholder),
        jnp.where(interior_slice, heat_updated, empty_placeholder),
    )


def solution(mesh):
    return jax.shard_map(
        on_device,
        mesh=mesh,
        in_specs=(
            P("wave", None, "lev", None),
            P("wave", None, "lev", None),
            P("wave", None, "lev", None),
            P("lev", "wave", None, None),
            P(),
            P(),
            P("wave"),
        ),
        out_specs=(
            P("wave", None, "lev", None),
            P("wave", None, "lev", None),
            P("wave", None, "lev", None),
        ),
        check_vma=False,
    )
```

```python
import functools
import jax
import jax.numpy as jnp
from jax import lax
from jax.experimental import pallas as pl
from jax.experimental.pallas import tpu as pltpu
from jax.sharding import PartitionSpec as P

LANES = 128
MESH = pl.DeviceIdType.MESH
NN = (((1,), (0,)), ((), ()))
NT = (((1,), (1,)), ((), ()))


def damping_table(level_gain, wavenumbers, total_n):
    scaled = (wavenumbers * (wavenumbers + 1)).astype(jnp.float32) / jnp.float32(
        (total_n - 1) * total_n
    )
    return 1.0 / (1.0 + level_gain[:, None] * scaled[None, :] ** 2)


def exchange_by_collectives(spreading_source, helmholtz_inverses, heat_spreading_coupler):
    lev_count = lax.axis_size("lev")
    row_count, part_count, lev_local, total_n = spreading_source.shape
    block_n = total_n // lev_count
    layer_count = lev_local * lev_count
    flat_rows = row_count * part_count
    wave_count = lax.axis_size("wave")
    local_n = block_n // wave_count
    rhs_div = lax.all_to_all(spreading_source, "lev", split_axis=3, concat_axis=2, tiled=True)
    outgoing = rhs_div.reshape(flat_rows, layer_count, wave_count, local_n).transpose(2, 3, 0, 1)
    outgoing = outgoing.reshape(wave_count, local_n, flat_rows * layer_count)
    columns = lax.all_to_all(outgoing, "wave", split_axis=0, concat_axis=0, tiled=True)
    columns = columns.reshape(wave_count, local_n, flat_rows, layer_count)
    solved_columns = jnp.einsum(
        "jkp,wjcp->wjck", helmholtz_inverses[0], columns, preferred_element_type=jnp.float32
    ).astype(jnp.bfloat16)
    solved_columns = solved_columns.reshape(wave_count, local_n, flat_rows * layer_count)
    returned = lax.all_to_all(solved_columns, "wave", split_axis=0, concat_axis=0, tiled=True)
    answer_fields = returned.reshape(block_n, flat_rows, layer_count).transpose(1, 2, 0)
    coupled = jnp.einsum(
        "om,dms->dos", heat_spreading_coupler, answer_fields, preferred_element_type=jnp.float32
    ).astype(jnp.bfloat16)
    both = jnp.stack([answer_fields, coupled])
    both = lax.all_to_all(both, "lev", split_axis=2, concat_axis=3, tiled=True)
    both = both.reshape(2, row_count, part_count, lev_local, total_n)
    spreading_updated, coupled_out = both[0], both[1]
    return spreading_updated, coupled_out


def f32_dot(left, right, dims):
    return lax.dot_general(left, right, dims, preferred_element_type=jnp.float32)


def grid_of(shape, axis):
    return lax.broadcasted_iota(jnp.int32, shape, axis)


def ones_where(condition, dtype=jnp.bfloat16):
    return jnp.where(condition, 1.0, 0.0).astype(dtype)


def flipped(value, mask):
    out, bit = value, 1
    while bit <= mask:
        if mask & bit:
            out = out + bit * (1 - 2 * lax.rem(lax.div(value, bit), 2))
        bit *= 2
    return out


def by_rows(ref):
    return ref.reshape(*ref.shape[:-3], ref.shape[-3] * 2, LANES)


def block_values(wire, weights, heat_flat, orders, r, block, block_n, step):
    wave_count = wire.shape[1]
    local_n = block_n // wave_count
    groups = local_n // 8
    fields = heat_flat.shape[1]
    rows_in = by_rows(wire)
    parts = (rows_in.shape[2] - 4) // local_n
    sides = [
        rows_in[r, :, c * local_n:(c + 1) * local_n].astype(jnp.float32).reshape(block_n, LANES)
        for c in range(parts)
    ]
    folded = rows_in[r, :, parts * local_n:].astype(jnp.float32)
    swung = pltpu.roll(folded.reshape(wave_count * 4, LANES), LANES // 2, 1)
    folded = jnp.concatenate([folded, swung.reshape(wave_count, 4, LANES)], axis=1)
    folded = folded.reshape(wave_count * 8, LANES)
    rest = [(pltpu.roll(folded, LANES - g * step, 1) if g else folded)
            .reshape(wave_count, 1, 8, LANES) for g in range(groups)]
    sides.append(jnp.concatenate(rest, axis=1).reshape(block_n, LANES))
    packed = jnp.concatenate(sides, axis=1).astype(jnp.bfloat16)
    result = f32_dot(weights[...], packed, NT)
    spots = pl.ds(pl.multiple_of(block * block_n, LANES), block_n)
    inside = block * block_n + grid_of((1, block_n), 1) >= orders[:, r:r + 1]
    coupled = result[fields:].astype(jnp.bfloat16).astype(jnp.float32)
    warmed = heat_flat[r, :, spots].astype(jnp.float32) - coupled
    return (
        jnp.where(inside, result[:fields], 0.0).astype(jnp.bfloat16),
        jnp.where(inside, warmed, 0.0).astype(jnp.bfloat16),
    )


def step_kernel(
    wave_count, lev_count, spin, source, heat, matrices, coupler, strengths, orders,
    vort_out, div_out, temp_out, relayed, weights, heat_in, orders_in,
    spin_in, source_in, mats_in, coupler_in, strengths_in,
    first_out, next_out, first_in, next_in, first_lev, next_lev, gathered, rest_in, tables, strided, rest_out,
    back_out, back_in,
    load_sem, fwd_send, fwd_recv, lev_recv, pass_send, back_send, back_recv, relay_send, relay_recv,
):
    wave, lev = lax.axis_index("wave"), lax.axis_index("lev")
    row_count, lev_local, part_count, total_n = source.shape
    block_n = total_n // lev_count
    local_n = block_n // wave_count
    groups = local_n // 8
    layer_count = lev_local * lev_count
    fields = lev_local * part_count
    half = LANES // part_count
    short = lev_local - half
    extra = layer_count - LANES
    depth = tables.shape[1]
    sources = wave_count * lev_count
    wide = 2 * LANES
    cells = [(h, g) for h in range(2) for g in range(groups)]
    fwd_step = row_count * part_count * short
    back_step = part_count * extra
    rest_step = row_count * part_count * extra

    middle = wave_count // 2
    block = lax.rem(wave, 4)
    across = middle * (1 - lax.div(wave, middle))
    flips = [flipped(wave, mask) for mask in range(wave_count)]
    peer = flips[:middle]
    peer += [across + i // 4 * 4 + flipped(block, i % 4) for i in range(middle)]
    rank = [*range(middle), *(lax.div(lax.rem(wave, middle), 4) * 4 + i % 4 for i in range(middle))]
    other = lax.rem(lev + 1, lev_count)
    outward = [*range(1, wave_count), 0]
    barrier = pltpu.get_barrier_semaphore()

    def greet(masks):
        for mask in masks:
            for t, q in enumerate((lev, other)):
                if mask or t:
                    pl.semaphore_signal(
                        barrier, inc=1, device_id=(flips[mask], q), device_id_type=MESH
                    )

    greet(range(wave_count - 1, middle - 1, -1))
    loads = []
    small = [(matrices, mats_in), (coupler, coupler_in), (strengths, strengths_in),
             (orders, orders_in), (spin, spin_in), (heat, heat_in)]
    for i, (src, dst) in enumerate(
        [(source, source_in), *small]
    ):
        copy = pltpu.make_async_copy(src, dst, load_sem.at[i])
        copy.start()
        loads.append(copy)
    source_load, loads = loads[0], loads[1:]

    greet(range(middle - 1, -1, -1))

    out_row, in_row = grid_of((wide, fields), 0), grid_of((wide, fields), 1)
    level, part = in_row // part_count, in_row % part_count
    main_spot = lax.rem(part + lev, part_count) * half + level
    main_pick = ones_where(
        (out_row == main_spot)[:LANES] & (level < half)[:LANES]
    )
    rest_picks = [
        ones_where(
            (out_row == (r * part_count + part) * short + level - half)[:LANES]
            & (level >= half)[:LANES]
        )
        for r in range(row_count)
    ]
    eye = ones_where(grid_of((wide, wide), 0) == grid_of((wide, wide), 1))
    flat = source_in.reshape(row_count, fields, total_n)
    mine = lev * wave_count + wave

    def turn(rows):
        return jnp.concatenate(
            [f32_dot(eye, rows[:, k:k + wide], NT) for k in range(0, total_n, wide)], axis=0
        )

    outgoing, incoming = [first_out, next_out], [first_in, next_in]

    def await_bytes(ref, sem):
        pltpu.make_async_copy(ref, ref, sem).wait()

    crossing = [first_lev, next_lev]
    home = middle - across
    planes = [across + i for i in range(0, middle, 4)]
    planes += [home + lax.rem(lax.rem(wave - block - home, middle) + i, middle)
               for i in range(4, middle, 4)]
    planes += [wave - block]

    def cross(r):
        for i, plane in enumerate(planes):
            pltpu.make_async_remote_copy(
                src_ref=outgoing[r].at[pl.ds(other * wave_count + plane, 4)],
                dst_ref=crossing[r].at[pl.ds(plane, 4)],
                send_sem=fwd_send.at[r], recv_sem=lev_recv.at[r, i],
                device_id=(wave, other), device_id_type=MESH,
            ).start()

    def send(r, masks):
        for mask in masks:
            pltpu.make_async_remote_copy(
                src_ref=outgoing[r].at[lev * wave_count + flips[mask]],
                dst_ref=incoming[r].at[mine],
                send_sem=fwd_send.at[r], recv_sem=fwd_recv.at[r],
                device_id=(flips[mask], lev), device_id_type=MESH,
            ).start()

    def pass_on(r, which):
        for i in which:
            plane = planes[i]
            await_bytes(crossing[r].at[pl.ds(0, 4)], lev_recv.at[r, i])
            last = i == len(planes) - 1
            for k in range(1 if last else 0, 4):
                target = plane + flipped(block, k)
                pltpu.make_async_remote_copy(
                    src_ref=crossing[r].at[target],
                    dst_ref=incoming[r].at[other * wave_count + wave],
                    send_sem=pass_send.at[r], recv_sem=fwd_recv.at[r],
                    device_id=(target, lev), device_id_type=MESH,
                ).start()
            if last:
                incoming[r][other * wave_count + wave] = crossing[r][wave]

    source_load.wait()
    main = f32_dot(main_pick, flat[0], NN)
    rest = f32_dot(rest_picks[0], flat[0], NN)
    for r in range(1, row_count):
        rest += f32_dot(rest_picks[r], flat[r], NN)
    turned = turn(jnp.concatenate([main, rest], axis=0).astype(jnp.bfloat16))
    tail = turned[:, LANES:].reshape(sources, groups, 8, LANES)
    folded = tail[:, 0].reshape(sources * 8, LANES)
    for g in range(1, groups):
        folded += pltpu.roll(tail[:, g].reshape(sources * 8, LANES), g * fwd_step, 1)
    swung = pltpu.roll(folded, half, 1).reshape(sources, 8, LANES)
    folded = folded.reshape(sources, 8, LANES)[:, :4] + swung[:, 4:]
    by_rows(first_out)[:, :local_n] = (
        turned[:, :LANES].reshape(sources, local_n, LANES).astype(jnp.bfloat16)
    )
    by_rows(first_out)[:, local_n:] = folded.astype(jnp.bfloat16)
    pl.semaphore_wait(barrier, sources - 1)
    cross(0)
    send(0, range(1, wave_count))
    incoming[0][mine] = outgoing[0][mine]
    for r in range(1, row_count):
        turned = turn(f32_dot(main_pick, flat[r], NN).astype(jnp.bfloat16))
        by_rows(next_out)[...] = turned.reshape(sources, local_n, LANES).astype(jnp.bfloat16)
        send(r, range(1, middle))
        incoming[r][mine] = outgoing[r][mine]

    loads[0].wait()
    deep, flat_level = grid_of((depth, layer_count), 0), grid_of((depth, layer_count), 1)
    owner, place = flat_level // lev_local, flat_level % lev_local
    spot = jnp.where(place < half, owner * half + place, LANES + owner * short + place - half)
    ordered = ones_where(deep == spot)
    zeros = jnp.zeros((depth, LANES - extra), jnp.float32)

    def prepare(t, carry):
        for h, g in cells:
            j = g * 8 + h * 4 + t
            turned = f32_dot(ordered, mats_in[j], NT)
            last = jnp.concatenate([turned[:, LANES:], zeros], axis=1)
            shift = h * half + g * back_step
            if shift:
                last = pltpu.roll(last, shift, 1)
            tables[j] = jnp.concatenate([turned[:, :LANES], last], axis=1).astype(jnp.bfloat16)
        return carry

    lax.fori_loop(0, 4, prepare, 0)
    cross(1)
    pass_on(0, range(2))

    @pl.when(wave >= middle)
    def _():
        send(1, range(middle, wave_count))

    pass_on(0, range(2, len(planes)))

    come, go = grid_of((lev_count * LANES, wide), 0), grid_of((lev_count * LANES, wide), 1)
    p, lane = come // LANES, come % LANES
    h, lane = lane // half, lane % half
    g, lane = lane // fwd_step, lane % fwd_step
    target = h * LANES + g * rest_step + lane // short * extra + p * short + lane % short
    spread = ones_where((go == target) & (g < groups))

    loads[1].wait()
    row, col = grid_of((fields, layer_count), 0), grid_of((fields, layer_count), 1)
    chosen = ones_where(col == lev * lev_local + row // part_count)
    coupled_rows = f32_dot(chosen, coupler_in[...], NN)
    tops = jnp.concatenate([chosen.astype(jnp.float32), coupled_rows], axis=0)
    tops_part = lax.rem(grid_of(tops.shape, 0), part_count)
    keeps = [jnp.where(tops_part == c, tops, 0.0) for c in range(part_count)]
    pieces = [k[:, :LANES] for k in keeps] + [k[:, LANES:] for k in keeps]
    pieces.append(jnp.zeros((2 * fields, LANES - part_count * extra), jnp.float32))
    weights[...] = jnp.concatenate(pieces, axis=1).astype(jnp.bfloat16)

    for copy in loads[2:5]:
        copy.wait()
    gain = jnp.sum(
        jnp.where(col == lev * lev_local + row // part_count, strengths_in[...], 0.0),
        axis=1, keepdims=True,
    )
    n = grid_of((1, total_n), 1)
    scaled = (n * (n + 1)).astype(jnp.float32) / jnp.float32((total_n - 1) * total_n)
    damping = 1.0 / (1.0 + gain * scaled ** 2)
    spin_flat = spin_in.reshape(row_count, fields, total_n)
    vort_flat = vort_out.reshape(row_count, fields, total_n)
    for r in range(row_count):
        value = (spin_flat[r].astype(jnp.float32) * damping)
        value = jnp.where(n >= orders_in[:, r:r + 1], value, 0.0)
        vort_flat[r] = value.astype(jnp.bfloat16)


    @pl.when(wave < middle)
    def _():
        send(1, range(middle, wave_count))

    pass_on(1, range(len(planes)))
    lane = grid_of((wave_count, LANES), 1)
    near, mid, widths = range(1, 4), range(4, middle), (2, 1)
    parties = [
        [near, mid, *(range(i, i + width) for i in range(middle, wave_count, width))]
        for width in widths
    ]
    first_group = (0, len(parties[0]))

    def hand_over(ref, r, spot, target):
        pltpu.make_async_remote_copy(
            src_ref=ref, dst_ref=relayed.at[r, spot],
            send_sem=relay_send.at[r], recv_sem=relay_recv.at[r],
            device_id=(target, other), device_id_type=MESH,
        ).start()

    def give_back(r, masks):
        for mask in masks:
            copy = pltpu.make_async_remote_copy(
                src_ref=back_out.at[r, peer[mask]], dst_ref=back_in.at[r, wave],
                send_sem=back_send.at[r], recv_sem=back_recv.at[
                    first_group[r] + (
                        (mask >= 4) if mask < middle else 2 + lax.div(rank[mask], widths[r])
                    )
                ],
                device_id=(peer[mask], lev), device_id_type=MESH,
            )
            copy.start()
            if mask in near:
                hand_over(back_out.at[r, peer[mask]], r, wave, peer[mask])

    def await_group(r, group):
        party = parties[r][group]
        await_bytes(back_in.at[r, pl.ds(0, len(party))], back_recv.at[first_group[r] + group])

    def relay(r, masks):
        if masks[0]:
            await_group(r, parties[r].index(masks))
        for mask in masks:
            hand_over((back_in if mask else back_out).at[r, peer[mask]], r, peer[mask], wave)

    def solve_chunk(r):
        rows_in = by_rows(incoming[r])
        for q in range(lev_count):
            main = rows_in[pl.ds(q * wave_count, wave_count), :local_n]
            gathered[q] = main.astype(jnp.float32).reshape(block_n, LANES)
        if r == 0:
            rests = [
                rows_in[pl.ds(q * wave_count, wave_count), local_n:]
                .astype(jnp.float32).reshape(wave_count * 4, LANES)
                for q in range(lev_count)
            ]
            value = jnp.concatenate(rests, axis=1).astype(jnp.bfloat16)
            value = f32_dot(value, spread, NN)
            for h in range(2):
                rest_in[h] = value[:, h * LANES:(h + 1) * LANES]

        def solve(t, carry):
            every = pl.ds(t, wave_count, stride=4)
            lasts = None
            for h, g in cells:
                j = g * 8 + h * 4 + t
                rest = rest_in[h, every, :]
                rows = pl.ds(j, wave_count, stride=local_n)
                low, high = gathered[0, rows, :], gathered[1, rows, :]
                sides = [jnp.where(lane < half, low, high),
                         pltpu.roll(jnp.where(lane < half, high, low), half, 1)]
                stacked = []
                for c in range(part_count):
                    shift = g * rest_step + (r * part_count + c) * extra
                    moved = pltpu.roll(rest, LANES - shift, 1) if shift else rest
                    stacked.append(jnp.concatenate([sides[c], moved], axis=1)[:, :depth])
                stacked = jnp.concatenate(stacked, axis=0).astype(jnp.bfloat16)
                result = f32_dot(stacked, tables[j], NN)
                for c in range(part_count):
                    strided[c, rows, :] = result[c * wave_count:(c + 1) * wave_count, :LANES]
                last = result[:, LANES:]
                lasts = last if lasts is None else lasts + last
            total = lasts[:wave_count]
            for c in range(1, part_count):
                total += pltpu.roll(lasts[c * wave_count:(c + 1) * wave_count], c * extra, 1)
            rest_out[every, :] = total
            return carry

        lax.fori_loop(0, 4, solve, 0, unroll=4)
        rows_out = by_rows(back_out)
        for c in range(part_count):
            rows_out[r, :, c * local_n:(c + 1) * local_n] = (
                strided[c].reshape(wave_count, local_n, LANES).astype(jnp.bfloat16)
            )
        rows_out[r, :, part_count * local_n:] = (
            rest_out[...].reshape(wave_count, 4, LANES).astype(jnp.bfloat16)
        )
        relay(r, [0])
        give_back(r, range(1, wave_count if r == 0 else middle + 4))
        back_in[r, wave] = back_out[r, wave]

    heat_flat = heat_in.reshape(row_count, fields, total_n)
    div_flat = div_out.reshape(row_count, fields, total_n)
    temp_flat = temp_out.reshape(row_count, fields, total_n)

    def finish(r, wire, block):
        spots = pl.ds(pl.multiple_of(block * block_n, LANES), block_n)
        div_flat[r, :, spots], temp_flat[r, :, spots] = block_values(
            wire, weights, heat_flat, orders_in, r, block, block_n, back_step
        )

    loads[5].wait()
    for r in range(row_count):
        await_bytes(incoming[r].at[pl.ds(0, sources - 2)], fwd_recv.at[r])
        solve_chunk(r)
    def on_half(high, r):
        @pl.when((wave >= middle) if high else (wave < middle))
        def _():
            relay(r, mid)

    on_half(True, 0)
    give_back(1, [middle + 4])
    for i, party in enumerate(parties[0][2:]):
        relay(0, party)
        if i == 0:
            give_back(1, [middle + 5])
        if i == 1:
            give_back(1, range(middle + 6, wave_count))
            on_half(False, 0)
            on_half(True, 1)
    on_half(False, 1)
    for r in range(row_count):
        await_bytes(outgoing[r].at[pl.ds(0, sources - 1)], fwd_send.at[r])
        await_bytes(crossing[r].at[pl.ds(0, wave_count - 1)], pass_send.at[r])
    await_group(0, 0)
    finish(0, back_in, lev)
    for party in parties[1][2:]:
        relay(1, party)
    await_group(1, 0)
    finish(1, back_in, lev)
    for r in range(row_count):
        await_bytes(back_out.at[r, pl.ds(0, wave_count - 1)], back_send.at[r])
    for r in range(row_count):
        await_bytes(relayed.at[r], relay_recv.at[r])
        if r + 1 < row_count:
            finish(r, relayed, other)
    for r in range(row_count):
        await_bytes(relayed.at[r], relay_send.at[r])


def store_kernel(
    lev_count, step, vort, div, temp, wire, weights, heat, orders, vort_out, div_out, temp_out,
    div_last, temp_last, sems,
):
    row_count, lev_local, part_count, total_n = vort.shape
    block_n = total_n // lev_count
    last = row_count - 1
    lev = lax.axis_index("lev")
    mine, others = (
        pl.ds(pl.multiple_of(block * block_n, LANES), block_n)
        for block in (lev, lax.rem(lev + 1, lev_count))
    )
    pairs = [(vort, vort_out)]
    for src, dst in ((div, div_out), (temp, temp_out)):
        pairs += [(src.at[r], dst.at[r]) for r in range(last)]
        pairs.append((src.at[last, :, :, mine], dst.at[last, :, :, mine]))
    late = [(div_last, div_out.at[last, :, :, others]), (temp_last, temp_out.at[last, :, :, others])]
    copies = [
        pltpu.make_async_copy(src, dst, sems.at[i]) for i, (src, dst) in enumerate(pairs + late)
    ]
    for copy in copies[:len(pairs)]:
        copy.start()
    fields = lev_local * part_count
    values = block_values(
        wire, weights, heat.reshape(row_count, fields, total_n), orders, last,
        lax.rem(lev + 1, lev_count), block_n, step,
    )
    for ref, value in zip((div_last, temp_last), values):
        ref.reshape(fields, block_n)[...] = value
    for copy in copies[len(pairs):]:
        copy.start()
    for copy in copies:
        copy.wait()


def by_kernel(spin, source, heat, matrices, coupler, strengths, orders):
    lev_count, wave_count = lax.axis_size("lev"), lax.axis_size("wave")
    row_count, part_count, lev_local, total_n = source.shape
    block_n = total_n // lev_count
    local_n = block_n // wave_count
    layer_count = lev_local * lev_count
    fields = lev_local * part_count
    sources = wave_count * lev_count
    depth = -(-layer_count // 16) * 16
    anywhere, vmem = pl.BlockSpec(memory_space=pltpu.HBM), pl.BlockSpec(memory_space=pltpu.VMEM)
    shape = (row_count, lev_local, part_count, total_n)
    bf16, f32 = jnp.bfloat16, jnp.float32
    field = jax.ShapeDtypeStruct(shape, bf16)
    dma = pltpu.SemaphoreType.DMA
    main_pairs, rest_pairs = local_n // 2, 2
    wire_shape = (row_count, wave_count, part_count * main_pairs + rest_pairs, 2, LANES)
    wire = pltpu.VMEM(wire_shape, bf16)

    def first(count):
        return pltpu.VMEM((count, main_pairs + rest_pairs, 2, LANES), bf16)

    def following(count):
        return pltpu.VMEM((count, main_pairs, 2, LANES), bf16)

    each = dma((row_count,))
    outs = pl.pallas_call(
        functools.partial(step_kernel, wave_count, lev_count),
        out_shape=(
            field, field, field, jax.ShapeDtypeStruct(wire_shape, bf16),
            jax.ShapeDtypeStruct((2 * fields, 3 * LANES), bf16), field,
            jax.ShapeDtypeStruct((1, row_count), jnp.int32),
        ),
        in_specs=[anywhere] * 7,
        out_specs=(vmem,) * 7,
        scratch_shapes=[
            pltpu.VMEM(shape, bf16), pltpu.VMEM(shape, bf16),
            pltpu.VMEM(matrices.shape[1:], bf16), pltpu.VMEM(coupler.shape, bf16),
            pltpu.VMEM((1, layer_count), f32),
            first(sources), following(sources), first(sources), following(sources),
            first(wave_count), following(wave_count),
            pltpu.VMEM((lev_count, block_n, LANES), f32),
            pltpu.VMEM((2, wave_count * 4, LANES), f32),
            pltpu.VMEM((local_n, depth, 2 * LANES), bf16),
            pltpu.VMEM((part_count, block_n, LANES), f32),
            pltpu.VMEM((wave_count * 4, LANES), f32),
            wire, wire,
            dma((7,)), each, each, dma((row_count, wave_count // 4)), each,
            each, dma((4 + wave_count // 4 + wave_count // 2,)), each, each,
        ],
        compiler_params=pltpu.CompilerParams(
            collective_id=0, has_side_effects=True, vmem_limit_bytes=48 * 2**20
        ),
    )(
        *(
            pltpu.with_memory_space_constraint(value, pltpu.HBM)
            for value in (
                spin.transpose(0, 2, 1, 3), source.transpose(0, 2, 1, 3), heat.transpose(0, 2, 1, 3),
                matrices[0], coupler, strengths.reshape(1, layer_count), orders.reshape(1, row_count),
            )
        )
    )
    extra = layer_count - LANES
    last_block = pltpu.VMEM((lev_local, part_count, block_n), bf16)
    outs = pl.pallas_call(
        functools.partial(store_kernel, lev_count, part_count * extra),
        out_shape=(field,) * 3, in_specs=[vmem] * 7, out_specs=(anywhere,) * 3,
        scratch_shapes=[last_block, last_block, dma((2 * row_count + 3,))],
        compiler_params=pltpu.CompilerParams(vmem_limit_bytes=8 * 2**20),
    )(*outs)
    return tuple(out.transpose(0, 2, 1, 3) for out in outs)


def kernel_fits(source_shape, lev_count, wave_count):
    row_count, part_count, lev_local, total_n = source_shape
    block_n = total_n // lev_count
    extra = lev_local * lev_count - LANES
    half = LANES // 2
    groups = block_n // (8 * wave_count)
    return (
        lev_count == 2
        and part_count == 2
        and row_count == 2
        and wave_count > 8
        and wave_count & (wave_count - 1) == 0
        and wave_count % 8 == 0
        and block_n % LANES == 0
        and total_n % (2 * LANES) == 0
        and block_n % (8 * wave_count) == 0
        and extra > 0
        and extra * row_count * part_count * groups <= LANES
        and (lev_local - half) * row_count * part_count * groups <= half
        and extra * part_count * groups <= half
    )


def on_device(
    spin_tendency,
    spreading_source,
    heat_source,
    helmholtz_inverses,
    heat_spreading_coupler,
    smoothing_strengths,
    azimuthal_order_list,
):
    lev_count, wave_count = lax.axis_size("lev"), lax.axis_size("wave")
    lev_index = lax.axis_index("lev")
    lev_local, total_n = spreading_source.shape[2:]
    empty_placeholder = jnp.zeros((), jnp.bfloat16)
    if kernel_fits(spreading_source.shape, lev_count, wave_count):
        return by_kernel(
            spin_tendency, spreading_source, heat_source, helmholtz_inverses,
            heat_spreading_coupler, smoothing_strengths, azimuthal_order_list,
        )
    spreading_updated, coupled_out = exchange_by_collectives(
        spreading_source, helmholtz_inverses, heat_spreading_coupler
    )
    heat_updated = (heat_source.astype(jnp.float32) - coupled_out.astype(jnp.float32)).astype(
        jnp.bfloat16
    )
    level_gain = lax.dynamic_slice_in_dim(smoothing_strengths, lev_index * lev_local, lev_local)
    damping = damping_table(level_gain, jnp.arange(total_n, dtype=jnp.int32), total_n)
    spin_updated = (spin_tendency.astype(jnp.float32) * damping[None, None]).astype(jnp.bfloat16)
    interior_slice = (
        jnp.arange(total_n, dtype=jnp.int32)[None, :] >= azimuthal_order_list[:, None]
    )[:, None, None, :]
    return (
        jnp.where(interior_slice, spin_updated, empty_placeholder),
        jnp.where(interior_slice, spreading_updated, empty_placeholder),
        jnp.where(interior_slice, heat_updated, empty_placeholder),
    )


def solution(mesh):
    return jax.shard_map(
        on_device,
        mesh=mesh,
        in_specs=(
            P("wave", None, "lev", None),
            P("wave", None, "lev", None),
            P("wave", None, "lev", None),
            P("lev", "wave", None, None),
            P(),
            P(),
            P("wave"),
        ),
        out_specs=(
            P("wave", None, "lev", None),
            P("wave", None, "lev", None),
            P("wave", None, "lev", None),
        ),
        check_vma=False,
    )
```

```python
import functools
import jax
import jax.numpy as jnp
from jax import lax
from jax.experimental import pallas as pl
from jax.experimental.pallas import tpu as pltpu
from jax.sharding import PartitionSpec as P

LANES = 128
MESH = pl.DeviceIdType.MESH
NN = (((1,), (0,)), ((), ()))
NT = (((1,), (1,)), ((), ()))


def damping_table(level_gain, wavenumbers, total_n):
    scaled = (wavenumbers * (wavenumbers + 1)).astype(jnp.float32) / jnp.float32(
        (total_n - 1) * total_n
    )
    return 1.0 / (1.0 + level_gain[:, None] * scaled[None, :] ** 2)


def exchange_by_collectives(spreading_source, helmholtz_inverses, heat_spreading_coupler):
    lev_count = lax.axis_size("lev")
    row_count, part_count, lev_local, total_n = spreading_source.shape
    block_n = total_n // lev_count
    layer_count = lev_local * lev_count
    flat_rows = row_count * part_count
    wave_count = lax.axis_size("wave")
    local_n = block_n // wave_count
    rhs_div = lax.all_to_all(spreading_source, "lev", split_axis=3, concat_axis=2, tiled=True)
    outgoing = rhs_div.reshape(flat_rows, layer_count, wave_count, local_n).transpose(2, 3, 0, 1)
    outgoing = outgoing.reshape(wave_count, local_n, flat_rows * layer_count)
    columns = lax.all_to_all(outgoing, "wave", split_axis=0, concat_axis=0, tiled=True)
    columns = columns.reshape(wave_count, local_n, flat_rows, layer_count)
    solved_columns = jnp.einsum(
        "jkp,wjcp->wjck", helmholtz_inverses[0], columns, preferred_element_type=jnp.float32
    ).astype(jnp.bfloat16)
    solved_columns = solved_columns.reshape(wave_count, local_n, flat_rows * layer_count)
    returned = lax.all_to_all(solved_columns, "wave", split_axis=0, concat_axis=0, tiled=True)
    answer_fields = returned.reshape(block_n, flat_rows, layer_count).transpose(1, 2, 0)
    coupled = jnp.einsum(
        "om,dms->dos", heat_spreading_coupler, answer_fields, preferred_element_type=jnp.float32
    ).astype(jnp.bfloat16)
    both = jnp.stack([answer_fields, coupled])
    both = lax.all_to_all(both, "lev", split_axis=2, concat_axis=3, tiled=True)
    both = both.reshape(2, row_count, part_count, lev_local, total_n)
    spreading_updated, coupled_out = both[0], both[1]
    return spreading_updated, coupled_out


def f32_dot(left, right, dims):
    return lax.dot_general(left, right, dims, preferred_element_type=jnp.float32)


def grid_of(shape, axis):
    return lax.broadcasted_iota(jnp.int32, shape, axis)


def ones_where(condition, dtype=jnp.bfloat16):
    return jnp.where(condition, 1.0, 0.0).astype(dtype)


def flipped(value, mask):
    out, bit = value, 1
    while bit <= mask:
        if mask & bit:
            out = out + bit * (1 - 2 * lax.rem(lax.div(value, bit), 2))
        bit *= 2
    return out


def by_rows(ref):
    return ref.reshape(*ref.shape[:-3], ref.shape[-3] * 2, LANES)


def block_values(wire, weights, heat_flat, orders, r, block, block_n, step):
    wave_count = wire.shape[1]
    local_n = block_n // wave_count
    groups = local_n // 8
    fields = heat_flat.shape[1]
    rows_in = by_rows(wire)
    parts = (rows_in.shape[2] - 4) // local_n
    sides = [
        rows_in[r, :, c * local_n:(c + 1) * local_n].astype(jnp.float32).reshape(block_n, LANES)
        for c in range(parts)
    ]
    folded = rows_in[r, :, parts * local_n:].astype(jnp.float32)
    swung = pltpu.roll(folded.reshape(wave_count * 4, LANES), LANES // 2, 1)
    folded = jnp.concatenate([folded, swung.reshape(wave_count, 4, LANES)], axis=1)
    folded = folded.reshape(wave_count * 8, LANES)
    rest = [(pltpu.roll(folded, LANES - g * step, 1) if g else folded)
            .reshape(wave_count, 1, 8, LANES) for g in range(groups)]
    sides.append(jnp.concatenate(rest, axis=1).reshape(block_n, LANES))
    packed = jnp.concatenate(sides, axis=1).astype(jnp.bfloat16)
    result = f32_dot(weights[...], packed, NT)
    spots = pl.ds(pl.multiple_of(block * block_n, LANES), block_n)
    inside = block * block_n + grid_of((1, block_n), 1) >= orders[:, r:r + 1]
    coupled = result[fields:].astype(jnp.bfloat16).astype(jnp.float32)
    warmed = heat_flat[r, :, spots].astype(jnp.float32) - coupled
    return (
        jnp.where(inside, result[:fields], 0.0).astype(jnp.bfloat16),
        jnp.where(inside, warmed, 0.0).astype(jnp.bfloat16),
    )


def step_kernel(
    wave_count, lev_count, spin, source, heat, matrices, coupler, strengths, orders,
    vort_out, div_out, temp_out, relayed, weights, heat_in, orders_in,
    spin_in, source_in, mats_in, coupler_in, strengths_in,
    first_out, next_out, first_in, next_in, first_lev, next_lev, gathered, rest_in, tables, strided, rest_out,
    back_out, back_in,
    load_sem, fwd_send, fwd_recv, lev_recv, pass_send, back_send, back_recv, relay_send, relay_recv,
):
    wave, lev = lax.axis_index("wave"), lax.axis_index("lev")
    row_count, lev_local, part_count, total_n = source.shape
    block_n = total_n // lev_count
    local_n = block_n // wave_count
    groups = local_n // 8
    layer_count = lev_local * lev_count
    fields = lev_local * part_count
    half = LANES // part_count
    short = lev_local - half
    extra = layer_count - LANES
    depth = tables.shape[1]
    sources = wave_count * lev_count
    wide = 2 * LANES
    cells = [(h, g) for h in range(2) for g in range(groups)]
    fwd_step = row_count * part_count * short
    back_step = part_count * extra
    rest_step = row_count * part_count * extra

    middle = wave_count // 2
    block = lax.rem(wave, 4)
    across = middle * (1 - lax.div(wave, middle))
    flips = [flipped(wave, mask) for mask in range(wave_count)]
    peer = flips[:middle]
    peer += [across + i // 4 * 4 + flipped(block, i % 4) for i in range(middle)]
    rank = [*range(middle), *(lax.div(lax.rem(wave, middle), 4) * 4 + i % 4 for i in range(middle))]
    other = lax.rem(lev + 1, lev_count)
    outward = [*range(1, wave_count), 0]
    barrier = pltpu.get_barrier_semaphore()

    def greet(masks):
        for mask in masks:
            for t, q in enumerate((lev, other)):
                if mask or t:
                    pl.semaphore_signal(
                        barrier, inc=1, device_id=(flips[mask], q), device_id_type=MESH
                    )

    greet(range(wave_count - 1, middle - 1, -1))
    loads = []
    small = [(matrices, mats_in), (coupler, coupler_in), (strengths, strengths_in),
             (orders, orders_in), (spin, spin_in), (heat, heat_in)]
    for i, (src, dst) in enumerate(
        [(source, source_in), *small]
    ):
        copy = pltpu.make_async_copy(src, dst, load_sem.at[i])
        copy.start()
        loads.append(copy)
    source_load, loads = loads[0], loads[1:]

    greet(range(middle - 1, -1, -1))

    out_row, in_row = grid_of((wide, fields), 0), grid_of((wide, fields), 1)
    level, part = in_row // part_count, in_row % part_count
    main_spot = lax.rem(part + lev, part_count) * half + level
    main_pick = ones_where(
        (out_row == main_spot)[:LANES] & (level < half)[:LANES]
    )
    rest_picks = [
        ones_where(
            (out_row == (r * part_count + part) * short + level - half)[:LANES]
            & (level >= half)[:LANES]
        )
        for r in range(row_count)
    ]
    eye = ones_where(grid_of((wide, wide), 0) == grid_of((wide, wide), 1))
    flat = source_in.reshape(row_count, fields, total_n)
    mine = lev * wave_count + wave

    def turn(rows):
        return jnp.concatenate(
            [f32_dot(eye, rows[:, k:k + wide], NT) for k in range(0, total_n, wide)], axis=0
        )

    outgoing, incoming = [first_out, next_out], [first_in, next_in]

    def await_bytes(ref, sem):
        pltpu.make_async_copy(ref, ref, sem).wait()

    crossing = [first_lev, next_lev]
    home = middle - across
    planes = [across + i for i in range(0, middle, 4)]
    planes += [home + lax.rem(lax.rem(wave - block - home, middle) + i, middle)
               for i in range(4, middle, 4)]
    planes += [wave - block]

    def cross(r):
        for i, plane in enumerate(planes):
            pltpu.make_async_remote_copy(
                src_ref=outgoing[r].at[pl.ds(other * wave_count + plane, 4)],
                dst_ref=crossing[r].at[pl.ds(plane, 4)],
                send_sem=fwd_send.at[r], recv_sem=lev_recv.at[r, i],
                device_id=(wave, other), device_id_type=MESH,
            ).start()

    def send(r, masks):
        for mask in masks:
            pltpu.make_async_remote_copy(
                src_ref=outgoing[r].at[lev * wave_count + flips[mask]],
                dst_ref=incoming[r].at[mine],
                send_sem=fwd_send.at[r], recv_sem=fwd_recv.at[r],
                device_id=(flips[mask], lev), device_id_type=MESH,
            ).start()

    def pass_on(r, which):
        for i in which:
            plane = planes[i]
            await_bytes(crossing[r].at[pl.ds(0, 4)], lev_recv.at[r, i])
            last = i == len(planes) - 1
            for k in range(1 if last else 0, 4):
                target = plane + flipped(block, k)
                pltpu.make_async_remote_copy(
                    src_ref=crossing[r].at[target],
                    dst_ref=incoming[r].at[other * wave_count + wave],
                    send_sem=pass_send.at[r], recv_sem=fwd_recv.at[r],
                    device_id=(target, lev), device_id_type=MESH,
                ).start()
            if last:
                incoming[r][other * wave_count + wave] = crossing[r][wave]

    source_load.wait()
    main = f32_dot(main_pick, flat[0], NN)
    rest = f32_dot(rest_picks[0], flat[0], NN)
    for r in range(1, row_count):
        rest += f32_dot(rest_picks[r], flat[r], NN)
    turned = turn(jnp.concatenate([main, rest], axis=0).astype(jnp.bfloat16))
    tail = turned[:, LANES:].reshape(sources, groups, 8, LANES)
    folded = tail[:, 0].reshape(sources * 8, LANES)
    for g in range(1, groups):
        folded += pltpu.roll(tail[:, g].reshape(sources * 8, LANES), g * fwd_step, 1)
    swung = pltpu.roll(folded, half, 1).reshape(sources, 8, LANES)
    folded = folded.reshape(sources, 8, LANES)[:, :4] + swung[:, 4:]
    by_rows(first_out)[:, :local_n] = (
        turned[:, :LANES].reshape(sources, local_n, LANES).astype(jnp.bfloat16)
    )
    by_rows(first_out)[:, local_n:] = folded.astype(jnp.bfloat16)
    pl.semaphore_wait(barrier, sources - 1)
    cross(0)
    send(0, range(1, wave_count))
    incoming[0][mine] = outgoing[0][mine]
    for r in range(1, row_count):
        turned = turn(f32_dot(main_pick, flat[r], NN).astype(jnp.bfloat16))
        by_rows(next_out)[...] = turned.reshape(sources, local_n, LANES).astype(jnp.bfloat16)
        send(r, range(1, middle))
        incoming[r][mine] = outgoing[r][mine]

    loads[0].wait()
    deep, flat_level = grid_of((depth, layer_count), 0), grid_of((depth, layer_count), 1)
    owner, place = flat_level // lev_local, flat_level % lev_local
    spot = jnp.where(place < half, owner * half + place, LANES + owner * short + place - half)
    ordered = ones_where(deep == spot)
    zeros = jnp.zeros((depth, LANES - extra), jnp.float32)

    def prepare(t, carry):
        for h, g in cells:
            j = g * 8 + h * 4 + t
            turned = f32_dot(ordered, mats_in[j], NT)
            last = jnp.concatenate([turned[:, LANES:], zeros], axis=1)
            shift = h * half + g * back_step
            if shift:
                last = pltpu.roll(last, shift, 1)
            tables[j] = jnp.concatenate([turned[:, :LANES], last], axis=1).astype(jnp.bfloat16)
        return carry

    lax.fori_loop(0, 4, prepare, 0)
    cross(1)
    pass_on(0, range(2))

    @pl.when(wave >= middle)
    def _():
        send(1, range(middle, wave_count))

    pass_on(0, range(2, len(planes)))

    come, go = grid_of((lev_count * LANES, wide), 0), grid_of((lev_count * LANES, wide), 1)
    p, lane = come // LANES, come % LANES
    h, lane = lane // half, lane % half
    g, lane = lane // fwd_step, lane % fwd_step
    target = h * LANES + g * rest_step + lane // short * extra + p * short + lane % short
    spread = ones_where((go == target) & (g < groups))

    loads[1].wait()
    row, col = grid_of((fields, layer_count), 0), grid_of((fields, layer_count), 1)
    chosen = ones_where(col == lev * lev_local + row // part_count)
    coupled_rows = f32_dot(chosen, coupler_in[...], NN)
    tops = jnp.concatenate([chosen.astype(jnp.float32), coupled_rows], axis=0)
    tops_part = lax.rem(grid_of(tops.shape, 0), part_count)
    keeps = [jnp.where(tops_part == c, tops, 0.0) for c in range(part_count)]
    pieces = [k[:, :LANES] for k in keeps] + [k[:, LANES:] for k in keeps]
    pieces.append(jnp.zeros((2 * fields, LANES - part_count * extra), jnp.float32))
    weights[...] = jnp.concatenate(pieces, axis=1).astype(jnp.bfloat16)

    for copy in loads[2:5]:
        copy.wait()
    gain = jnp.sum(
        jnp.where(col == lev * lev_local + row // part_count, strengths_in[...], 0.0),
        axis=1, keepdims=True,
    )
    n = grid_of((1, total_n), 1)
    scaled = (n * (n + 1)).astype(jnp.float32) / jnp.float32((total_n - 1) * total_n)
    damping = 1.0 / (1.0 + gain * scaled ** 2)
    spin_flat = spin_in.reshape(row_count, fields, total_n)
    vort_flat = vort_out.reshape(row_count, fields, total_n)
    for r in range(row_count):
        value = (spin_flat[r].astype(jnp.float32) * damping)
        value = jnp.where(n >= orders_in[:, r:r + 1], value, 0.0)
        vort_flat[r] = value.astype(jnp.bfloat16)


    @pl.when(wave < middle)
    def _():
        send(1, range(middle, wave_count))

    pass_on(1, range(len(planes)))
    lane = grid_of((wave_count, LANES), 1)
    near, mid, widths = range(1, 4), range(4, middle), (2, 1)
    parties = [
        [near, mid, *(range(i, i + width) for i in range(middle, wave_count, width))]
        for width in widths
    ]
    first_group = (0, len(parties[0]))

    def hand_over(ref, r, spot, target):
        pltpu.make_async_remote_copy(
            src_ref=ref, dst_ref=relayed.at[r, spot],
            send_sem=relay_send.at[r], recv_sem=relay_recv.at[r],
            device_id=(target, other), device_id_type=MESH,
        ).start()

    def give_back(r, masks):
        for mask in masks:
            copy = pltpu.make_async_remote_copy(
                src_ref=back_out.at[r, peer[mask]], dst_ref=back_in.at[r, wave],
                send_sem=back_send.at[r], recv_sem=back_recv.at[
                    first_group[r] + (
                        (mask >= 4) if mask < middle else 2 + lax.div(rank[mask], widths[r])
                    )
                ],
                device_id=(peer[mask], lev), device_id_type=MESH,
            )
            copy.start()
            if mask in near:
                hand_over(back_out.at[r, peer[mask]], r, wave, peer[mask])

    def await_group(r, group):
        party = parties[r][group]
        await_bytes(back_in.at[r, pl.ds(0, len(party))], back_recv.at[first_group[r] + group])

    def relay(r, masks):
        if masks[0]:
            await_group(r, parties[r].index(masks))
        for mask in masks:
            hand_over((back_in if mask else back_out).at[r, peer[mask]], r, peer[mask], wave)

    def solve_chunk(r):
        rows_in = by_rows(incoming[r])
        for q in range(lev_count):
            main = rows_in[pl.ds(q * wave_count, wave_count), :local_n]
            gathered[q] = main.astype(jnp.float32).reshape(block_n, LANES)
        if r == 0:
            rests = [
                rows_in[pl.ds(q * wave_count, wave_count), local_n:]
                .astype(jnp.float32).reshape(wave_count * 4, LANES)
                for q in range(lev_count)
            ]
            value = jnp.concatenate(rests, axis=1).astype(jnp.bfloat16)
            value = f32_dot(value, spread, NN)
            for h in range(2):
                rest_in[h] = value[:, h * LANES:(h + 1) * LANES]

        def solve(t, carry):
            every = pl.ds(t, wave_count, stride=4)
            lasts = None
            for h, g in cells:
                j = g * 8 + h * 4 + t
                rest = rest_in[h, every, :]
                rows = pl.ds(j, wave_count, stride=local_n)
                low, high = gathered[0, rows, :], gathered[1, rows, :]
                sides = [jnp.where(lane < half, low, high),
                         pltpu.roll(jnp.where(lane < half, high, low), half, 1)]
                stacked = []
                for c in range(part_count):
                    shift = g * rest_step + (r * part_count + c) * extra
                    moved = pltpu.roll(rest, LANES - shift, 1) if shift else rest
                    stacked.append(jnp.concatenate([sides[c], moved], axis=1)[:, :depth])
                stacked = jnp.concatenate(stacked, axis=0).astype(jnp.bfloat16)
                result = f32_dot(stacked, tables[j], NN)
                for c in range(part_count):
                    strided[c, rows, :] = result[c * wave_count:(c + 1) * wave_count, :LANES]
                last = result[:, LANES:]
                lasts = last if lasts is None else lasts + last
            total = lasts[:wave_count]
            for c in range(1, part_count):
                total += pltpu.roll(lasts[c * wave_count:(c + 1) * wave_count], c * extra, 1)
            rest_out[every, :] = total
            return carry

        lax.fori_loop(0, 4, solve, 0, unroll=4)
        rows_out = by_rows(back_out)
        for c in range(part_count):
            rows_out[r, :, c * local_n:(c + 1) * local_n] = (
                strided[c].reshape(wave_count, local_n, LANES).astype(jnp.bfloat16)
            )
        rows_out[r, :, part_count * local_n:] = (
            rest_out[...].reshape(wave_count, 4, LANES).astype(jnp.bfloat16)
        )
        relay(r, [0])
        give_back(r, range(1, wave_count if r == 0 else middle + 4))
        back_in[r, wave] = back_out[r, wave]

    heat_flat = heat_in.reshape(row_count, fields, total_n)
    div_flat = div_out.reshape(row_count, fields, total_n)
    temp_flat = temp_out.reshape(row_count, fields, total_n)

    def finish(r, wire, block):
        spots = pl.ds(pl.multiple_of(block * block_n, LANES), block_n)
        div_flat[r, :, spots], temp_flat[r, :, spots] = block_values(
            wire, weights, heat_flat, orders_in, r, block, block_n, back_step
        )

    loads[5].wait()
    for r in range(row_count):
        await_bytes(incoming[r].at[pl.ds(0, sources - 2)], fwd_recv.at[r])
        solve_chunk(r)
    def mid_if(condition, r):
        @pl.when(condition)
        def _():
            relay(r, mid)

    mid_if(wave >= 4, 0)
    give_back(1, [middle + 4])
    for i, party in enumerate(parties[0][2:]):
        relay(0, party)
        if i == 0:
            give_back(1, [middle + 5])
        if i == 1:
            give_back(1, range(middle + 6, wave_count))
            mid_if(wave >= middle, 1)
        if i == 2:
            mid_if(wave < 4, 0)
    mid_if(wave < middle, 1)
    for r in range(row_count):
        await_bytes(outgoing[r].at[pl.ds(0, sources - 1)], fwd_send.at[r])
        await_bytes(crossing[r].at[pl.ds(0, wave_count - 1)], pass_send.at[r])
    await_group(0, 0)
    finish(0, back_in, lev)
    for party in parties[1][2:]:
        relay(1, party)
    await_group(1, 0)
    finish(1, back_in, lev)
    for r in range(row_count):
        await_bytes(back_out.at[r, pl.ds(0, wave_count - 1)], back_send.at[r])
    for r in range(row_count):
        await_bytes(relayed.at[r], relay_recv.at[r])
        if r + 1 < row_count:
            finish(r, relayed, other)
    for r in range(row_count):
        await_bytes(relayed.at[r], relay_send.at[r])


def store_kernel(
    lev_count, step, vort, div, temp, wire, weights, heat, orders, vort_out, div_out, temp_out,
    div_last, temp_last, sems,
):
    row_count, lev_local, part_count, total_n = vort.shape
    block_n = total_n // lev_count
    last = row_count - 1
    lev = lax.axis_index("lev")
    mine, others = (
        pl.ds(pl.multiple_of(block * block_n, LANES), block_n)
        for block in (lev, lax.rem(lev + 1, lev_count))
    )
    pairs = [(vort, vort_out)]
    for src, dst in ((div, div_out), (temp, temp_out)):
        pairs += [(src.at[r], dst.at[r]) for r in range(last)]
        pairs.append((src.at[last, :, :, mine], dst.at[last, :, :, mine]))
    late = [(div_last, div_out.at[last, :, :, others]), (temp_last, temp_out.at[last, :, :, others])]
    copies = [
        pltpu.make_async_copy(src, dst, sems.at[i]) for i, (src, dst) in enumerate(pairs + late)
    ]
    for copy in copies[:len(pairs)]:
        copy.start()
    fields = lev_local * part_count
    values = block_values(
        wire, weights, heat.reshape(row_count, fields, total_n), orders, last,
        lax.rem(lev + 1, lev_count), block_n, step,
    )
    for ref, value in zip((div_last, temp_last), values):
        ref.reshape(fields, block_n)[...] = value
    for copy in copies[len(pairs):]:
        copy.start()
    for copy in copies:
        copy.wait()


def by_kernel(spin, source, heat, matrices, coupler, strengths, orders):
    lev_count, wave_count = lax.axis_size("lev"), lax.axis_size("wave")
    row_count, part_count, lev_local, total_n = source.shape
    block_n = total_n // lev_count
    local_n = block_n // wave_count
    layer_count = lev_local * lev_count
    fields = lev_local * part_count
    sources = wave_count * lev_count
    depth = -(-layer_count // 16) * 16
    anywhere, vmem = pl.BlockSpec(memory_space=pltpu.HBM), pl.BlockSpec(memory_space=pltpu.VMEM)
    shape = (row_count, lev_local, part_count, total_n)
    bf16, f32 = jnp.bfloat16, jnp.float32
    field = jax.ShapeDtypeStruct(shape, bf16)
    dma = pltpu.SemaphoreType.DMA
    main_pairs, rest_pairs = local_n // 2, 2
    wire_shape = (row_count, wave_count, part_count * main_pairs + rest_pairs, 2, LANES)
    wire = pltpu.VMEM(wire_shape, bf16)

    def first(count):
        return pltpu.VMEM((count, main_pairs + rest_pairs, 2, LANES), bf16)

    def following(count):
        return pltpu.VMEM((count, main_pairs, 2, LANES), bf16)

    each = dma((row_count,))
    outs = pl.pallas_call(
        functools.partial(step_kernel, wave_count, lev_count),
        out_shape=(
            field, field, field, jax.ShapeDtypeStruct(wire_shape, bf16),
            jax.ShapeDtypeStruct((2 * fields, 3 * LANES), bf16), field,
            jax.ShapeDtypeStruct((1, row_count), jnp.int32),
        ),
        in_specs=[anywhere] * 7,
        out_specs=(vmem,) * 7,
        scratch_shapes=[
            pltpu.VMEM(shape, bf16), pltpu.VMEM(shape, bf16),
            pltpu.VMEM(matrices.shape[1:], bf16), pltpu.VMEM(coupler.shape, bf16),
            pltpu.VMEM((1, layer_count), f32),
            first(sources), following(sources), first(sources), following(sources),
            first(wave_count), following(wave_count),
            pltpu.VMEM((lev_count, block_n, LANES), f32),
            pltpu.VMEM((2, wave_count * 4, LANES), f32),
            pltpu.VMEM((local_n, depth, 2 * LANES), bf16),
            pltpu.VMEM((part_count, block_n, LANES), f32),
            pltpu.VMEM((wave_count * 4, LANES), f32),
            wire, wire,
            dma((7,)), each, each, dma((row_count, wave_count // 4)), each,
            each, dma((4 + wave_count // 4 + wave_count // 2,)), each, each,
        ],
        compiler_params=pltpu.CompilerParams(
            collective_id=0, has_side_effects=True, vmem_limit_bytes=48 * 2**20
        ),
    )(
        *(
            pltpu.with_memory_space_constraint(value, pltpu.HBM)
            for value in (
                spin.transpose(0, 2, 1, 3), source.transpose(0, 2, 1, 3), heat.transpose(0, 2, 1, 3),
                matrices[0], coupler, strengths.reshape(1, layer_count), orders.reshape(1, row_count),
            )
        )
    )
    extra = layer_count - LANES
    last_block = pltpu.VMEM((lev_local, part_count, block_n), bf16)
    outs = pl.pallas_call(
        functools.partial(store_kernel, lev_count, part_count * extra),
        out_shape=(field,) * 3, in_specs=[vmem] * 7, out_specs=(anywhere,) * 3,
        scratch_shapes=[last_block, last_block, dma((2 * row_count + 3,))],
        compiler_params=pltpu.CompilerParams(vmem_limit_bytes=8 * 2**20),
    )(*outs)
    return tuple(out.transpose(0, 2, 1, 3) for out in outs)


def kernel_fits(source_shape, lev_count, wave_count):
    row_count, part_count, lev_local, total_n = source_shape
    block_n = total_n // lev_count
    extra = lev_local * lev_count - LANES
    half = LANES // 2
    groups = block_n // (8 * wave_count)
    return (
        lev_count == 2
        and part_count == 2
        and row_count == 2
        and wave_count > 8
        and wave_count & (wave_count - 1) == 0
        and wave_count % 8 == 0
        and block_n % LANES == 0
        and total_n % (2 * LANES) == 0
        and block_n % (8 * wave_count) == 0
        and extra > 0
        and extra * row_count * part_count * groups <= LANES
        and (lev_local - half) * row_count * part_count * groups <= half
        and extra * part_count * groups <= half
    )


def on_device(
    spin_tendency,
    spreading_source,
    heat_source,
    helmholtz_inverses,
    heat_spreading_coupler,
    smoothing_strengths,
    azimuthal_order_list,
):
    lev_count, wave_count = lax.axis_size("lev"), lax.axis_size("wave")
    lev_index = lax.axis_index("lev")
    lev_local, total_n = spreading_source.shape[2:]
    empty_placeholder = jnp.zeros((), jnp.bfloat16)
    if kernel_fits(spreading_source.shape, lev_count, wave_count):
        return by_kernel(
            spin_tendency, spreading_source, heat_source, helmholtz_inverses,
            heat_spreading_coupler, smoothing_strengths, azimuthal_order_list,
        )
    spreading_updated, coupled_out = exchange_by_collectives(
        spreading_source, helmholtz_inverses, heat_spreading_coupler
    )
    heat_updated = (heat_source.astype(jnp.float32) - coupled_out.astype(jnp.float32)).astype(
        jnp.bfloat16
    )
    level_gain = lax.dynamic_slice_in_dim(smoothing_strengths, lev_index * lev_local, lev_local)
    damping = damping_table(level_gain, jnp.arange(total_n, dtype=jnp.int32), total_n)
    spin_updated = (spin_tendency.astype(jnp.float32) * damping[None, None]).astype(jnp.bfloat16)
    interior_slice = (
        jnp.arange(total_n, dtype=jnp.int32)[None, :] >= azimuthal_order_list[:, None]
    )[:, None, None, :]
    return (
        jnp.where(interior_slice, spin_updated, empty_placeholder),
        jnp.where(interior_slice, spreading_updated, empty_placeholder),
        jnp.where(interior_slice, heat_updated, empty_placeholder),
    )


def solution(mesh):
    return jax.shard_map(
        on_device,
        mesh=mesh,
        in_specs=(
            P("wave", None, "lev", None),
            P("wave", None, "lev", None),
            P("wave", None, "lev", None),
            P("lev", "wave", None, None),
            P(),
            P(),
            P("wave"),
        ),
        out_specs=(
            P("wave", None, "lev", None),
            P("wave", None, "lev", None),
            P("wave", None, "lev", None),
        ),
        check_vma=False,
    )
```

```python
import functools
import jax
import jax.numpy as jnp
from jax import lax
from jax.experimental import pallas as pl
from jax.experimental.pallas import tpu as pltpu
from jax.sharding import PartitionSpec as P

LANES = 128
MESH = pl.DeviceIdType.MESH
NN = (((1,), (0,)), ((), ()))
NT = (((1,), (1,)), ((), ()))


def damping_table(level_gain, wavenumbers, total_n):
    scaled = (wavenumbers * (wavenumbers + 1)).astype(jnp.float32) / jnp.float32(
        (total_n - 1) * total_n
    )
    return 1.0 / (1.0 + level_gain[:, None] * scaled[None, :] ** 2)


def exchange_by_collectives(spreading_source, helmholtz_inverses, heat_spreading_coupler):
    lev_count = lax.axis_size("lev")
    row_count, part_count, lev_local, total_n = spreading_source.shape
    block_n = total_n // lev_count
    layer_count = lev_local * lev_count
    flat_rows = row_count * part_count
    wave_count = lax.axis_size("wave")
    local_n = block_n // wave_count
    rhs_div = lax.all_to_all(spreading_source, "lev", split_axis=3, concat_axis=2, tiled=True)
    outgoing = rhs_div.reshape(flat_rows, layer_count, wave_count, local_n).transpose(2, 3, 0, 1)
    outgoing = outgoing.reshape(wave_count, local_n, flat_rows * layer_count)
    columns = lax.all_to_all(outgoing, "wave", split_axis=0, concat_axis=0, tiled=True)
    columns = columns.reshape(wave_count, local_n, flat_rows, layer_count)
    solved_columns = jnp.einsum(
        "jkp,wjcp->wjck", helmholtz_inverses[0], columns, preferred_element_type=jnp.float32
    ).astype(jnp.bfloat16)
    solved_columns = solved_columns.reshape(wave_count, local_n, flat_rows * layer_count)
    returned = lax.all_to_all(solved_columns, "wave", split_axis=0, concat_axis=0, tiled=True)
    answer_fields = returned.reshape(block_n, flat_rows, layer_count).transpose(1, 2, 0)
    coupled = jnp.einsum(
        "om,dms->dos", heat_spreading_coupler, answer_fields, preferred_element_type=jnp.float32
    ).astype(jnp.bfloat16)
    both = jnp.stack([answer_fields, coupled])
    both = lax.all_to_all(both, "lev", split_axis=2, concat_axis=3, tiled=True)
    both = both.reshape(2, row_count, part_count, lev_local, total_n)
    spreading_updated, coupled_out = both[0], both[1]
    return spreading_updated, coupled_out


def f32_dot(left, right, dims):
    return lax.dot_general(left, right, dims, preferred_element_type=jnp.float32)


def grid_of(shape, axis):
    return lax.broadcasted_iota(jnp.int32, shape, axis)


def ones_where(condition, dtype=jnp.bfloat16):
    return jnp.where(condition, 1.0, 0.0).astype(dtype)


def flipped(value, mask):
    out, bit = value, 1
    while bit <= mask:
        if mask & bit:
            out = out + bit * (1 - 2 * lax.rem(lax.div(value, bit), 2))
        bit *= 2
    return out


def by_rows(ref):
    return ref.reshape(*ref.shape[:-3], ref.shape[-3] * 2, LANES)


def block_values(wire, weights, heat_flat, orders, r, block, block_n, step):
    wave_count = wire.shape[1]
    local_n = block_n // wave_count
    groups = local_n // 8
    fields = heat_flat.shape[1]
    rows_in = by_rows(wire)
    parts = (rows_in.shape[2] - 4) // local_n
    sides = [
        rows_in[r, :, c * local_n:(c + 1) * local_n].astype(jnp.float32).reshape(block_n, LANES)
        for c in range(parts)
    ]
    folded = rows_in[r, :, parts * local_n:].astype(jnp.float32)
    swung = pltpu.roll(folded.reshape(wave_count * 4, LANES), LANES // 2, 1)
    folded = jnp.concatenate([folded, swung.reshape(wave_count, 4, LANES)], axis=1)
    folded = folded.reshape(wave_count * 8, LANES)
    rest = [(pltpu.roll(folded, LANES - g * step, 1) if g else folded)
            .reshape(wave_count, 1, 8, LANES) for g in range(groups)]
    sides.append(jnp.concatenate(rest, axis=1).reshape(block_n, LANES))
    packed = jnp.concatenate(sides, axis=1).astype(jnp.bfloat16)
    result = f32_dot(weights[...], packed, NT)
    spots = pl.ds(pl.multiple_of(block * block_n, LANES), block_n)
    inside = block * block_n + grid_of((1, block_n), 1) >= orders[:, r:r + 1]
    coupled = result[fields:].astype(jnp.bfloat16).astype(jnp.float32)
    warmed = heat_flat[r, :, spots].astype(jnp.float32) - coupled
    return (
        jnp.where(inside, result[:fields], 0.0).astype(jnp.bfloat16),
        jnp.where(inside, warmed, 0.0).astype(jnp.bfloat16),
    )


def step_kernel(
    wave_count, lev_count, spin, source, heat, matrices, coupler, strengths, orders,
    vort_out, div_out, temp_out, relayed, weights, heat_in, orders_in,
    spin_in, source_in, mats_in, coupler_in, strengths_in,
    first_out, next_out, first_in, next_in, first_lev, next_lev, gathered, rest_in, tables, strided, rest_out,
    back_out, back_in,
    load_sem, fwd_send, fwd_recv, lev_recv, pass_send, back_send, back_recv, relay_send, relay_recv,
):
    wave, lev = lax.axis_index("wave"), lax.axis_index("lev")
    row_count, lev_local, part_count, total_n = source.shape
    block_n = total_n // lev_count
    local_n = block_n // wave_count
    groups = local_n // 8
    layer_count = lev_local * lev_count
    fields = lev_local * part_count
    half = LANES // part_count
    short = lev_local - half
    extra = layer_count - LANES
    depth = tables.shape[1]
    sources = wave_count * lev_count
    wide = 2 * LANES
    cells = [(h, g) for h in range(2) for g in range(groups)]
    fwd_step = row_count * part_count * short
    back_step = part_count * extra
    rest_step = row_count * part_count * extra

    middle = wave_count // 2
    block = lax.rem(wave, 4)
    across = middle * (1 - lax.div(wave, middle))
    flips = [flipped(wave, mask) for mask in range(wave_count)]
    peer = flips[:middle]
    side, core = lax.div(block, 2), lax.rem(block, 2)
    peer += [across + i // 2 * 2 + flipped(core, i % 2) for i in range(middle)]
    rank = [
        lax.div(lax.rem(wave, middle), 4) * 4 + side * 2 + i % 2 for i in range(middle)
    ]
    rank = [*range(middle), *rank]
    other = lax.rem(lev + 1, lev_count)
    outward = [*range(1, wave_count), 0]
    barrier = pltpu.get_barrier_semaphore()

    def greet(masks):
        for mask in masks:
            for t, q in enumerate((lev, other)):
                if mask or t:
                    pl.semaphore_signal(
                        barrier, inc=1, device_id=(flips[mask], q), device_id_type=MESH
                    )

    greet(range(wave_count - 1, middle - 1, -1))
    loads = []
    small = [(matrices, mats_in), (coupler, coupler_in), (strengths, strengths_in),
             (orders, orders_in), (spin, spin_in), (heat, heat_in)]
    for i, (src, dst) in enumerate(
        [(source, source_in), *small]
    ):
        copy = pltpu.make_async_copy(src, dst, load_sem.at[i])
        copy.start()
        loads.append(copy)
    source_load, loads = loads[0], loads[1:]

    greet(range(middle - 1, -1, -1))

    out_row, in_row = grid_of((wide, fields), 0), grid_of((wide, fields), 1)
    level, part = in_row // part_count, in_row % part_count
    main_spot = lax.rem(part + lev, part_count) * half + level
    main_pick = ones_where(
        (out_row == main_spot)[:LANES] & (level < half)[:LANES]
    )
    rest_picks = [
        ones_where(
            (out_row == (r * part_count + part) * short + level - half)[:LANES]
            & (level >= half)[:LANES]
        )
        for r in range(row_count)
    ]
    eye = ones_where(grid_of((wide, wide), 0) == grid_of((wide, wide), 1))
    flat = source_in.reshape(row_count, fields, total_n)
    mine = lev * wave_count + wave

    def turn(rows):
        return jnp.concatenate(
            [f32_dot(eye, rows[:, k:k + wide], NT) for k in range(0, total_n, wide)], axis=0
        )

    outgoing, incoming = [first_out, next_out], [first_in, next_in]

    def await_bytes(ref, sem):
        pltpu.make_async_copy(ref, ref, sem).wait()

    crossing = [first_lev, next_lev]
    home = middle - across
    planes = [across + i for i in range(0, middle, 4)]
    planes += [home + lax.rem(lax.rem(wave - block - home, middle) + i, middle)
               for i in range(4, middle, 4)]
    planes += [wave - block]

    def cross(r):
        for i, plane in enumerate(planes):
            pltpu.make_async_remote_copy(
                src_ref=outgoing[r].at[pl.ds(other * wave_count + plane, 4)],
                dst_ref=crossing[r].at[pl.ds(plane, 4)],
                send_sem=fwd_send.at[r], recv_sem=lev_recv.at[r, i],
                device_id=(wave, other), device_id_type=MESH,
            ).start()

    def send(r, masks):
        for mask in masks:
            pltpu.make_async_remote_copy(
                src_ref=outgoing[r].at[lev * wave_count + flips[mask]],
                dst_ref=incoming[r].at[mine],
                send_sem=fwd_send.at[r], recv_sem=fwd_recv.at[r],
                device_id=(flips[mask], lev), device_id_type=MESH,
            ).start()

    def pass_on(r, which):
        for i in which:
            plane = planes[i]
            await_bytes(crossing[r].at[pl.ds(0, 4)], lev_recv.at[r, i])
            last = i == len(planes) - 1
            for k in range(1 if last else 0, 4):
                target = plane + flipped(block, k)
                pltpu.make_async_remote_copy(
                    src_ref=crossing[r].at[target],
                    dst_ref=incoming[r].at[other * wave_count + wave],
                    send_sem=pass_send.at[r], recv_sem=fwd_recv.at[r],
                    device_id=(target, lev), device_id_type=MESH,
                ).start()
            if last:
                incoming[r][other * wave_count + wave] = crossing[r][wave]

    source_load.wait()
    main = f32_dot(main_pick, flat[0], NN)
    rest = f32_dot(rest_picks[0], flat[0], NN)
    for r in range(1, row_count):
        rest += f32_dot(rest_picks[r], flat[r], NN)
    turned = turn(jnp.concatenate([main, rest], axis=0).astype(jnp.bfloat16))
    tail = turned[:, LANES:].reshape(sources, groups, 8, LANES)
    folded = tail[:, 0].reshape(sources * 8, LANES)
    for g in range(1, groups):
        folded += pltpu.roll(tail[:, g].reshape(sources * 8, LANES), g * fwd_step, 1)
    swung = pltpu.roll(folded, half, 1).reshape(sources, 8, LANES)
    folded = folded.reshape(sources, 8, LANES)[:, :4] + swung[:, 4:]
    by_rows(first_out)[:, :local_n] = (
        turned[:, :LANES].reshape(sources, local_n, LANES).astype(jnp.bfloat16)
    )
    by_rows(first_out)[:, local_n:] = folded.astype(jnp.bfloat16)
    pl.semaphore_wait(barrier, sources - 1)
    cross(0)
    send(0, range(1, wave_count))
    incoming[0][mine] = outgoing[0][mine]
    for r in range(1, row_count):
        turned = turn(f32_dot(main_pick, flat[r], NN).astype(jnp.bfloat16))
        by_rows(next_out)[...] = turned.reshape(sources, local_n, LANES).astype(jnp.bfloat16)
        send(r, range(1, middle))
        incoming[r][mine] = outgoing[r][mine]

    loads[0].wait()
    deep, flat_level = grid_of((depth, layer_count), 0), grid_of((depth, layer_count), 1)
    owner, place = flat_level // lev_local, flat_level % lev_local
    spot = jnp.where(place < half, owner * half + place, LANES + owner * short + place - half)
    ordered = ones_where(deep == spot)
    zeros = jnp.zeros((depth, LANES - extra), jnp.float32)

    def prepare(t, carry):
        for h, g in cells:
            j = g * 8 + h * 4 + t
            turned = f32_dot(ordered, mats_in[j], NT)
            last = jnp.concatenate([turned[:, LANES:], zeros], axis=1)
            shift = h * half + g * back_step
            if shift:
                last = pltpu.roll(last, shift, 1)
            tables[j] = jnp.concatenate([turned[:, :LANES], last], axis=1).astype(jnp.bfloat16)
        return carry

    lax.fori_loop(0, 4, prepare, 0)
    cross(1)
    pass_on(0, range(2))

    @pl.when(wave >= middle)
    def _():
        send(1, range(middle, wave_count))

    pass_on(0, range(2, len(planes)))

    come, go = grid_of((lev_count * LANES, wide), 0), grid_of((lev_count * LANES, wide), 1)
    p, lane = come // LANES, come % LANES
    h, lane = lane // half, lane % half
    g, lane = lane // fwd_step, lane % fwd_step
    target = h * LANES + g * rest_step + lane // short * extra + p * short + lane % short
    spread = ones_where((go == target) & (g < groups))

    loads[1].wait()
    row, col = grid_of((fields, layer_count), 0), grid_of((fields, layer_count), 1)
    chosen = ones_where(col == lev * lev_local + row // part_count)
    coupled_rows = f32_dot(chosen, coupler_in[...], NN)
    tops = jnp.concatenate([chosen.astype(jnp.float32), coupled_rows], axis=0)
    tops_part = lax.rem(grid_of(tops.shape, 0), part_count)
    keeps = [jnp.where(tops_part == c, tops, 0.0) for c in range(part_count)]
    pieces = [k[:, :LANES] for k in keeps] + [k[:, LANES:] for k in keeps]
    pieces.append(jnp.zeros((2 * fields, LANES - part_count * extra), jnp.float32))
    weights[...] = jnp.concatenate(pieces, axis=1).astype(jnp.bfloat16)

    for copy in loads[2:5]:
        copy.wait()
    gain = jnp.sum(
        jnp.where(col == lev * lev_local + row // part_count, strengths_in[...], 0.0),
        axis=1, keepdims=True,
    )
    n = grid_of((1, total_n), 1)
    scaled = (n * (n + 1)).astype(jnp.float32) / jnp.float32((total_n - 1) * total_n)
    damping = 1.0 / (1.0 + gain * scaled ** 2)
    spin_flat = spin_in.reshape(row_count, fields, total_n)
    vort_flat = vort_out.reshape(row_count, fields, total_n)
    for r in range(row_count):
        value = (spin_flat[r].astype(jnp.float32) * damping)
        value = jnp.where(n >= orders_in[:, r:r + 1], value, 0.0)
        vort_flat[r] = value.astype(jnp.bfloat16)


    @pl.when(wave < middle)
    def _():
        send(1, range(middle, wave_count))

    pass_on(1, range(len(planes)))
    lane = grid_of((wave_count, LANES), 1)
    near, mid, widths = range(1, 4), range(4, middle), (2, 1)
    parties = [
        [near, mid, *(range(i, i + width) for i in range(middle, wave_count, width))]
        for width in widths
    ]
    first_group = (0, len(parties[0]))

    def hand_over(ref, r, spot, target):
        pltpu.make_async_remote_copy(
            src_ref=ref, dst_ref=relayed.at[r, spot],
            send_sem=relay_send.at[r], recv_sem=relay_recv.at[r],
            device_id=(target, other), device_id_type=MESH,
        ).start()

    def give_back(r, masks):
        for mask in masks:
            copy = pltpu.make_async_remote_copy(
                src_ref=back_out.at[r, peer[mask]], dst_ref=back_in.at[r, wave],
                send_sem=back_send.at[r], recv_sem=back_recv.at[
                    first_group[r] + (
                        (mask >= 4) if mask < middle else 2 + lax.div(rank[mask], widths[r])
                    )
                ],
                device_id=(peer[mask], lev), device_id_type=MESH,
            )
            copy.start()
            if mask in near:
                hand_over(back_out.at[r, peer[mask]], r, wave, peer[mask])

    def await_group(r, group):
        party = parties[r][group]
        await_bytes(back_in.at[r, pl.ds(0, len(party))], back_recv.at[first_group[r] + group])

    def relay(r, masks):
        if masks[0]:
            await_group(r, parties[r].index(masks))
        for mask in masks:
            hand_over((back_in if mask else back_out).at[r, peer[mask]], r, peer[mask], wave)

    def solve_chunk(r):
        rows_in = by_rows(incoming[r])
        for q in range(lev_count):
            main = rows_in[pl.ds(q * wave_count, wave_count), :local_n]
            gathered[q] = main.astype(jnp.float32).reshape(block_n, LANES)
        if r == 0:
            rests = [
                rows_in[pl.ds(q * wave_count, wave_count), local_n:]
                .astype(jnp.float32).reshape(wave_count * 4, LANES)
                for q in range(lev_count)
            ]
            value = jnp.concatenate(rests, axis=1).astype(jnp.bfloat16)
            value = f32_dot(value, spread, NN)
            for h in range(2):
                rest_in[h] = value[:, h * LANES:(h + 1) * LANES]

        def solve(t, carry):
            every = pl.ds(t, wave_count, stride=4)
            lasts = None
            for h, g in cells:
                j = g * 8 + h * 4 + t
                rest = rest_in[h, every, :]
                rows = pl.ds(j, wave_count, stride=local_n)
                low, high = gathered[0, rows, :], gathered[1, rows, :]
                sides = [jnp.where(lane < half, low, high),
                         pltpu.roll(jnp.where(lane < half, high, low), half, 1)]
                stacked = []
                for c in range(part_count):
                    shift = g * rest_step + (r * part_count + c) * extra
                    moved = pltpu.roll(rest, LANES - shift, 1) if shift else rest
                    stacked.append(jnp.concatenate([sides[c], moved], axis=1)[:, :depth])
                stacked = jnp.concatenate(stacked, axis=0).astype(jnp.bfloat16)
                result = f32_dot(stacked, tables[j], NN)
                for c in range(part_count):
                    strided[c, rows, :] = result[c * wave_count:(c + 1) * wave_count, :LANES]
                last = result[:, LANES:]
                lasts = last if lasts is None else lasts + last
            total = lasts[:wave_count]
            for c in range(1, part_count):
                total += pltpu.roll(lasts[c * wave_count:(c + 1) * wave_count], c * extra, 1)
            rest_out[every, :] = total
            return carry

        lax.fori_loop(0, 4, solve, 0, unroll=4)
        rows_out = by_rows(back_out)
        for c in range(part_count):
            rows_out[r, :, c * local_n:(c + 1) * local_n] = (
                strided[c].reshape(wave_count, local_n, LANES).astype(jnp.bfloat16)
            )
        rows_out[r, :, part_count * local_n:] = (
            rest_out[...].reshape(wave_count, 4, LANES).astype(jnp.bfloat16)
        )
        relay(r, [0])
        give_back(r, range(1, wave_count if r == 0 else middle + 4))
        back_in[r, wave] = back_out[r, wave]

    heat_flat = heat_in.reshape(row_count, fields, total_n)
    div_flat = div_out.reshape(row_count, fields, total_n)
    temp_flat = temp_out.reshape(row_count, fields, total_n)

    def finish(r, wire, block):
        spots = pl.ds(pl.multiple_of(block * block_n, LANES), block_n)
        div_flat[r, :, spots], temp_flat[r, :, spots] = block_values(
            wire, weights, heat_flat, orders_in, r, block, block_n, back_step
        )

    loads[5].wait()
    for r in range(row_count):
        await_bytes(incoming[r].at[pl.ds(0, sources - 2)], fwd_recv.at[r])
        solve_chunk(r)
    def mid_if(condition, r):
        @pl.when(condition)
        def _():
            relay(r, mid)

    mid_if(wave >= 4, 0)
    give_back(1, [middle + 4])
    for i, party in enumerate(parties[0][2:]):
        relay(0, party)
        if i == 0:
            give_back(1, [middle + 5])
        if i == 1:
            give_back(1, range(middle + 6, wave_count))
            mid_if(wave >= middle, 1)
        if i == 2:
            mid_if(wave < 4, 0)
    mid_if(wave < middle, 1)
    for r in range(row_count):
        await_bytes(outgoing[r].at[pl.ds(0, sources - 1)], fwd_send.at[r])
        await_bytes(crossing[r].at[pl.ds(0, wave_count - 1)], pass_send.at[r])
    await_group(0, 0)
    finish(0, back_in, lev)
    for party in parties[1][2:]:
        relay(1, party)
    await_group(1, 0)
    finish(1, back_in, lev)
    for r in range(row_count):
        await_bytes(back_out.at[r, pl.ds(0, wave_count - 1)], back_send.at[r])
    for r in range(row_count):
        await_bytes(relayed.at[r], relay_recv.at[r])
        if r + 1 < row_count:
            finish(r, relayed, other)
    for r in range(row_count):
        await_bytes(relayed.at[r], relay_send.at[r])


def store_kernel(
    lev_count, step, vort, div, temp, wire, weights, heat, orders, vort_out, div_out, temp_out,
    div_last, temp_last, sems,
):
    row_count, lev_local, part_count, total_n = vort.shape
    block_n = total_n // lev_count
    last = row_count - 1
    lev = lax.axis_index("lev")
    mine, others = (
        pl.ds(pl.multiple_of(block * block_n, LANES), block_n)
        for block in (lev, lax.rem(lev + 1, lev_count))
    )
    pairs = [(vort, vort_out)]
    for src, dst in ((div, div_out), (temp, temp_out)):
        pairs += [(src.at[r], dst.at[r]) for r in range(last)]
        pairs.append((src.at[last, :, :, mine], dst.at[last, :, :, mine]))
    late = [(div_last, div_out.at[last, :, :, others]), (temp_last, temp_out.at[last, :, :, others])]
    copies = [
        pltpu.make_async_copy(src, dst, sems.at[i]) for i, (src, dst) in enumerate(pairs + late)
    ]
    for copy in copies[:len(pairs)]:
        copy.start()
    fields = lev_local * part_count
    values = block_values(
        wire, weights, heat.reshape(row_count, fields, total_n), orders, last,
        lax.rem(lev + 1, lev_count), block_n, step,
    )
    for ref, value in zip((div_last, temp_last), values):
        ref.reshape(fields, block_n)[...] = value
    for copy in copies[len(pairs):]:
        copy.start()
    for copy in copies:
        copy.wait()


def by_kernel(spin, source, heat, matrices, coupler, strengths, orders):
    lev_count, wave_count = lax.axis_size("lev"), lax.axis_size("wave")
    row_count, part_count, lev_local, total_n = source.shape
    block_n = total_n // lev_count
    local_n = block_n // wave_count
    layer_count = lev_local * lev_count
    fields = lev_local * part_count
    sources = wave_count * lev_count
    depth = -(-layer_count // 16) * 16
    anywhere, vmem = pl.BlockSpec(memory_space=pltpu.HBM), pl.BlockSpec(memory_space=pltpu.VMEM)
    shape = (row_count, lev_local, part_count, total_n)
    bf16, f32 = jnp.bfloat16, jnp.float32
    field = jax.ShapeDtypeStruct(shape, bf16)
    dma = pltpu.SemaphoreType.DMA
    main_pairs, rest_pairs = local_n // 2, 2
    wire_shape = (row_count, wave_count, part_count * main_pairs + rest_pairs, 2, LANES)
    wire = pltpu.VMEM(wire_shape, bf16)

    def first(count):
        return pltpu.VMEM((count, main_pairs + rest_pairs, 2, LANES), bf16)

    def following(count):
        return pltpu.VMEM((count, main_pairs, 2, LANES), bf16)

    each = dma((row_count,))
    outs = pl.pallas_call(
        functools.partial(step_kernel, wave_count, lev_count),
        out_shape=(
            field, field, field, jax.ShapeDtypeStruct(wire_shape, bf16),
            jax.ShapeDtypeStruct((2 * fields, 3 * LANES), bf16), field,
            jax.ShapeDtypeStruct((1, row_count), jnp.int32),
        ),
        in_specs=[anywhere] * 7,
        out_specs=(vmem,) * 7,
        scratch_shapes=[
            pltpu.VMEM(shape, bf16), pltpu.VMEM(shape, bf16),
            pltpu.VMEM(matrices.shape[1:], bf16), pltpu.VMEM(coupler.shape, bf16),
            pltpu.VMEM((1, layer_count), f32),
            first(sources), following(sources), first(sources), following(sources),
            first(wave_count), following(wave_count),
            pltpu.VMEM((lev_count, block_n, LANES), f32),
            pltpu.VMEM((2, wave_count * 4, LANES), f32),
            pltpu.VMEM((local_n, depth, 2 * LANES), bf16),
            pltpu.VMEM((part_count, block_n, LANES), f32),
            pltpu.VMEM((wave_count * 4, LANES), f32),
            wire, wire,
            dma((7,)), each, each, dma((row_count, wave_count // 4)), each,
            each, dma((4 + wave_count // 4 + wave_count // 2,)), each, each,
        ],
        compiler_params=pltpu.CompilerParams(
            collective_id=0, has_side_effects=True, vmem_limit_bytes=48 * 2**20
        ),
    )(
        *(
            pltpu.with_memory_space_constraint(value, pltpu.HBM)
            for value in (
                spin.transpose(0, 2, 1, 3), source.transpose(0, 2, 1, 3), heat.transpose(0, 2, 1, 3),
                matrices[0], coupler, strengths.reshape(1, layer_count), orders.reshape(1, row_count),
            )
        )
    )
    extra = layer_count - LANES
    last_block = pltpu.VMEM((lev_local, part_count, block_n), bf16)
    outs = pl.pallas_call(
        functools.partial(store_kernel, lev_count, part_count * extra),
        out_shape=(field,) * 3, in_specs=[vmem] * 7, out_specs=(anywhere,) * 3,
        scratch_shapes=[last_block, last_block, dma((2 * row_count + 3,))],
        compiler_params=pltpu.CompilerParams(vmem_limit_bytes=8 * 2**20),
    )(*outs)
    return tuple(out.transpose(0, 2, 1, 3) for out in outs)


def kernel_fits(source_shape, lev_count, wave_count):
    row_count, part_count, lev_local, total_n = source_shape
    block_n = total_n // lev_count
    extra = lev_local * lev_count - LANES
    half = LANES // 2
    groups = block_n // (8 * wave_count)
    return (
        lev_count == 2
        and part_count == 2
        and row_count == 2
        and wave_count > 8
        and wave_count & (wave_count - 1) == 0
        and wave_count % 8 == 0
        and block_n % LANES == 0
        and total_n % (2 * LANES) == 0
        and block_n % (8 * wave_count) == 0
        and extra > 0
        and extra * row_count * part_count * groups <= LANES
        and (lev_local - half) * row_count * part_count * groups <= half
        and extra * part_count * groups <= half
    )


def on_device(
    spin_tendency,
    spreading_source,
    heat_source,
    helmholtz_inverses,
    heat_spreading_coupler,
    smoothing_strengths,
    azimuthal_order_list,
):
    lev_count, wave_count = lax.axis_size("lev"), lax.axis_size("wave")
    lev_index = lax.axis_index("lev")
    lev_local, total_n = spreading_source.shape[2:]
    empty_placeholder = jnp.zeros((), jnp.bfloat16)
    if kernel_fits(spreading_source.shape, lev_count, wave_count):
        return by_kernel(
            spin_tendency, spreading_source, heat_source, helmholtz_inverses,
            heat_spreading_coupler, smoothing_strengths, azimuthal_order_list,
        )
    spreading_updated, coupled_out = exchange_by_collectives(
        spreading_source, helmholtz_inverses, heat_spreading_coupler
    )
    heat_updated = (heat_source.astype(jnp.float32) - coupled_out.astype(jnp.float32)).astype(
        jnp.bfloat16
    )
    level_gain = lax.dynamic_slice_in_dim(smoothing_strengths, lev_index * lev_local, lev_local)
    damping = damping_table(level_gain, jnp.arange(total_n, dtype=jnp.int32), total_n)
    spin_updated = (spin_tendency.astype(jnp.float32) * damping[None, None]).astype(jnp.bfloat16)
    interior_slice = (
        jnp.arange(total_n, dtype=jnp.int32)[None, :] >= azimuthal_order_list[:, None]
    )[:, None, None, :]
    return (
        jnp.where(interior_slice, spin_updated, empty_placeholder),
        jnp.where(interior_slice, spreading_updated, empty_placeholder),
        jnp.where(interior_slice, heat_updated, empty_placeholder),
    )


def solution(mesh):
    return jax.shard_map(
        on_device,
        mesh=mesh,
        in_specs=(
            P("wave", None, "lev", None),
            P("wave", None, "lev", None),
            P("wave", None, "lev", None),
            P("lev", "wave", None, None),
            P(),
            P(),
            P("wave"),
        ),
        out_specs=(
            P("wave", None, "lev", None),
            P("wave", None, "lev", None),
            P("wave", None, "lev", None),
        ),
        check_vma=False,
    )
```

```python
import functools
import jax
import jax.numpy as jnp
from jax import lax
from jax.experimental import pallas as pl
from jax.experimental.pallas import tpu as pltpu
from jax.sharding import PartitionSpec as P

LANES = 128
MESH = pl.DeviceIdType.MESH
NN = (((1,), (0,)), ((), ()))
NT = (((1,), (1,)), ((), ()))


def damping_table(level_gain, wavenumbers, total_n):
    scaled = (wavenumbers * (wavenumbers + 1)).astype(jnp.float32) / jnp.float32(
        (total_n - 1) * total_n
    )
    return 1.0 / (1.0 + level_gain[:, None] * scaled[None, :] ** 2)


def exchange_by_collectives(spreading_source, helmholtz_inverses, heat_spreading_coupler):
    lev_count = lax.axis_size("lev")
    row_count, part_count, lev_local, total_n = spreading_source.shape
    block_n = total_n // lev_count
    layer_count = lev_local * lev_count
    flat_rows = row_count * part_count
    wave_count = lax.axis_size("wave")
    local_n = block_n // wave_count
    rhs_div = lax.all_to_all(spreading_source, "lev", split_axis=3, concat_axis=2, tiled=True)
    outgoing = rhs_div.reshape(flat_rows, layer_count, wave_count, local_n).transpose(2, 3, 0, 1)
    outgoing = outgoing.reshape(wave_count, local_n, flat_rows * layer_count)
    columns = lax.all_to_all(outgoing, "wave", split_axis=0, concat_axis=0, tiled=True)
    columns = columns.reshape(wave_count, local_n, flat_rows, layer_count)
    solved_columns = jnp.einsum(
        "jkp,wjcp->wjck", helmholtz_inverses[0], columns, preferred_element_type=jnp.float32
    ).astype(jnp.bfloat16)
    solved_columns = solved_columns.reshape(wave_count, local_n, flat_rows * layer_count)
    returned = lax.all_to_all(solved_columns, "wave", split_axis=0, concat_axis=0, tiled=True)
    answer_fields = returned.reshape(block_n, flat_rows, layer_count).transpose(1, 2, 0)
    coupled = jnp.einsum(
        "om,dms->dos", heat_spreading_coupler, answer_fields, preferred_element_type=jnp.float32
    ).astype(jnp.bfloat16)
    both = jnp.stack([answer_fields, coupled])
    both = lax.all_to_all(both, "lev", split_axis=2, concat_axis=3, tiled=True)
    both = both.reshape(2, row_count, part_count, lev_local, total_n)
    spreading_updated, coupled_out = both[0], both[1]
    return spreading_updated, coupled_out


def f32_dot(left, right, dims):
    return lax.dot_general(left, right, dims, preferred_element_type=jnp.float32)


def grid_of(shape, axis):
    return lax.broadcasted_iota(jnp.int32, shape, axis)


def ones_where(condition, dtype=jnp.bfloat16):
    return jnp.where(condition, 1.0, 0.0).astype(dtype)


def flipped(value, mask):
    out, bit = value, 1
    while bit <= mask:
        if mask & bit:
            out = out + bit * (1 - 2 * lax.rem(lax.div(value, bit), 2))
        bit *= 2
    return out


def by_rows(ref):
    return ref.reshape(*ref.shape[:-3], ref.shape[-3] * 2, LANES)


def block_values(wire, weights, heat_flat, orders, r, block, block_n, step):
    wave_count = wire.shape[1]
    local_n = block_n // wave_count
    groups = local_n // 8
    fields = heat_flat.shape[1]
    rows_in = by_rows(wire)
    parts = (rows_in.shape[2] - 4) // local_n
    sides = [
        rows_in[r, :, c * local_n:(c + 1) * local_n].astype(jnp.float32).reshape(block_n, LANES)
        for c in range(parts)
    ]
    folded = rows_in[r, :, parts * local_n:].astype(jnp.float32)
    swung = pltpu.roll(folded.reshape(wave_count * 4, LANES), LANES // 2, 1)
    folded = jnp.concatenate([folded, swung.reshape(wave_count, 4, LANES)], axis=1)
    folded = folded.reshape(wave_count * 8, LANES)
    rest = [(pltpu.roll(folded, LANES - g * step, 1) if g else folded)
            .reshape(wave_count, 1, 8, LANES) for g in range(groups)]
    sides.append(jnp.concatenate(rest, axis=1).reshape(block_n, LANES))
    packed = jnp.concatenate(sides, axis=1).astype(jnp.bfloat16)
    result = f32_dot(weights[...], packed, NT)
    spots = pl.ds(pl.multiple_of(block * block_n, LANES), block_n)
    inside = block * block_n + grid_of((1, block_n), 1) >= orders[:, r:r + 1]
    coupled = result[fields:].astype(jnp.bfloat16).astype(jnp.float32)
    warmed = heat_flat[r, :, spots].astype(jnp.float32) - coupled
    return (
        jnp.where(inside, result[:fields], 0.0).astype(jnp.bfloat16),
        jnp.where(inside, warmed, 0.0).astype(jnp.bfloat16),
    )


def step_kernel(
    wave_count, lev_count, spin, source, heat, matrices, coupler, strengths, orders,
    vort_out, div_out, temp_out, relayed, weights, heat_in, orders_in,
    spin_in, source_in, mats_in, coupler_in, strengths_in,
    first_out, next_out, first_in, next_in, first_lev, next_lev, gathered, rest_in, tables, strided, rest_out,
    back_out, back_in,
    load_sem, fwd_send, fwd_recv, lev_recv, pass_send, back_send, back_recv, relay_send, relay_recv,
):
    wave, lev = lax.axis_index("wave"), lax.axis_index("lev")
    row_count, lev_local, part_count, total_n = source.shape
    block_n = total_n // lev_count
    local_n = block_n // wave_count
    groups = local_n // 8
    layer_count = lev_local * lev_count
    fields = lev_local * part_count
    half = LANES // part_count
    short = lev_local - half
    extra = layer_count - LANES
    depth = tables.shape[1]
    sources = wave_count * lev_count
    wide = 2 * LANES
    cells = [(h, g) for h in range(2) for g in range(groups)]
    fwd_step = row_count * part_count * short
    back_step = part_count * extra
    rest_step = row_count * part_count * extra

    middle = wave_count // 2
    block = lax.rem(wave, 4)
    across = middle * (1 - lax.div(wave, middle))
    flips = [flipped(wave, mask) for mask in range(wave_count)]
    peer = flips[:middle]
    side, core = lax.div(block, 2), lax.rem(block, 2)
    peer += [across + i // 2 * 2 + flipped(core, i % 2) for i in range(middle)]
    rank = [
        lax.div(lax.rem(wave, middle), 4) * 4 + side * 2 + i % 2 for i in range(middle)
    ]
    rank = [*range(middle), *rank]
    other = lax.rem(lev + 1, lev_count)
    outward = [*range(1, wave_count), 0]
    barrier = pltpu.get_barrier_semaphore()

    def greet(masks):
        for mask in masks:
            for t, q in enumerate((lev, other)):
                if mask or t:
                    pl.semaphore_signal(
                        barrier, inc=1, device_id=(flips[mask], q), device_id_type=MESH
                    )

    greet(range(wave_count - 1, middle - 1, -1))
    loads = []
    small = [(matrices, mats_in), (coupler, coupler_in), (strengths, strengths_in),
             (orders, orders_in), (spin, spin_in), (heat, heat_in)]
    for i, (src, dst) in enumerate(
        [(source, source_in), *small]
    ):
        copy = pltpu.make_async_copy(src, dst, load_sem.at[i])
        copy.start()
        loads.append(copy)
    source_load, loads = loads[0], loads[1:]

    greet(range(middle - 1, -1, -1))

    out_row, in_row = grid_of((wide, fields), 0), grid_of((wide, fields), 1)
    level, part = in_row // part_count, in_row % part_count
    main_spot = lax.rem(part + lev, part_count) * half + level
    main_pick = ones_where(
        (out_row == main_spot)[:LANES] & (level < half)[:LANES]
    )
    rest_picks = [
        ones_where(
            (out_row == (r * part_count + part) * short + level - half)[:LANES]
            & (level >= half)[:LANES]
        )
        for r in range(row_count)
    ]
    eye = ones_where(grid_of((wide, wide), 0) == grid_of((wide, wide), 1))
    flat = source_in.reshape(row_count, fields, total_n)
    mine = lev * wave_count + wave

    def turn(rows):
        return jnp.concatenate(
            [f32_dot(eye, rows[:, k:k + wide], NT) for k in range(0, total_n, wide)], axis=0
        )

    outgoing, incoming = [first_out, next_out], [first_in, next_in]

    def await_bytes(ref, sem):
        pltpu.make_async_copy(ref, ref, sem).wait()

    crossing = [first_lev, next_lev]
    home = middle - across
    planes = [across + i for i in range(0, middle, 4)]
    planes += [home + lax.rem(lax.rem(wave - block - home, middle) + i, middle)
               for i in range(4, middle, 4)]
    planes += [wave - block]

    def cross(r):
        for i, plane in enumerate(planes):
            pltpu.make_async_remote_copy(
                src_ref=outgoing[r].at[pl.ds(other * wave_count + plane, 4)],
                dst_ref=crossing[r].at[pl.ds(plane, 4)],
                send_sem=fwd_send.at[r], recv_sem=lev_recv.at[r, i],
                device_id=(wave, other), device_id_type=MESH,
            ).start()

    def send(r, masks):
        for mask in masks:
            pltpu.make_async_remote_copy(
                src_ref=outgoing[r].at[lev * wave_count + flips[mask]],
                dst_ref=incoming[r].at[mine],
                send_sem=fwd_send.at[r], recv_sem=fwd_recv.at[r],
                device_id=(flips[mask], lev), device_id_type=MESH,
            ).start()

    def pass_on(r, which):
        for i in which:
            plane = planes[i]
            await_bytes(crossing[r].at[pl.ds(0, 4)], lev_recv.at[r, i])
            last = i == len(planes) - 1
            for k in range(1 if last else 0, 4):
                target = plane + flipped(block, k)
                pltpu.make_async_remote_copy(
                    src_ref=crossing[r].at[target],
                    dst_ref=incoming[r].at[other * wave_count + wave],
                    send_sem=pass_send.at[r], recv_sem=fwd_recv.at[r],
                    device_id=(target, lev), device_id_type=MESH,
                ).start()
            if last:
                incoming[r][other * wave_count + wave] = crossing[r][wave]

    source_load.wait()
    main = f32_dot(main_pick, flat[0], NN)
    rest = f32_dot(rest_picks[0], flat[0], NN)
    for r in range(1, row_count):
        rest += f32_dot(rest_picks[r], flat[r], NN)
    turned = turn(jnp.concatenate([main, rest], axis=0).astype(jnp.bfloat16))
    tail = turned[:, LANES:].reshape(sources, groups, 8, LANES)
    folded = tail[:, 0].reshape(sources * 8, LANES)
    for g in range(1, groups):
        folded += pltpu.roll(tail[:, g].reshape(sources * 8, LANES), g * fwd_step, 1)
    swung = pltpu.roll(folded, half, 1).reshape(sources, 8, LANES)
    folded = folded.reshape(sources, 8, LANES)[:, :4] + swung[:, 4:]
    by_rows(first_out)[:, :local_n] = (
        turned[:, :LANES].reshape(sources, local_n, LANES).astype(jnp.bfloat16)
    )
    by_rows(first_out)[:, local_n:] = folded.astype(jnp.bfloat16)
    pl.semaphore_wait(barrier, sources - 1)
    cross(0)
    send(0, range(1, wave_count))
    incoming[0][mine] = outgoing[0][mine]
    for r in range(1, row_count):
        turned = turn(f32_dot(main_pick, flat[r], NN).astype(jnp.bfloat16))
        by_rows(next_out)[...] = turned.reshape(sources, local_n, LANES).astype(jnp.bfloat16)
        send(r, range(1, middle))
        incoming[r][mine] = outgoing[r][mine]

    loads[0].wait()
    deep, flat_level = grid_of((depth, layer_count), 0), grid_of((depth, layer_count), 1)
    owner, place = flat_level // lev_local, flat_level % lev_local
    spot = jnp.where(place < half, owner * half + place, LANES + owner * short + place - half)
    ordered = ones_where(deep == spot)
    zeros = jnp.zeros((depth, LANES - extra), jnp.float32)

    def prepare(t, carry):
        for h, g in cells:
            j = g * 8 + h * 4 + t
            turned = f32_dot(ordered, mats_in[j], NT)
            last = jnp.concatenate([turned[:, LANES:], zeros], axis=1)
            shift = h * half + g * back_step
            if shift:
                last = pltpu.roll(last, shift, 1)
            tables[j] = jnp.concatenate([turned[:, :LANES], last], axis=1).astype(jnp.bfloat16)
        return carry

    lax.fori_loop(0, 4, prepare, 0)
    cross(1)
    pass_on(0, range(2))

    @pl.when(wave >= middle)
    def _():
        send(1, range(middle, wave_count))

    pass_on(0, range(2, len(planes)))

    come, go = grid_of((lev_count * LANES, wide), 0), grid_of((lev_count * LANES, wide), 1)
    p, lane = come // LANES, come % LANES
    h, lane = lane // half, lane % half
    g, lane = lane // fwd_step, lane % fwd_step
    target = h * LANES + g * rest_step + lane // short * extra + p * short + lane % short
    spread = ones_where((go == target) & (g < groups))

    loads[1].wait()
    row, col = grid_of((fields, layer_count), 0), grid_of((fields, layer_count), 1)
    chosen = ones_where(col == lev * lev_local + row // part_count)
    coupled_rows = f32_dot(chosen, coupler_in[...], NN)
    tops = jnp.concatenate([chosen.astype(jnp.float32), coupled_rows], axis=0)
    tops_part = lax.rem(grid_of(tops.shape, 0), part_count)
    keeps = [jnp.where(tops_part == c, tops, 0.0) for c in range(part_count)]
    pieces = [k[:, :LANES] for k in keeps] + [k[:, LANES:] for k in keeps]
    pieces.append(jnp.zeros((2 * fields, LANES - part_count * extra), jnp.float32))
    weights[...] = jnp.concatenate(pieces, axis=1).astype(jnp.bfloat16)

    for copy in loads[2:5]:
        copy.wait()
    gain = jnp.sum(
        jnp.where(col == lev * lev_local + row // part_count, strengths_in[...], 0.0),
        axis=1, keepdims=True,
    )
    n = grid_of((1, total_n), 1)
    scaled = (n * (n + 1)).astype(jnp.float32) / jnp.float32((total_n - 1) * total_n)
    damping = 1.0 / (1.0 + gain * scaled ** 2)
    spin_flat = spin_in.reshape(row_count, fields, total_n)
    vort_flat = vort_out.reshape(row_count, fields, total_n)
    for r in range(row_count):
        value = (spin_flat[r].astype(jnp.float32) * damping)
        value = jnp.where(n >= orders_in[:, r:r + 1], value, 0.0)
        vort_flat[r] = value.astype(jnp.bfloat16)


    @pl.when(wave < middle)
    def _():
        send(1, range(middle, wave_count))

    pass_on(1, range(len(planes)))
    lane = grid_of((wave_count, LANES), 1)
    near, mid, widths = range(1, 4), range(4, middle), (2, 1)
    parties = [
        [near, mid, *(range(i, i + width) for i in range(middle, wave_count, width))]
        for width in widths
    ]
    first_group = (0, len(parties[0]))

    def hand_over(ref, r, spot, target):
        pltpu.make_async_remote_copy(
            src_ref=ref, dst_ref=relayed.at[r, spot],
            send_sem=relay_send.at[r], recv_sem=relay_recv.at[r],
            device_id=(target, other), device_id_type=MESH,
        ).start()

    def give_back(r, masks):
        for mask in masks:
            copy = pltpu.make_async_remote_copy(
                src_ref=back_out.at[r, peer[mask]], dst_ref=back_in.at[r, wave],
                send_sem=back_send.at[r], recv_sem=back_recv.at[
                    first_group[r] + (
                        (mask >= 4) if mask < middle else 2 + lax.div(rank[mask], widths[r])
                    )
                ],
                device_id=(peer[mask], lev), device_id_type=MESH,
            )
            copy.start()
            if mask in near:
                hand_over(back_out.at[r, peer[mask]], r, wave, peer[mask])

    def await_group(r, group):
        party = parties[r][group]
        await_bytes(back_in.at[r, pl.ds(0, len(party))], back_recv.at[first_group[r] + group])

    def relay(r, masks):
        if masks[0]:
            await_group(r, parties[r].index(masks))
        for mask in masks:
            hand_over((back_in if mask else back_out).at[r, peer[mask]], r, peer[mask], wave)

    def solve_chunk(r):
        rows_in = by_rows(incoming[r])
        for q in range(lev_count):
            main = rows_in[pl.ds(q * wave_count, wave_count), :local_n]
            gathered[q] = main.astype(jnp.float32).reshape(block_n, LANES)
        if r == 0:
            rests = [
                rows_in[pl.ds(q * wave_count, wave_count), local_n:]
                .astype(jnp.float32).reshape(wave_count * 4, LANES)
                for q in range(lev_count)
            ]
            value = jnp.concatenate(rests, axis=1).astype(jnp.bfloat16)
            value = f32_dot(value, spread, NN)
            for h in range(2):
                rest_in[h] = value[:, h * LANES:(h + 1) * LANES]

        def solve(t, carry):
            every = pl.ds(t, wave_count, stride=4)
            lasts = None
            for h, g in cells:
                j = g * 8 + h * 4 + t
                rest = rest_in[h, every, :]
                rows = pl.ds(j, wave_count, stride=local_n)
                low, high = gathered[0, rows, :], gathered[1, rows, :]
                sides = [jnp.where(lane < half, low, high),
                         pltpu.roll(jnp.where(lane < half, high, low), half, 1)]
                stacked = []
                for c in range(part_count):
                    shift = g * rest_step + (r * part_count + c) * extra
                    moved = pltpu.roll(rest, LANES - shift, 1) if shift else rest
                    stacked.append(jnp.concatenate([sides[c], moved], axis=1)[:, :depth])
                stacked = jnp.concatenate(stacked, axis=0).astype(jnp.bfloat16)
                result = f32_dot(stacked, tables[j], NN)
                for c in range(part_count):
                    strided[c, rows, :] = result[c * wave_count:(c + 1) * wave_count, :LANES]
                last = result[:, LANES:]
                lasts = last if lasts is None else lasts + last
            total = lasts[:wave_count]
            for c in range(1, part_count):
                total += pltpu.roll(lasts[c * wave_count:(c + 1) * wave_count], c * extra, 1)
            rest_out[every, :] = total
            return carry

        lax.fori_loop(0, 4, solve, 0, unroll=4)
        rows_out = by_rows(back_out)
        for c in range(part_count):
            rows_out[r, :, c * local_n:(c + 1) * local_n] = (
                strided[c].reshape(wave_count, local_n, LANES).astype(jnp.bfloat16)
            )
        rows_out[r, :, part_count * local_n:] = (
            rest_out[...].reshape(wave_count, 4, LANES).astype(jnp.bfloat16)
        )
        relay(r, [0])
        give_back(r, range(1, wave_count if r == 0 else middle + 4))
        back_in[r, wave] = back_out[r, wave]

    heat_flat = heat_in.reshape(row_count, fields, total_n)
    div_flat = div_out.reshape(row_count, fields, total_n)
    temp_flat = temp_out.reshape(row_count, fields, total_n)

    def finish(r, wire, block):
        spots = pl.ds(pl.multiple_of(block * block_n, LANES), block_n)
        div_flat[r, :, spots], temp_flat[r, :, spots] = block_values(
            wire, weights, heat_flat, orders_in, r, block, block_n, back_step
        )

    loads[5].wait()
    for r in range(row_count):
        await_bytes(incoming[r].at[pl.ds(0, sources - 2)], fwd_recv.at[r])
        solve_chunk(r)
    def mid_if(condition, r):
        @pl.when(condition)
        def _():
            relay(r, mid)

    mid_if(wave >= 4, 0)
    give_back(1, [middle + 4])
    for i, party in enumerate(parties[0][2:]):
        relay(0, party)
        if i == 0:
            give_back(1, [middle + 5])
        if i == 1:
            give_back(1, range(middle + 6, wave_count))
            mid_if(wave >= middle, 1)
        if i == 2:
            mid_if(wave < 4, 0)
    mid_if(wave < middle, 1)
    for r in range(row_count):
        await_bytes(outgoing[r].at[pl.ds(0, sources - 1)], fwd_send.at[r])
        await_bytes(crossing[r].at[pl.ds(0, wave_count - 1)], pass_send.at[r])
    for party in parties[1][2:]:
        relay(1, party)
    await_group(0, 0)
    finish(0, back_in, lev)
    await_group(1, 0)
    finish(1, back_in, lev)
    for r in range(row_count):
        await_bytes(back_out.at[r, pl.ds(0, wave_count - 1)], back_send.at[r])
    for r in range(row_count):
        await_bytes(relayed.at[r], relay_recv.at[r])
        if r + 1 < row_count:
            finish(r, relayed, other)
    for r in range(row_count):
        await_bytes(relayed.at[r], relay_send.at[r])


def store_kernel(
    lev_count, step, vort, div, temp, wire, weights, heat, orders, vort_out, div_out, temp_out,
    div_last, temp_last, sems,
):
    row_count, lev_local, part_count, total_n = vort.shape
    block_n = total_n // lev_count
    last = row_count - 1
    lev = lax.axis_index("lev")
    mine, others = (
        pl.ds(pl.multiple_of(block * block_n, LANES), block_n)
        for block in (lev, lax.rem(lev + 1, lev_count))
    )
    pairs = [(vort, vort_out)]
    for src, dst in ((div, div_out), (temp, temp_out)):
        pairs += [(src.at[r], dst.at[r]) for r in range(last)]
        pairs.append((src.at[last, :, :, mine], dst.at[last, :, :, mine]))
    late = [(div_last, div_out.at[last, :, :, others]), (temp_last, temp_out.at[last, :, :, others])]
    copies = [
        pltpu.make_async_copy(src, dst, sems.at[i]) for i, (src, dst) in enumerate(pairs + late)
    ]
    for copy in copies[:len(pairs)]:
        copy.start()
    fields = lev_local * part_count
    values = block_values(
        wire, weights, heat.reshape(row_count, fields, total_n), orders, last,
        lax.rem(lev + 1, lev_count), block_n, step,
    )
    for ref, value in zip((div_last, temp_last), values):
        ref.reshape(fields, block_n)[...] = value
    for copy in copies[len(pairs):]:
        copy.start()
    for copy in copies:
        copy.wait()


def by_kernel(spin, source, heat, matrices, coupler, strengths, orders):
    lev_count, wave_count = lax.axis_size("lev"), lax.axis_size("wave")
    row_count, part_count, lev_local, total_n = source.shape
    block_n = total_n // lev_count
    local_n = block_n // wave_count
    layer_count = lev_local * lev_count
    fields = lev_local * part_count
    sources = wave_count * lev_count
    depth = -(-layer_count // 16) * 16
    anywhere, vmem = pl.BlockSpec(memory_space=pltpu.HBM), pl.BlockSpec(memory_space=pltpu.VMEM)
    shape = (row_count, lev_local, part_count, total_n)
    bf16, f32 = jnp.bfloat16, jnp.float32
    field = jax.ShapeDtypeStruct(shape, bf16)
    dma = pltpu.SemaphoreType.DMA
    main_pairs, rest_pairs = local_n // 2, 2
    wire_shape = (row_count, wave_count, part_count * main_pairs + rest_pairs, 2, LANES)
    wire = pltpu.VMEM(wire_shape, bf16)

    def first(count):
        return pltpu.VMEM((count, main_pairs + rest_pairs, 2, LANES), bf16)

    def following(count):
        return pltpu.VMEM((count, main_pairs, 2, LANES), bf16)

    each = dma((row_count,))
    outs = pl.pallas_call(
        functools.partial(step_kernel, wave_count, lev_count),
        out_shape=(
            field, field, field, jax.ShapeDtypeStruct(wire_shape, bf16),
            jax.ShapeDtypeStruct((2 * fields, 3 * LANES), bf16), field,
            jax.ShapeDtypeStruct((1, row_count), jnp.int32),
        ),
        in_specs=[anywhere] * 7,
        out_specs=(vmem,) * 7,
        scratch_shapes=[
            pltpu.VMEM(shape, bf16), pltpu.VMEM(shape, bf16),
            pltpu.VMEM(matrices.shape[1:], bf16), pltpu.VMEM(coupler.shape, bf16),
            pltpu.VMEM((1, layer_count), f32),
            first(sources), following(sources), first(sources), following(sources),
            first(wave_count), following(wave_count),
            pltpu.VMEM((lev_count, block_n, LANES), f32),
            pltpu.VMEM((2, wave_count * 4, LANES), f32),
            pltpu.VMEM((local_n, depth, 2 * LANES), bf16),
            pltpu.VMEM((part_count, block_n, LANES), f32),
            pltpu.VMEM((wave_count * 4, LANES), f32),
            wire, wire,
            dma((7,)), each, each, dma((row_count, wave_count // 4)), each,
            each, dma((4 + wave_count // 4 + wave_count // 2,)), each, each,
        ],
        compiler_params=pltpu.CompilerParams(
            collective_id=0, has_side_effects=True, vmem_limit_bytes=48 * 2**20
        ),
    )(
        *(
            pltpu.with_memory_space_constraint(value, pltpu.HBM)
            for value in (
                spin.transpose(0, 2, 1, 3), source.transpose(0, 2, 1, 3), heat.transpose(0, 2, 1, 3),
                matrices[0], coupler, strengths.reshape(1, layer_count), orders.reshape(1, row_count),
            )
        )
    )
    extra = layer_count - LANES
    last_block = pltpu.VMEM((lev_local, part_count, block_n), bf16)
    outs = pl.pallas_call(
        functools.partial(store_kernel, lev_count, part_count * extra),
        out_shape=(field,) * 3, in_specs=[vmem] * 7, out_specs=(anywhere,) * 3,
        scratch_shapes=[last_block, last_block, dma((2 * row_count + 3,))],
        compiler_params=pltpu.CompilerParams(vmem_limit_bytes=8 * 2**20),
    )(*outs)
    return tuple(out.transpose(0, 2, 1, 3) for out in outs)


def kernel_fits(source_shape, lev_count, wave_count):
    row_count, part_count, lev_local, total_n = source_shape
    block_n = total_n // lev_count
    extra = lev_local * lev_count - LANES
    half = LANES // 2
    groups = block_n // (8 * wave_count)
    return (
        lev_count == 2
        and part_count == 2
        and row_count == 2
        and wave_count > 8
        and wave_count & (wave_count - 1) == 0
        and wave_count % 8 == 0
        and block_n % LANES == 0
        and total_n % (2 * LANES) == 0
        and block_n % (8 * wave_count) == 0
        and extra > 0
        and extra * row_count * part_count * groups <= LANES
        and (lev_local - half) * row_count * part_count * groups <= half
        and extra * part_count * groups <= half
    )


def on_device(
    spin_tendency,
    spreading_source,
    heat_source,
    helmholtz_inverses,
    heat_spreading_coupler,
    smoothing_strengths,
    azimuthal_order_list,
):
    lev_count, wave_count = lax.axis_size("lev"), lax.axis_size("wave")
    lev_index = lax.axis_index("lev")
    lev_local, total_n = spreading_source.shape[2:]
    empty_placeholder = jnp.zeros((), jnp.bfloat16)
    if kernel_fits(spreading_source.shape, lev_count, wave_count):
        return by_kernel(
            spin_tendency, spreading_source, heat_source, helmholtz_inverses,
            heat_spreading_coupler, smoothing_strengths, azimuthal_order_list,
        )
    spreading_updated, coupled_out = exchange_by_collectives(
        spreading_source, helmholtz_inverses, heat_spreading_coupler
    )
    heat_updated = (heat_source.astype(jnp.float32) - coupled_out.astype(jnp.float32)).astype(
        jnp.bfloat16
    )
    level_gain = lax.dynamic_slice_in_dim(smoothing_strengths, lev_index * lev_local, lev_local)
    damping = damping_table(level_gain, jnp.arange(total_n, dtype=jnp.int32), total_n)
    spin_updated = (spin_tendency.astype(jnp.float32) * damping[None, None]).astype(jnp.bfloat16)
    interior_slice = (
        jnp.arange(total_n, dtype=jnp.int32)[None, :] >= azimuthal_order_list[:, None]
    )[:, None, None, :]
    return (
        jnp.where(interior_slice, spin_updated, empty_placeholder),
        jnp.where(interior_slice, spreading_updated, empty_placeholder),
        jnp.where(interior_slice, heat_updated, empty_placeholder),
    )


def solution(mesh):
    return jax.shard_map(
        on_device,
        mesh=mesh,
        in_specs=(
            P("wave", None, "lev", None),
            P("wave", None, "lev", None),
            P("wave", None, "lev", None),
            P("lev", "wave", None, None),
            P(),
            P(),
            P("wave"),
        ),
        out_specs=(
            P("wave", None, "lev", None),
            P("wave", None, "lev", None),
            P("wave", None, "lev", None),
        ),
        check_vma=False,
    )
```
